8 devices in a mesh: dp: 8 (over z, y, x, core).
Axes of the slice: x: 2, y: 2, z: 1, core: 2. Of those that a mesh axis runs over, the one named last changes fastest.
Arguments:
- act_in: bfloat16 [1024, 7, 7, 1024], P('dp')
- shortcut: bfloat16 [1024, 7, 7, 2048], P('dp')
- labels: int32 [1024], P('dp')
- w_conv: float32 [1024, 2048], replicated
- bn_gamma: float32 [2048], replicated
- bn_beta: float32 [2048], replicated
- w_fc: float32 [2048, 1000], replicated
- fc_bias: float32 [1000], replicated
- vel_conv: float32 [1024, 2048], replicated
- vel_gamma: float32 [2048], replicated
- vel_beta: float32 [2048], replicated
- vel_fc: float32 [2048, 1000], replicated
- vel_bias: float32 [1000], replicated
- learn_rate: float32 [], replicated
Outputs:
- output 1: float32 [1024, 2048], replicated
- output 2: float32 [2048], replicated
- output 3: float32 [2048], replicated
- output 4: float32 [2048, 1000], replicated
- output 5: float32 [1000], replicated
- output 6: float32 [1024, 2048], replicated
- output 7: float32 [2048], replicated
- output 8: float32 [2048], replicated
- output 9: float32 [2048, 1000], replicated
- output 10: float32 [1000], replicated
- output 11: float32 [], replicated
All inputs are finite; a program needn't handle non-finite values.
Results may differ from the reference program's by a relative error of at most 0.00917121.
Values sent between devices are 32-bit elements.
A program may use at most 1 GiB of HBM per device.

```python
import jax
import jax.numpy as jnp
from jax import lax

B_DEV = 128
DP = 8
SIDE = 7
C_MID = 1024
C_OUT = 2048
CLASSES = 1000

BN_EPS = 1e-5
SMOOTHING = 0.1
MOMENTUM = 0.9
TRUST_COEF = 0.001
WEIGHT_DECAY = 5e-5


def setup_inputs(seed: int = 0) -> dict:
    root_key = jax.random.key(seed)
    sub_keys = jax.random.split(root_key, 16)
    global_rows = DP * B_DEV
    step_scale = 2.5
    dev_shift = 0.5 * jax.random.normal(sub_keys[0], (DP, 1, 1, 1, C_MID), jnp.float32)
    act_in = jax.nn.relu(jax.random.normal(sub_keys[1], (DP, B_DEV, SIDE, SIDE, C_MID), jnp.float32) + dev_shift)
    act_in = act_in.reshape(global_rows, SIDE, SIDE, C_MID).astype(jnp.bfloat16)
    shortcut = jax.nn.relu(jax.random.normal(sub_keys[2], (global_rows, SIDE, SIDE, C_OUT), jnp.float32)).astype(jnp.bfloat16)
    labels = jax.random.randint(sub_keys[3], (global_rows,), 0, CLASSES, jnp.int32)
    w_conv = C_MID ** -0.5 * jax.random.normal(sub_keys[4], (C_MID, C_OUT), jnp.float32)
    bn_gamma = jax.random.uniform(sub_keys[5], (C_OUT,), jnp.float32, 0.5, 1.5)
    bn_beta = 0.5 * jax.random.normal(sub_keys[6], (C_OUT,), jnp.float32)
    w_fc = C_OUT ** -0.5 * jax.random.normal(sub_keys[7], (C_OUT, CLASSES), jnp.float32)
    fc_bias = 0.5 * jax.random.normal(sub_keys[8], (CLASSES,), jnp.float32)
    vel_conv = 0.001 * step_scale * C_MID ** -0.5 * jax.random.normal(sub_keys[9], (C_MID, C_OUT), jnp.float32)
    vel_gamma = 0.5 * step_scale * (global_rows * C_OUT) ** -0.5 * jax.random.normal(sub_keys[10], (C_OUT,), jnp.float32)
    vel_beta = 0.5 * step_scale * (global_rows * C_OUT) ** -0.5 * jax.random.normal(sub_keys[11], (C_OUT,), jnp.float32)
    vel_fc = 0.001 * step_scale * C_OUT ** -0.5 * jax.random.normal(sub_keys[12], (C_OUT, CLASSES), jnp.float32)
    vel_bias = 0.9 * step_scale * (global_rows * CLASSES) ** -0.5 * jax.random.normal(sub_keys[13], (CLASSES,), jnp.float32)
    learn_rate = jax.random.uniform(sub_keys[14], (), jnp.float32, 1.0, 4.0)
    return {'act_in': act_in, 'shortcut': shortcut, 'labels': labels, 'w_conv': w_conv, 'bn_gamma': bn_gamma, 'bn_beta': bn_beta, 'w_fc': w_fc, 'fc_bias': fc_bias, 'vel_conv': vel_conv, 'vel_gamma': vel_gamma, 'vel_beta': vel_beta, 'vel_fc': vel_fc, 'vel_bias': vel_bias, 'learn_rate': learn_rate}


def group_loss(params, act_grp, short_grp, label_grp):
    w_conv, bn_gamma, bn_beta, w_fc, fc_bias = params
    pos_count = B_DEV * SIDE * SIDE
    conv_out = jnp.dot(act_grp.reshape(pos_count, C_MID), w_conv.astype(jnp.bfloat16), preferred_element_type=jnp.float32)
    batch_mean = jnp.mean(conv_out, axis=0)
    centered = conv_out - batch_mean
    batch_var = jnp.mean(jnp.square(centered), axis=0)
    x_hat = centered * lax.rsqrt(batch_var + BN_EPS)
    activ = jax.nn.relu(x_hat * bn_gamma + bn_beta + short_grp.reshape(pos_count, C_OUT).astype(jnp.float32))
    pooled = jnp.mean(activ.reshape(B_DEV, SIDE * SIDE, C_OUT), axis=1)
    logits = jnp.dot(pooled.astype(jnp.bfloat16), w_fc.astype(jnp.bfloat16), preferred_element_type=jnp.float32) + fc_bias
    log_prob = jax.nn.log_softmax(logits, axis=-1)
    one_hot_lab = (label_grp[:, None] == jnp.arange(CLASSES)[None, :]).astype(jnp.float32)
    target = SMOOTHING / CLASSES + (1.0 - SMOOTHING) * one_hot_lab
    return -jnp.sum(target * log_prob)


def lars_update(weight, gradient, velocity, learn_rate):
    w_norm = jnp.sqrt(jnp.sum(jnp.square(weight)))
    g_norm = jnp.sqrt(jnp.sum(jnp.square(gradient)))
    trust = TRUST_COEF * w_norm / (g_norm + WEIGHT_DECAY * w_norm)
    new_vel = MOMENTUM * velocity + learn_rate * trust * (gradient + WEIGHT_DECAY * weight)
    return weight - new_vel, new_vel


def reference(act_in, shortcut, labels, w_conv, bn_gamma, bn_beta, w_fc, fc_bias, vel_conv, vel_gamma, vel_beta, vel_fc, vel_bias, learn_rate):
    params = (w_conv, bn_gamma, bn_beta, w_fc, fc_bias)
    grad_fn = jax.value_and_grad(group_loss)
    global_rows = DP * B_DEV

    def scan_body(carry, group_batch):
        loss_sum, grad_sum = carry
        loss_val, grads = grad_fn(params, group_batch[0], group_batch[1], group_batch[2])
        return (loss_sum + loss_val, jax.tree.map(jnp.add, grad_sum, grads)), None

    init_carry = (jnp.zeros((), jnp.float32), jax.tree.map(jnp.zeros_like, params))
    group_data = (act_in.reshape(DP, B_DEV, SIDE, SIDE, C_MID), shortcut.reshape(DP, B_DEV, SIDE, SIDE, C_OUT), labels.reshape(DP, B_DEV))
    (loss_sum, grad_sum), unused_out = lax.scan(scan_body, init_carry, group_data)
    g_conv, g_gamma, g_beta, g_fc, g_bias = [grad_part / global_rows for grad_part in grad_sum]
    conv_new, conv_vel_new = lars_update(w_conv, g_conv, vel_conv, learn_rate)
    fc_new, fc_vel_new = lars_update(w_fc, g_fc, vel_fc, learn_rate)
    gamma_vel_new = MOMENTUM * vel_gamma + learn_rate * g_gamma
    beta_vel_new = MOMENTUM * vel_beta + learn_rate * g_beta
    bias_vel_new = MOMENTUM * vel_bias + learn_rate * g_bias
    return (conv_new, bn_gamma - gamma_vel_new, bn_beta - beta_vel_new, fc_new, fc_bias - bias_vel_new, conv_vel_new, gamma_vel_new, beta_vel_new, fc_vel_new, bias_vel_new, loss_sum / global_rows)
```

```python
import functools
import jax, jax.numpy as jnp
from jax import lax
from jax.experimental import pallas as pl
from jax.experimental.pallas import tpu as pltpu

BN_EPS = 1e-5
IMG = 128
POS = 49
ROWS = IMG * POS
CIN = 1024
COUT = 2048
CB = 256
NB = COUT // CB
CH = 7
NCH = POS // CH
NT = 16
MS = 1


def fwd_kernel(a_ref, w_ref, s_ref, g_ref, b_ref, z_hbm, at_ref, pool_ref, cnt_ref, sx_ref, st_ref, zbuf, wbf, stat, zsem):
    j = pl.program_id(0)
    slot = lax.rem(j, 2)
    prev = 1 - slot

    def z_copy(jj, sl):
        return pltpu.make_async_copy(zbuf.at[sl], z_hbm.at[:, pl.ds(pl.multiple_of(jj * CB, CB), CB)], zsem.at[sl])

    @pl.when(j >= 2)
    def _():
        z_copy(j - 2, slot).wait()

    def step(do_mm, do_post):
        if do_mm:
            w = w_ref[...].astype(jnp.bfloat16)
            wbf[...] = w
            z0 = jnp.dot(a_ref[0:IMG, :], w, preferred_element_type=jnp.float32)
            m0 = jnp.sum(z0, axis=0, keepdims=True) * (1.0 / IMG)
            stat[0:8, :] = jnp.zeros((8, CB), jnp.float32)
            stat[8:16, :] = jnp.zeros((8, CB), jnp.float32)
        if do_post:
            mean = stat[16:17, :]
            inv = stat[17:18, :]
            gam = g_ref[...]
            sc = gam * inv
            sh = b_ref[...] - mean * sc
            sc_b = jnp.broadcast_to(sc, (8, CB))
            sh_b = jnp.broadcast_to(sh, (8, CB))
            pool_ref[...] = jnp.zeros_like(pool_ref)
            cnt_ref[...] = jnp.zeros_like(cnt_ref)
            sx_ref[...] = jnp.zeros_like(sx_ref)
            st_ref[...] = stat[16:24, :]

        def chunk(i, carry):
            base = pl.multiple_of(i * (CH * IMG), CH * IMG)
            if do_mm:
                for h in range(MS):
                    hr = pl.ds(base + h * (CH * IMG // MS), CH * IMG // MS)
                    zc = jnp.dot(a_ref[hr, :], wbf[...], preferred_element_type=jnp.float32)
                    zbuf[slot, hr, :] = zc
                    d = (zc - m0).reshape(CH * IMG // 8 // MS, 8, CB)
                    stat[0:8, :] += jnp.sum(d, axis=0)
                    stat[8:16, :] += jnp.sum(d * d, axis=0)
                at_ref[:, pl.ds(base, CH * IMG)] = a_ref[pl.ds(base, CH * IMG), pl.ds(pl.multiple_of(j * IMG, IMG), IMG)].astype(jnp.float32).T.astype(jnp.bfloat16)
            if do_post:
                for n in range(0, IMG, NT):
                    pa = pool_ref[n:n + NT, :]
                    ca = cnt_ref[n:n + NT, :]
                    xa = sx_ref[n:n + NT, :]
                    for p in range(CH):
                        zz = zbuf[prev, pl.ds(base + p * IMG + n, NT), :]
                        ss = s_ref[pl.ds(base + p * IMG + n, NT), :].astype(jnp.float32)
                        u = zz * sc + sh + ss
                        mk = u > 0
                        pa = pa + jnp.maximum(u, 0.0)
                        ca = ca + jnp.where(mk, 1.0, 0.0)
                        xa = xa + jnp.where(mk, zz, 0.0)
                    pool_ref[n:n + NT, :] = pa
                    cnt_ref[n:n + NT, :] = ca
                    sx_ref[n:n + NT, :] = xa
            return carry

        lax.fori_loop(0, NCH, chunk, 0)
        if do_post:
            pool_ref[...] = pool_ref[...] * (1.0 / POS)
            sx_ref[...] = (sx_ref[...] - mean * cnt_ref[...]) * inv
        if do_mm:
            dm = jnp.sum(stat[0:8, :], axis=0, keepdims=True) * (1.0 / ROWS)
            q = jnp.sum(stat[8:16, :], axis=0, keepdims=True) * (1.0 / ROWS)
            var = jnp.maximum(q - dm * dm, 0.0)
            stat[16:17, :] = m0 + dm
            stat[17:18, :] = lax.rsqrt(var + BN_EPS)
            z_copy(j, slot).start()

    @pl.when(j == 0)
    def _():
        step(True, False)

    @pl.when(jnp.logical_and(j > 0, j < NB))
    def _():
        step(True, True)

    @pl.when(j == NB)
    def _():
        step(False, True)
        z_copy(NB - 1, (NB - 1) % 2).wait()


def forward(a, w, s, gamma, beta):
    prev = lambda j: (0, jnp.maximum(j - 1, 0))
    cur = lambda j: (0, jnp.minimum(j, NB - 1))
    f32 = jnp.float32
    return pl.pallas_call(
        fwd_kernel,
        grid=(NB + 1,),
        in_specs=[
            pl.BlockSpec((ROWS, CIN), lambda j: (0, 0), pipeline_mode=pl.Buffered(1)),
            pl.BlockSpec((CIN, CB), cur),
            pl.BlockSpec((ROWS, CB), prev),
            pl.BlockSpec((1, CB), prev),
            pl.BlockSpec((1, CB), prev),
        ],
        out_specs=[
            pl.BlockSpec(memory_space=pl.ANY),
            pl.BlockSpec((IMG, ROWS), lambda j: (jnp.minimum(j, NB - 1), 0)),
            pl.BlockSpec((IMG, CB), prev),
            pl.BlockSpec((IMG, CB), prev),
            pl.BlockSpec((IMG, CB), prev),
            pl.BlockSpec((8, CB), prev),
        ],
        out_shape=[
            jax.ShapeDtypeStruct((ROWS, COUT), f32),
            jax.ShapeDtypeStruct((CIN, ROWS), jnp.bfloat16),
            jax.ShapeDtypeStruct((IMG, COUT), f32),
            jax.ShapeDtypeStruct((IMG, COUT), f32),
            jax.ShapeDtypeStruct((IMG, COUT), f32),
            jax.ShapeDtypeStruct((8, COUT), f32),
        ],
        scratch_shapes=[
            pltpu.VMEM((2, ROWS, CB), f32),
            pltpu.VMEM((CIN, CB), jnp.bfloat16),
            pltpu.VMEM((24, CB), f32),
            pltpu.SemaphoreType.DMA((2,)),
        ],
        compiler_params=pltpu.CompilerParams(vmem_limit_bytes=60 * 1024 * 1024),
        cost_estimate=pl.CostEstimate(flops=2 * ROWS * CIN * COUT, bytes_accessed=120_000_000, transcendentals=0),
        name="fwd_conv",
    )(a, w, s, gamma, beta)


def bwd_kernel(at_ref, z_ref, s_ref, sc_ref, sh_ref, bb_ref, cc_ref, da_ref, dw_ref, dz):
    j = pl.program_id(0)
    slot = lax.rem(j, 2)
    prev = 1 - slot

    def step(do_pre, do_mm):
        if do_pre:
            sc = sc_ref[...]
            sh = sh_ref[...]
            bb = bb_ref[...]
            cc = cc_ref[...]

        def pre(base, slabs):
            for n in range(0, IMG, NT):
                da = da_ref[n:n + NT, :]
                for p in range(slabs):
                    r = pl.ds(base + p * IMG + n, NT)
                    zz = z_ref[r, :]
                    u = zz * sc + sh + s_ref[r, :].astype(jnp.float32)
                    dz[slot, r, :] = (jnp.where(u > 0, da, 0.0) + (zz * cc + bb)).astype(jnp.bfloat16)

        def mm(base, size):
            return jnp.dot(at_ref[:, pl.ds(base, size)], dz[prev, pl.ds(base, size), :], preferred_element_type=jnp.float32)

        if do_mm:
            dw_ref[...] = mm(5376, 896)
        if do_pre:
            pre(5376, 7)

        def chunk(i, carry):
            base = pl.multiple_of(i * 1792, 1792)
            if do_mm:
                dw_ref[...] += mm(base, 1792)
            if do_pre:
                pre(base, 14)
            return carry
        lax.fori_loop(0, 3, chunk, 0)

    @pl.when(j == 0)
    def _():
        step(True, False)

    @pl.when(jnp.logical_and(j > 0, j < NB))
    def _():
        step(True, True)

    @pl.when(j == NB)
    def _():
        step(False, True)


def backward(at, z, s, sc, sh, bb, cc, da):
    prev = lambda j: (0, jnp.maximum(j - 1, 0))
    cur = lambda j: (0, jnp.minimum(j, NB - 1))
    row = pl.BlockSpec((1, CB), cur)
    return pl.pallas_call(
        bwd_kernel,
        grid=(NB + 1,),
        in_specs=[
            pl.BlockSpec((CIN, ROWS), lambda j: (0, 0), pipeline_mode=pl.Buffered(1)),
            pl.BlockSpec((ROWS, CB), cur),
            pl.BlockSpec((ROWS, CB), cur),
            row, row, row, row,
            pl.BlockSpec((IMG, CB), cur),
        ],
        out_specs=pl.BlockSpec((CIN, CB), prev),
        out_shape=jax.ShapeDtypeStruct((CIN, COUT), jnp.float32),
        scratch_shapes=[pltpu.VMEM((2, ROWS, CB), jnp.bfloat16)],
        compiler_params=pltpu.CompilerParams(vmem_limit_bytes=60 * 1024 * 1024),
        cost_estimate=pl.CostEstimate(flops=2 * ROWS * CIN * COUT, bytes_accessed=120_000_000, transcendentals=0),
        name="bwd_conv",
    )(at, z, s, sc, sh, bb, cc, da)
import jax
import jax.numpy as jnp
from jax.sharding import PartitionSpec as P

SMOOTHING = 0.1
MOMENTUM = 0.9
TRUST_COEF = 0.001
WEIGHT_DECAY = 5e-5


def lars_update(weight, gradient, velocity, learn_rate):
    w_norm = jnp.sqrt(jnp.sum(jnp.square(weight)))
    g_norm = jnp.sqrt(jnp.sum(jnp.square(gradient)))
    trust = TRUST_COEF * w_norm / (g_norm + WEIGHT_DECAY * w_norm)
    new_vel = MOMENTUM * velocity + learn_rate * trust * (gradient + WEIGHT_DECAY * weight)
    return weight - new_vel, new_vel


def head(pooled, labels, w_fc_t, fc_bias, total):
    bf = jnp.bfloat16
    f32 = jnp.float32
    classes = w_fc_t.shape[0]
    pb = pooled.astype(bf)
    wb = w_fc_t.astype(bf)
    logits = jnp.einsum('nc,kc->nk', pb, wb, preferred_element_type=f32) + fc_bias
    log_prob = jax.nn.log_softmax(logits, axis=-1)
    one_hot = (labels[:, None] == jnp.arange(classes, dtype=jnp.int32)[None, :]).astype(f32)
    target = SMOOTHING / classes + (1.0 - SMOOTHING) * one_hot
    loss = -jnp.sum(target * log_prob) / total
    dl = (jnp.exp(log_prob) - target) / total
    return pb, wb, dl, dl.astype(bf), loss


def solution(mesh):
    groups = mesh.shape['dp']

    def local_step(act_in, shortcut, labels, w_conv, gamma, beta, w_fc, fc_bias, vel_conv, vel_gamma, vel_beta, vel_fc, vel_bias, lr):
        f32 = jnp.float32
        total = IMG * groups
        a = act_in.transpose(1, 2, 0, 3).reshape(ROWS, CIN)
        s = shortcut.transpose(1, 2, 0, 3).reshape(ROWS, COUT)
        w_fc_t = w_fc.T
        z, at, pooled, cnt, sx, st = forward(a, w_conv, s, gamma[None], beta[None])
        pb, wb, dl, dlb, loss = head(pooled, labels, w_fc_t, fc_bias, total)
        dpool = jnp.einsum('nk,kc->nc', dlb, wb, preferred_element_type=f32) / POS
        mean = st[0:1]
        inv = st[1:2]
        gam = gamma[None]
        d_beta = jnp.sum(dpool * cnt, axis=0, keepdims=True)
        d_gamma = jnp.sum(dpool * sx, axis=0, keepdims=True)
        sc = gam * inv
        sh = beta[None] - mean * sc
        cc = -(sc * inv) * (d_gamma / ROWS)
        bb = -sc * (d_beta / ROWS) - mean * cc
        dw = backward(at, z, s, sc, sh, bb, cc, dpool * sc)
        g_fc_t = jnp.einsum('nk,nc->kc', dlb, pb, preferred_element_type=f32)
        g_bias = jnp.sum(dl, axis=0)
        g_conv, g_gamma, g_beta, g_fc_t, g_bias, loss = lax.psum((dw, d_gamma[0], d_beta[0], g_fc_t, g_bias, loss), 'dp')
        conv_new, conv_vel_new = lars_update(w_conv, g_conv, vel_conv, lr)
        fc_new, fc_vel_new = lars_update(w_fc_t, g_fc_t, vel_fc.T, lr)
        gv = MOMENTUM * vel_gamma + lr * g_gamma
        bv = MOMENTUM * vel_beta + lr * g_beta
        cv = MOMENTUM * vel_bias + lr * g_bias
        return (conv_new, gamma - gv, beta - bv, fc_new.T, fc_bias - cv, conv_vel_new, gv, bv, fc_vel_new.T, cv, loss)

    return jax.shard_map(local_step, mesh=mesh, in_specs=(P('dp'),) * 3 + (P(),) * 11, out_specs=(P(),) * 11, check_vma=False)
```

```python
import functools
import jax, jax.numpy as jnp
from jax import lax
from jax.experimental import pallas as pl
from jax.experimental.pallas import tpu as pltpu

BN_EPS = 1e-5
IMG = 128
POS = 49
ROWS = IMG * POS
CIN = 1024
COUT = 2048
CB = 256
NB = COUT // CB
CH = 7
NCH = POS // CH
NT = 16
MS = 1

MESH = pl.DeviceIdType.MESH
TAIL = 3


def position():
    me = lax.axis_index('dp')
    core = lax.rem(me, 2)
    x = lax.rem(me // 2, 2)
    y = me // 4
    return me, core, x, y


def dev(core, x, y):
    return (y * 2 + x) * 2 + core


def enter_all():
    me = lax.axis_index('dp')
    bar = pltpu.get_barrier_semaphore()
    for k in range(1, 8):
        pl.semaphore_signal(bar, inc=1, device_id=(lax.rem(me + k, 8),), device_id_type=MESH)
    pl.semaphore_wait(bar, 7)


def rcopy(src, dst, send, recv, target):
    return pltpu.make_async_remote_copy(src_ref=src, dst_ref=dst, send_sem=send, recv_sem=recv, device_id=(target,), device_id_type=MESH)


def gather_copies(buf, send, recv, b):
    me, core, x, y = position()
    ca = pl.ds(pl.multiple_of(b * CB, CB), CB // 2)
    cb = pl.ds(pl.multiple_of(b * CB + CB // 2, CB // 2), CB // 2)
    cc = pl.ds(pl.multiple_of(b * CB, CB), CB)
    xn, yn, pn = dev(core, 1 - x, y), dev(core, x, 1 - y), dev(1 - core, x, y)
    def cp(k, ref, target):
        return rcopy(ref, ref, send.at[k, b], recv.at[k, b], target)
    return (cp(0, buf.at[core, y, x, :, ca], yn), cp(1, buf.at[core, y, x, :, cb], xn),
            cp(2, buf.at[core, :, x, :, ca], xn), cp(3, buf.at[core, y, :, :, cb], yn),
            cp(4, buf.at[core, :, :, :, cc], pn))


def when_block(b, fn):
    @pl.when(jnp.logical_and(b >= 0, b < NB))
    def _():
        fn(b)


def fwd_kernel(a_ref, w_ref, s_ref, g_ref, b_ref, lab_ref, z_hbm, at_ref, pool_ref, cnt_ref, sx_ref, st_ref, pall_ref, lall_ref, zbuf, wbf, stat, pfull, lfull, zsem, gs, gr, ls, lr):
    j = pl.program_id(0)
    slot = lax.rem(j, 2)
    prev = 1 - slot

    def z_copy(jj, sl):
        return pltpu.make_async_copy(zbuf.at[sl], z_hbm.at[:, pl.ds(pl.multiple_of(jj * CB, CB), CB)], zsem.at[sl])

    me, core, x, y = position()

    def label_copy(k):
        return rcopy(lab_ref, lfull.at[core, y, x], ls.at[k], lr.at[k], lax.rem(me + k, 8))

    @pl.when(j == 0)
    def _():
        enter_all()
        for k in range(1, 8):
            label_copy(k).start()
        lfull[core, y, x] = lab_ref[...]

    def second(b):
        c = gather_copies(pfull, gs, gr, b)
        c[0].wait_recv()
        c[1].wait_recv()
        c[2].start()
        c[3].start()

    def third(b):
        c = gather_copies(pfull, gs, gr, b)
        c[2].wait_recv()
        c[3].wait_recv()
        c[4].start()

    def last(b):
        gather_copies(pfull, gs, gr, b)[4].wait_recv()
        for q in range(8):
            pall_ref[q * IMG:(q + 1) * IMG, :] = pfull[q // 4, (q // 2) % 2, q % 2, :, pl.ds(pl.multiple_of(b * CB, CB), CB)].astype(jnp.bfloat16)

    when_block(j - 2, second)
    when_block(j - 3, third)
    when_block(j - 4, last)

    @pl.when(jnp.logical_and(j >= 2, j < NB + 2))
    def _():
        z_copy(j - 2, slot).wait()

    def step(do_mm, do_post):
        if do_mm:
            w = w_ref[...].astype(jnp.bfloat16)
            wbf[...] = w
            z0 = jnp.dot(a_ref[0:IMG, :], w, preferred_element_type=jnp.float32)
            m0 = jnp.sum(z0, axis=0, keepdims=True) * (1.0 / IMG)
            stat[0:8, :] = jnp.zeros((8, CB), jnp.float32)
            stat[8:16, :] = jnp.zeros((8, CB), jnp.float32)
        if do_post:
            mean = stat[16:17, :]
            inv = stat[17:18, :]
            gam = g_ref[...]
            sc = gam * inv
            sh = b_ref[...] - mean * sc
            sc_b = jnp.broadcast_to(sc, (8, CB))
            sh_b = jnp.broadcast_to(sh, (8, CB))
            pool_ref[...] = jnp.zeros_like(pool_ref)
            cnt_ref[...] = jnp.zeros_like(cnt_ref)
            sx_ref[...] = jnp.zeros_like(sx_ref)
            st_ref[...] = stat[16:24, :]

        def chunk(i, carry):
            base = pl.multiple_of(i * (CH * IMG), CH * IMG)
            if do_mm:
                for h in range(MS):
                    hr = pl.ds(base + h * (CH * IMG // MS), CH * IMG // MS)
                    zc = jnp.dot(a_ref[hr, :], wbf[...], preferred_element_type=jnp.float32)
                    zbuf[slot, hr, :] = zc
                    d = (zc - m0).reshape(CH * IMG // 8 // MS, 8, CB)
                    stat[0:8, :] += jnp.sum(d, axis=0)
                    stat[8:16, :] += jnp.sum(d * d, axis=0)
                at_ref[:, pl.ds(base, CH * IMG)] = a_ref[pl.ds(base, CH * IMG), pl.ds(pl.multiple_of(j * IMG, IMG), IMG)].astype(jnp.float32).T.astype(jnp.bfloat16)
            if do_post:
                for n in range(0, IMG, NT):
                    pa = pool_ref[n:n + NT, :]
                    ca = cnt_ref[n:n + NT, :]
                    xa = sx_ref[n:n + NT, :]
                    for p in range(CH):
                        zz = zbuf[prev, pl.ds(base + p * IMG + n, NT), :]
                        ss = s_ref[pl.ds(base + p * IMG + n, NT), :].astype(jnp.float32)
                        u = zz * sc + sh + ss
                        mk = u > 0
                        pa = pa + jnp.maximum(u, 0.0)
                        ca = ca + jnp.where(mk, 1.0, 0.0)
                        xa = xa + jnp.where(mk, zz, 0.0)
                    pool_ref[n:n + NT, :] = pa
                    cnt_ref[n:n + NT, :] = ca
                    sx_ref[n:n + NT, :] = xa
            return carry

        lax.fori_loop(0, NCH, chunk, 0)
        if do_post:
            pooled = pool_ref[...] * (1.0 / POS)
            pool_ref[...] = pooled
            pfull[core, y, x, :, pl.ds(pl.multiple_of((j - 1) * CB, CB), CB)] = pooled
            c = gather_copies(pfull, gs, gr, j - 1)
            c[0].start()
            c[1].start()
            sx_ref[...] = (sx_ref[...] - mean * cnt_ref[...]) * inv
        if do_mm:
            dm = jnp.sum(stat[0:8, :], axis=0, keepdims=True) * (1.0 / ROWS)
            q = jnp.sum(stat[8:16, :], axis=0, keepdims=True) * (1.0 / ROWS)
            var = jnp.maximum(q - dm * dm, 0.0)
            stat[16:17, :] = m0 + dm
            stat[17:18, :] = lax.rsqrt(var + BN_EPS)
            z_copy(j, slot).start()

    @pl.when(j == 0)
    def _():
        step(True, False)

    @pl.when(jnp.logical_and(j > 0, j < NB))
    def _():
        step(True, True)

    @pl.when(j == NB)
    def _():
        step(False, True)

    @pl.when(j == NB + TAIL)
    def _():
        for k in range(1, 8):
            label_copy(k).wait()
        lall_ref[...] = lfull[...]

        def drain(b, carry):
            for c in gather_copies(pfull, gs, gr, b):
                c.wait_send()
            return carry
        lax.fori_loop(0, NB, drain, 0)


def forward(a, w, s, gamma, beta, labels):
    prev = lambda j: (0, jnp.clip(j - 1, 0, NB - 1))
    late = lambda j: (0, jnp.clip(j - 4, 0, NB - 1))
    cur = lambda j: (0, jnp.minimum(j, NB - 1))
    f32 = jnp.float32
    return pl.pallas_call(
        fwd_kernel,
        grid=(NB + 1 + TAIL,),
        in_specs=[
            pl.BlockSpec((ROWS, CIN), lambda j: (0, 0), pipeline_mode=pl.Buffered(1)),
            pl.BlockSpec((CIN, CB), cur),
            pl.BlockSpec((ROWS, CB), prev),
            pl.BlockSpec((1, CB), prev),
            pl.BlockSpec((1, CB), prev),
            pl.BlockSpec((8, IMG), lambda j: (0, 0)),
        ],
        out_specs=[
            pl.BlockSpec(memory_space=pl.ANY),
            pl.BlockSpec((IMG, ROWS), lambda j: (jnp.minimum(j, NB - 1), 0)),
            pl.BlockSpec((IMG, CB), prev),
            pl.BlockSpec((IMG, CB), prev),
            pl.BlockSpec((IMG, CB), prev),
            pl.BlockSpec((8, CB), prev),
            pl.BlockSpec((8 * IMG, CB), late),
            pl.BlockSpec((2, 2, 2, 8, IMG), lambda j: (0, 0, 0, 0, 0)),
        ],
        out_shape=[
            jax.ShapeDtypeStruct((ROWS, COUT), f32),
            jax.ShapeDtypeStruct((CIN, ROWS), jnp.bfloat16),
            jax.ShapeDtypeStruct((IMG, COUT), f32),
            jax.ShapeDtypeStruct((IMG, COUT), f32),
            jax.ShapeDtypeStruct((IMG, COUT), f32),
            jax.ShapeDtypeStruct((8, COUT), f32),
            jax.ShapeDtypeStruct((8 * IMG, COUT), jnp.bfloat16),
            jax.ShapeDtypeStruct((2, 2, 2, 8, IMG), jnp.int32),
        ],
        scratch_shapes=[
            pltpu.VMEM((2, ROWS, CB), f32),
            pltpu.VMEM((CIN, CB), jnp.bfloat16),
            pltpu.VMEM((24, CB), f32),
            pltpu.VMEM((2, 2, 2, IMG, COUT), f32),
            pltpu.VMEM((2, 2, 2, 8, IMG), jnp.int32),
            pltpu.SemaphoreType.DMA((2,)),
            pltpu.SemaphoreType.DMA((5, NB)),
            pltpu.SemaphoreType.DMA((5, NB)),
            pltpu.SemaphoreType.DMA((8,)),
            pltpu.SemaphoreType.DMA((8,)),
        ],
        compiler_params=pltpu.CompilerParams(vmem_limit_bytes=60 * 1024 * 1024, collective_id=0, has_side_effects=True),
        cost_estimate=pl.CostEstimate(flops=2 * ROWS * CIN * COUT, bytes_accessed=120_000_000, transcendentals=0),
        name="fwd_conv",
    )(a, w, s, gamma, beta, labels)


BTAIL = 7
QR = CIN // 8


def bwd_kernel(at_ref, z_ref, s_ref, sc_ref, sh_ref, bb_ref, cc_ref, da_ref, db_ref, g_hbm, dbo_ref,
               dz, dw, rd, ha, hb, ra, rb, ka, kb, r2a, r2b, gfull, dball, ss, rs, gs, gr, bs, br, osem):
    j = pl.program_id(0)
    slot = lax.rem(j, 2)
    prev = 1 - slot
    me, core, x, y = position()
    xn, yn, pn = dev(core, 1 - x, y), dev(core, x, 1 - y), dev(1 - core, x, y)
    half = CIN // 2
    HC = CB // 2

    def db_copy(k):
        return rcopy(db_ref, dball.at[me], bs.at[k], br.at[k], lax.rem(me + k, 8))

    @pl.when(j == 0)
    def _():
        enter_all()
        for k in range(1, 8):
            db_copy(k).start()
        dball[me] = db_ref[...]

    def out_copy(b):
        cc = pl.ds(pl.multiple_of(b * CB, CB), CB)
        return pltpu.make_async_copy(gfull.at[:, :, :, :, cc], g_hbm.at[:, :, :, :, cc], osem.at[b])

    def core_copy(b):
        return rcopy(dw.at[lax.rem(b, 2), pl.ds(pl.multiple_of((1 - core) * half, half), half), :], rd.at[b], ss.at[0, b], rs.at[0, b], pn)

    def first_copies(b):
        sl = lax.rem(b, 2)
        return (rcopy(ha.at[sl, 1 - x], ra.at[b], ss.at[1, b], rs.at[1, b], xn),
                rcopy(hb.at[sl, 1 - y], rb.at[b], ss.at[2, b], rs.at[2, b], yn))

    def second_copies(b):
        sl = lax.rem(b, 2)
        return (rcopy(ka.at[sl, 1 - y], r2a.at[b], ss.at[3, b], rs.at[3, b], yn),
                rcopy(kb.at[sl, 1 - x], r2b.at[b], ss.at[4, b], rs.at[4, b], xn))

    def stage1(b):
        c = core_copy(b)
        c.wait()
        sl = lax.rem(b, 2)
        for py in range(2):
            for px in range(2):
                q = py * 2 + px
                own = pl.ds(pl.multiple_of(core * half + q * QR, QR), QR)
                ha[sl, px, py] = dw[sl, own, 0:HC] + rd[b, q * QR:(q + 1) * QR, 0:HC]
                hb[sl, py, px] = dw[sl, own, HC:CB] + rd[b, q * QR:(q + 1) * QR, HC:CB]
        for f in first_copies(b):
            f.start()

    def stage2(b):
        sl = lax.rem(b, 2)
        for f in first_copies(b):
            f.wait()
        for k in range(2):
            ka[sl, k] = ha[sl, x, k] + ra[b, k]
            kb[sl, k] = hb[sl, y, k] + rb[b, k]
        for f in second_copies(b):
            f.start()

    def stage3(b):
        sl = lax.rem(b, 2)
        for f in second_copies(b):
            f.wait()
        gfull[core, y, x, :, pl.ds(pl.multiple_of(b * CB, CB), HC)] = ka[sl, y] + r2a[b]
        gfull[core, y, x, :, pl.ds(pl.multiple_of(b * CB + HC, HC), HC)] = kb[sl, x] + r2b[b]
        c = gather_copies(gfull, gs, gr, b)
        c[0].start()
        c[1].start()

    def stage4(b):
        c = gather_copies(gfull, gs, gr, b)
        c[0].wait_recv()
        c[1].wait_recv()
        c[2].start()
        c[3].start()

    def stage5(b):
        c = gather_copies(gfull, gs, gr, b)
        c[2].wait_recv()
        c[3].wait_recv()
        c[4].start()

    def stage6(b):
        gather_copies(gfull, gs, gr, b)[4].wait_recv()
        out_copy(b).start()

    when_block(j - 2, stage1)
    when_block(j - 3, stage2)
    when_block(j - 4, stage3)
    when_block(j - 5, stage4)
    when_block(j - 6, stage5)
    when_block(j - 7, stage6)

    def step(do_pre, do_mm):
        if do_pre:
            sc = sc_ref[...]
            sh = sh_ref[...]
            bb = bb_ref[...]
            cc = cc_ref[...]

        def pre(base, slabs):
            for n in range(0, IMG, NT):
                da = da_ref[n:n + NT, :]
                for p in range(slabs):
                    r = pl.ds(base + p * IMG + n, NT)
                    zz = z_ref[r, :]
                    u = zz * sc + sh + s_ref[r, :].astype(jnp.float32)
                    dz[slot, r, :] = (jnp.where(u > 0, da, 0.0) + (zz * cc + bb)).astype(jnp.bfloat16)

        def mm(base, size):
            return jnp.dot(at_ref[:, pl.ds(base, size)], dz[prev, pl.ds(base, size), :], preferred_element_type=jnp.float32)

        if do_mm:
            dw[prev] = mm(5376, 896)
        if do_pre:
            pre(5376, 7)

        def chunk(i, carry):
            base = pl.multiple_of(i * 1792, 1792)
            if do_mm:
                dw[prev] += mm(base, 1792)
            if do_pre:
                pre(base, 14)
            return carry
        lax.fori_loop(0, 3, chunk, 0)
        if do_mm:
            core_copy(j - 1).start()

    @pl.when(j == 0)
    def _():
        step(True, False)

    @pl.when(jnp.logical_and(j > 0, j < NB))
    def _():
        step(True, True)

    @pl.when(j == NB)
    def _():
        step(False, True)

    @pl.when(j == NB + BTAIL - 1)
    def _():
        for k in range(1, 8):
            db_copy(k).wait()
        acc = dball[0]
        for k in range(1, 8):
            acc = acc + dball[k]
        dbo_ref[...] = acc

        def drain(b, carry):
            for c in gather_copies(gfull, gs, gr, b):
                c.wait_send()
            out_copy(b).wait()
            return carry
        lax.fori_loop(0, NB, drain, 0)


def backward(at, z, s, sc, sh, bb, cc, da, dgb):
    f32 = jnp.float32
    cur = lambda j: (0, jnp.minimum(j, NB - 1))
    row = pl.BlockSpec((1, CB), cur)
    return pl.pallas_call(
        bwd_kernel,
        grid=(NB + BTAIL,),
        in_specs=[
            pl.BlockSpec((CIN, ROWS), lambda j: (0, 0), pipeline_mode=pl.Buffered(1)),
            pl.BlockSpec((ROWS, CB), cur),
            pl.BlockSpec((ROWS, CB), cur),
            row, row, row, row,
            pl.BlockSpec((IMG, CB), cur),
            pl.BlockSpec((16, CB), lambda j: (0, 0)),
        ],
        out_specs=[pl.BlockSpec(memory_space=pl.ANY), pl.BlockSpec((16, CB), lambda j: (0, 0))],
        out_shape=[jax.ShapeDtypeStruct((2, 2, 2, QR, COUT), f32), jax.ShapeDtypeStruct((16, CB), f32)],
        scratch_shapes=[
            pltpu.VMEM((2, ROWS, CB), jnp.bfloat16),
            pltpu.VMEM((2, CIN, CB), f32),
            pltpu.VMEM((NB, CIN // 2, CB), f32),
            pltpu.VMEM((2, 2, 2, QR, CB // 2), f32),
            pltpu.VMEM((2, 2, 2, QR, CB // 2), f32),
            pltpu.VMEM((NB, 2, QR, CB // 2), f32),
            pltpu.VMEM((NB, 2, QR, CB // 2), f32),
            pltpu.VMEM((2, 2, QR, CB // 2), f32),
            pltpu.VMEM((2, 2, QR, CB // 2), f32),
            pltpu.VMEM((NB, QR, CB // 2), f32),
            pltpu.VMEM((NB, QR, CB // 2), f32),
            pltpu.VMEM((2, 2, 2, QR, COUT), f32),
            pltpu.VMEM((8, 16, CB), f32),
            pltpu.SemaphoreType.DMA((5, NB)),
            pltpu.SemaphoreType.DMA((5, NB)),
            pltpu.SemaphoreType.DMA((5, NB)),
            pltpu.SemaphoreType.DMA((5, NB)),
            pltpu.SemaphoreType.DMA((8,)),
            pltpu.SemaphoreType.DMA((8,)),
            pltpu.SemaphoreType.DMA((NB,)),
        ],
        compiler_params=pltpu.CompilerParams(vmem_limit_bytes=63 * 1024 * 1024, collective_id=1, has_side_effects=True),
        cost_estimate=pl.CostEstimate(flops=2 * ROWS * CIN * COUT, bytes_accessed=120_000_000, transcendentals=0),
        name="bwd_conv",
    )(at, z, s, sc, sh, bb, cc, da, dgb)
import jax
import jax.numpy as jnp
from jax.sharding import PartitionSpec as P

SMOOTHING = 0.1
MOMENTUM = 0.9
TRUST_COEF = 0.001
WEIGHT_DECAY = 5e-5


def lars_update(weight, gradient, velocity, learn_rate):
    w_norm = jnp.sqrt(jnp.sum(jnp.square(weight)))
    g_norm = jnp.sqrt(jnp.sum(jnp.square(gradient)))
    trust = TRUST_COEF * w_norm / (g_norm + WEIGHT_DECAY * w_norm)
    new_vel = MOMENTUM * velocity + learn_rate * trust * (gradient + WEIGHT_DECAY * weight)
    return weight - new_vel, new_vel


def head(pb, labels, w_fc_t, fc_bias, total):
    bf = jnp.bfloat16
    f32 = jnp.float32
    classes = w_fc_t.shape[0]
    wb = w_fc_t.astype(bf)
    logits = jnp.einsum('nc,kc->nk', pb, wb, preferred_element_type=f32) + fc_bias
    log_prob = jax.nn.log_softmax(logits, axis=-1)
    one_hot = (labels[:, None] == jnp.arange(classes, dtype=jnp.int32)[None, :]).astype(f32)
    target = SMOOTHING / classes + (1.0 - SMOOTHING) * one_hot
    loss = -jnp.sum(target * log_prob) / total
    dl = (jnp.exp(log_prob) - target) / total
    return pb, wb, dl, dl.astype(bf), loss


def solution(mesh):
    groups = mesh.shape['dp']

    def local_step(act_in, shortcut, labels, w_conv, gamma, beta, w_fc, fc_bias, vel_conv, vel_gamma, vel_beta, vel_fc, vel_bias, lr):
        f32 = jnp.float32
        total = IMG * groups
        a = act_in.transpose(1, 2, 0, 3).reshape(ROWS, CIN)
        s = shortcut.transpose(1, 2, 0, 3).reshape(ROWS, COUT)
        w_fc_t = w_fc.T
        lab8 = jnp.broadcast_to(labels[None], (8, IMG))
        z, at, pooled, cnt, sx, st, pall, lall = forward(a, w_conv, s, gamma[None], beta[None], lab8)
        _, wb, _, dlb, _ = head(pooled.astype(jnp.bfloat16), labels, w_fc_t, fc_bias, total)
        dpool = jnp.einsum('nk,kc->nc', dlb, wb, preferred_element_type=f32) / POS
        mean = st[0:1]
        inv = st[1:2]
        gam = gamma[None]
        d_beta = jnp.sum(dpool * cnt, axis=0, keepdims=True)
        d_gamma = jnp.sum(dpool * sx, axis=0, keepdims=True)
        sc = gam * inv
        sh = beta[None] - mean * sc
        cc = -(sc * inv) * (d_gamma / ROWS)
        bb = -sc * (d_beta / ROWS) - mean * cc
        dgb = jnp.concatenate([d_gamma.reshape(8, CB), d_beta.reshape(8, CB)])
        g8, dgb = backward(at, z, s, sc, sh, bb, cc, dpool * sc, dgb)
        g_conv = g8.reshape(CIN, COUT)
        g_gamma = dgb[0:8].reshape(COUT)
        g_beta = dgb[8:16].reshape(COUT)
        _, _, dl, dlb, loss = head(pall, lall[:, :, :, 0].reshape(total), w_fc_t, fc_bias, total)
        g_fc_t = jnp.einsum('nk,nc->kc', dlb, pall, preferred_element_type=f32)
        g_bias = jnp.sum(dl, axis=0)
        conv_new, conv_vel_new = lars_update(w_conv, g_conv, vel_conv, lr)
        fc_new, fc_vel_new = lars_update(w_fc_t, g_fc_t, vel_fc.T, lr)
        gv = MOMENTUM * vel_gamma + lr * g_gamma
        bv = MOMENTUM * vel_beta + lr * g_beta
        cv = MOMENTUM * vel_bias + lr * g_bias
        return (conv_new, gamma - gv, beta - bv, fc_new.T, fc_bias - cv, conv_vel_new, gv, bv, fc_vel_new.T, cv, loss)

    return jax.shard_map(local_step, mesh=mesh, in_specs=(P('dp'),) * 3 + (P(),) * 11, out_specs=(P(),) * 11, check_vma=False)
```

```python
import functools
import jax, jax.numpy as jnp
from jax import lax
from jax.experimental import pallas as pl
from jax.experimental.pallas import tpu as pltpu

BN_EPS = 1e-5
IMG = 128
POS = 49
ROWS = IMG * POS
CIN = 1024
COUT = 2048
CB = 256
NB = COUT // CB
CH = 7
NCH = POS // CH
NT = 16
MS = 1

MESH = pl.DeviceIdType.MESH
TAIL = 3


def position():
    me = lax.axis_index('dp')
    core = lax.rem(me, 2)
    x = lax.rem(me // 2, 2)
    y = me // 4
    return me, core, x, y


def dev(core, x, y):
    return (y * 2 + x) * 2 + core


def enter_all():
    me = lax.axis_index('dp')
    bar = pltpu.get_barrier_semaphore()
    for k in range(1, 8):
        pl.semaphore_signal(bar, inc=1, device_id=(lax.rem(me + k, 8),), device_id_type=MESH)
    pl.semaphore_wait(bar, 7)


def rcopy(src, dst, send, recv, target):
    return pltpu.make_async_remote_copy(src_ref=src, dst_ref=dst, send_sem=send, recv_sem=recv, device_id=(target,), device_id_type=MESH)


def gather_copies(buf, send, recv, b):
    me, core, x, y = position()
    ca = pl.ds(pl.multiple_of(b * CB, CB), CB // 2)
    cb = pl.ds(pl.multiple_of(b * CB + CB // 2, CB // 2), CB // 2)
    cc = pl.ds(pl.multiple_of(b * CB, CB), CB)
    xn, yn, pn = dev(core, 1 - x, y), dev(core, x, 1 - y), dev(1 - core, x, y)
    def cp(k, ref, target):
        return rcopy(ref, ref, send.at[k, b], recv.at[k, b], target)
    return (cp(0, buf.at[core, y, x, :, ca], yn), cp(1, buf.at[core, y, x, :, cb], xn),
            cp(2, buf.at[core, :, x, :, ca], xn), cp(3, buf.at[core, y, :, :, cb], yn),
            cp(4, buf.at[core, :, :, :, cc], pn))


def when_block(b, fn):
    @pl.when(jnp.logical_and(b >= 0, b < NB))
    def _():
        fn(b)


def fwd_kernel(a_ref, w_ref, s_ref, g_ref, b_ref, lab_ref, z_hbm, at_ref, pool_ref, cnt_ref, sx_ref, st_ref, pall_ref, lall_ref, wsq_ref, zbuf, wbf, stat, pfull, lfull, zsem, gs, gr, ls, lr):
    j = pl.program_id(0)
    slot = lax.rem(j, 2)
    prev = 1 - slot

    def z_copy(jj, sl):
        return pltpu.make_async_copy(zbuf.at[sl], z_hbm.at[jj], zsem.at[sl])

    me, core, x, y = position()

    def label_copy(k):
        return rcopy(lab_ref, lfull.at[core, y, x], ls.at[k], lr.at[k], lax.rem(me + k, 8))

    @pl.when(j == 0)
    def _():
        enter_all()
        for k in range(1, 8):
            label_copy(k).start()
        lfull[core, y, x] = lab_ref[...]
        wsq_ref[...] = jnp.zeros_like(wsq_ref)

    def second(b):
        c = gather_copies(pfull, gs, gr, b)
        c[0].wait_recv()
        c[1].wait_recv()
        c[2].start()
        c[3].start()

    def third(b):
        c = gather_copies(pfull, gs, gr, b)
        c[2].wait_recv()
        c[3].wait_recv()
        c[4].start()

    def last(b):
        gather_copies(pfull, gs, gr, b)[4].wait_recv()
        for q in range(8):
            pall_ref[q * IMG:(q + 1) * IMG, :] = pfull[q // 4, (q // 2) % 2, q % 2, :, pl.ds(pl.multiple_of(b * CB, CB), CB)].astype(jnp.bfloat16)

    def stages():
        when_block(j - 2, second)
        when_block(j - 3, third)
        when_block(j - 4, last)

    pl.when(j > NB)(stages)

    @pl.when(jnp.logical_and(j >= 2, j < NB + 2))
    def _():
        z_copy(j - 2, slot).wait()

    def step(do_mm, do_post):
        if do_mm:
            wf = w_ref[...]
            wsq_ref[...] += jnp.sum((wf * wf).reshape(CIN // 8, 8, CB), axis=0)
            w = wf.astype(jnp.bfloat16)
            wbf[...] = w
            z0 = jnp.dot(a_ref[0:IMG, :], w, preferred_element_type=jnp.float32)
            m0 = jnp.sum(z0, axis=0, keepdims=True) * (1.0 / IMG)
            stat[0:8, :] = jnp.zeros((8, CB), jnp.float32)
            stat[8:16, :] = jnp.zeros((8, CB), jnp.float32)
        if do_post:
            mean = stat[16:17, :]
            inv = stat[17:18, :]
            gam = g_ref[...]
            sc = gam * inv
            sh = b_ref[...] - mean * sc
            sc_b = jnp.broadcast_to(sc, (8, CB))
            sh_b = jnp.broadcast_to(sh, (8, CB))
            pool_ref[...] = jnp.zeros_like(pool_ref)
            cnt_ref[...] = jnp.zeros_like(cnt_ref)
            sx_ref[...] = jnp.zeros_like(sx_ref)
            st_ref[...] = stat[16:24, :]

        def chunk(i, carry):
            base = pl.multiple_of(i * (CH * IMG), CH * IMG)
            if do_post:
                pl.when(i == 4)(stages)
            if do_mm:
                for h in range(MS):
                    hr = pl.ds(base + h * (CH * IMG // MS), CH * IMG // MS)
                    zc = jnp.dot(a_ref[hr, :], wbf[...], preferred_element_type=jnp.float32)
                    zbuf[slot, hr, :] = zc
                    d = (zc - m0).reshape(CH * IMG // 8 // MS, 8, CB)
                    stat[0:8, :] += jnp.sum(d, axis=0)
                    stat[8:16, :] += jnp.sum(d * d, axis=0)
                at_ref[:, pl.ds(base, CH * IMG)] = a_ref[pl.ds(base, CH * IMG), pl.ds(pl.multiple_of(j * IMG, IMG), IMG)].astype(jnp.float32).T.astype(jnp.bfloat16)
            if do_post:
                for n in range(0, IMG, NT):
                    pa = pool_ref[n:n + NT, :]
                    ca = cnt_ref[n:n + NT, :]
                    xa = sx_ref[n:n + NT, :]
                    for p in range(CH):
                        zz = zbuf[prev, pl.ds(base + p * IMG + n, NT), :]
                        ss = s_ref[pl.ds(base + p * IMG + n, NT), :].astype(jnp.float32)
                        u = zz * sc + sh + ss
                        mk = u > 0
                        pa = pa + jnp.maximum(u, 0.0)
                        ca = ca + jnp.where(mk, 1.0, 0.0)
                        xa = xa + jnp.where(mk, zz, 0.0)
                    pool_ref[n:n + NT, :] = pa
                    cnt_ref[n:n + NT, :] = ca
                    sx_ref[n:n + NT, :] = xa
            return carry

        lax.fori_loop(0, NCH, chunk, 0)
        if do_post:
            pooled = pool_ref[...] * (1.0 / POS)
            pool_ref[...] = pooled
            pfull[core, y, x, :, pl.ds(pl.multiple_of((j - 1) * CB, CB), CB)] = pooled
            c = gather_copies(pfull, gs, gr, j - 1)
            c[0].start()
            c[1].start()
            sx_ref[...] = (sx_ref[...] - mean * cnt_ref[...]) * inv
        if do_mm:
            dm = jnp.sum(stat[0:8, :], axis=0, keepdims=True) * (1.0 / ROWS)
            q = jnp.sum(stat[8:16, :], axis=0, keepdims=True) * (1.0 / ROWS)
            var = jnp.maximum(q - dm * dm, 0.0)
            stat[16:17, :] = m0 + dm
            stat[17:18, :] = lax.rsqrt(var + BN_EPS)
            z_copy(j, slot).start()

    @pl.when(j == 0)
    def _():
        step(True, False)

    @pl.when(jnp.logical_and(j > 0, j < NB))
    def _():
        step(True, True)

    @pl.when(j == NB)
    def _():
        step(False, True)

    @pl.when(j == NB + TAIL)
    def _():
        for k in range(1, 8):
            label_copy(k).wait()
        lall_ref[...] = lfull[...]

        def drain(b, carry):
            for c in gather_copies(pfull, gs, gr, b):
                c.wait_send()
            return carry
        lax.fori_loop(0, NB, drain, 0)


def forward(a, w, s, gamma, beta, labels):
    prev = lambda j: (0, jnp.clip(j - 1, 0, NB - 1))
    late = lambda j: (0, jnp.clip(j - 4, 0, NB - 1))
    cur = lambda j: (0, jnp.minimum(j, NB - 1))
    f32 = jnp.float32
    return pl.pallas_call(
        fwd_kernel,
        grid=(NB + 1 + TAIL,),
        in_specs=[
            pl.BlockSpec((ROWS, CIN), lambda j: (0, 0), pipeline_mode=pl.Buffered(1)),
            pl.BlockSpec((CIN, CB), cur),
            pl.BlockSpec((ROWS, CB), prev),
            pl.BlockSpec((1, CB), prev),
            pl.BlockSpec((1, CB), prev),
            pl.BlockSpec((8, IMG), lambda j: (0, 0)),
        ],
        out_specs=[
            pl.BlockSpec(memory_space=pl.ANY),
            pl.BlockSpec((IMG, ROWS), lambda j: (jnp.minimum(j, NB - 1), 0)),
            pl.BlockSpec((IMG, CB), prev),
            pl.BlockSpec((IMG, CB), prev),
            pl.BlockSpec((IMG, CB), prev),
            pl.BlockSpec((8, CB), prev),
            pl.BlockSpec((8 * IMG, CB), late),
            pl.BlockSpec((2, 2, 2, 8, IMG), lambda j: (0, 0, 0, 0, 0)),
            pl.BlockSpec((8, CB), lambda j: (0, 0)),
        ],
        out_shape=[
            jax.ShapeDtypeStruct((NB, ROWS, CB), f32),
            jax.ShapeDtypeStruct((CIN, ROWS), jnp.bfloat16),
            jax.ShapeDtypeStruct((IMG, COUT), f32),
            jax.ShapeDtypeStruct((IMG, COUT), f32),
            jax.ShapeDtypeStruct((IMG, COUT), f32),
            jax.ShapeDtypeStruct((8, COUT), f32),
            jax.ShapeDtypeStruct((8 * IMG, COUT), jnp.bfloat16),
            jax.ShapeDtypeStruct((2, 2, 2, 8, IMG), jnp.int32),
            jax.ShapeDtypeStruct((8, CB), f32),
        ],
        scratch_shapes=[
            pltpu.VMEM((2, ROWS, CB), f32),
            pltpu.VMEM((CIN, CB), jnp.bfloat16),
            pltpu.VMEM((24, CB), f32),
            pltpu.VMEM((2, 2, 2, IMG, COUT), f32),
            pltpu.VMEM((2, 2, 2, 8, IMG), jnp.int32),
            pltpu.SemaphoreType.DMA((2,)),
            pltpu.SemaphoreType.DMA((5, NB)),
            pltpu.SemaphoreType.DMA((5, NB)),
            pltpu.SemaphoreType.DMA((8,)),
            pltpu.SemaphoreType.DMA((8,)),
        ],
        compiler_params=pltpu.CompilerParams(vmem_limit_bytes=60 * 1024 * 1024, collective_id=0, has_side_effects=True),
        cost_estimate=pl.CostEstimate(flops=2 * ROWS * CIN * COUT, bytes_accessed=120_000_000, transcendentals=0),
        name="fwd_conv",
    )(a, w, s, gamma, beta, labels)


BTAIL = 7
QR = CIN // 8


def bwd_kernel(at_ref, z_ref, s_ref, sc_ref, sh_ref, bb_ref, cc_ref, da_ref, db_ref, g_hbm, dbo_ref, gsq_ref,
               dz, dw, rd, ha, hb, ra, rb, ka, kb, r2a, r2b, gfull, dball, ss, rs, gs, gr, bs, br, osem):
    j = pl.program_id(0)
    slot = lax.rem(j, 2)
    prev = 1 - slot
    me, core, x, y = position()
    xn, yn, pn = dev(core, 1 - x, y), dev(core, x, 1 - y), dev(1 - core, x, y)
    half = CIN // 2
    HC = CB // 2

    def db_copy(k):
        return rcopy(db_ref, dball.at[me], bs.at[k], br.at[k], lax.rem(me + k, 8))

    @pl.when(j == 0)
    def _():
        enter_all()
        for k in range(1, 8):
            db_copy(k).start()
        dball[me] = db_ref[...]
        gsq_ref[...] = jnp.zeros_like(gsq_ref)

    def out_copy(b):
        cc = pl.ds(pl.multiple_of(b * CB, CB), CB)
        return pltpu.make_async_copy(gfull.at[:, :, :, :, cc], g_hbm.at[:, :, :, :, cc], osem.at[b])

    def core_copy(b):
        return rcopy(dw.at[lax.rem(b, 2), pl.ds(pl.multiple_of((1 - core) * half, half), half), :], rd.at[b], ss.at[0, b], rs.at[0, b], pn)

    def first_copies(b):
        sl = lax.rem(b, 2)
        return (rcopy(ha.at[sl, 1 - x], ra.at[b], ss.at[1, b], rs.at[1, b], xn),
                rcopy(hb.at[sl, 1 - y], rb.at[b], ss.at[2, b], rs.at[2, b], yn))

    def second_copies(b):
        sl = lax.rem(b, 2)
        return (rcopy(ka.at[sl, 1 - y], r2a.at[b], ss.at[3, b], rs.at[3, b], yn),
                rcopy(kb.at[sl, 1 - x], r2b.at[b], ss.at[4, b], rs.at[4, b], xn))

    def stage1(b):
        c = core_copy(b)
        c.wait()
        sl = lax.rem(b, 2)
        for py in range(2):
            for px in range(2):
                q = py * 2 + px
                own = pl.ds(pl.multiple_of(core * half + q * QR, QR), QR)
                ha[sl, px, py] = dw[sl, own, 0:HC] + rd[b, q * QR:(q + 1) * QR, 0:HC]
                hb[sl, py, px] = dw[sl, own, HC:CB] + rd[b, q * QR:(q + 1) * QR, HC:CB]
        for f in first_copies(b):
            f.start()

    def stage2(b):
        sl = lax.rem(b, 2)
        for f in first_copies(b):
            f.wait()
        for k in range(2):
            ka[sl, k] = ha[sl, x, k] + ra[b, k]
            kb[sl, k] = hb[sl, y, k] + rb[b, k]
        for f in second_copies(b):
            f.start()

    def stage3(b):
        sl = lax.rem(b, 2)
        for f in second_copies(b):
            f.wait()
        gfull[core, y, x, :, pl.ds(pl.multiple_of(b * CB, CB), HC)] = ka[sl, y] + r2a[b]
        gfull[core, y, x, :, pl.ds(pl.multiple_of(b * CB + HC, HC), HC)] = kb[sl, x] + r2b[b]
        c = gather_copies(gfull, gs, gr, b)
        c[0].start()
        c[1].start()

    def stage4(b):
        c = gather_copies(gfull, gs, gr, b)
        c[0].wait_recv()
        c[1].wait_recv()
        c[2].start()
        c[3].start()

    def stage5(b):
        c = gather_copies(gfull, gs, gr, b)
        c[2].wait_recv()
        c[3].wait_recv()
        c[4].start()

    def stage6(b):
        gather_copies(gfull, gs, gr, b)[4].wait_recv()
        out_copy(b).start()
        cc = pl.ds(pl.multiple_of(b * CB, CB), CB)
        acc = gsq_ref[...]
        for q in range(8):
            gv = gfull[q // 4, (q // 2) % 2, q % 2, :, cc]
            acc = acc + jnp.sum((gv * gv).reshape(QR // 8, 8, CB), axis=0)
        gsq_ref[...] = acc

    def stages():
        when_block(j - 2, stage1)
        when_block(j - 3, stage2)
        when_block(j - 4, stage3)
        when_block(j - 5, stage4)
        when_block(j - 6, stage5)
        when_block(j - 7, stage6)

    pl.when(j > NB)(stages)

    def step(do_pre, do_mm):
        if do_pre:
            sc = sc_ref[...]
            sh = sh_ref[...]
            bb = bb_ref[...]
            cc = cc_ref[...]

        def pre(base, slabs):
            for n in range(0, IMG, NT):
                da = da_ref[n:n + NT, :]
                for p in range(slabs):
                    r = pl.ds(base + p * IMG + n, NT)
                    zz = z_ref[r, :]
                    u = zz * sc + sh + s_ref[r, :].astype(jnp.float32)
                    dz[slot, r, :] = (jnp.where(u > 0, da, 0.0) + (zz * cc + bb)).astype(jnp.bfloat16)

        def mm(base, size):
            return jnp.dot(at_ref[:, pl.ds(base, size)], dz[prev, pl.ds(base, size), :], preferred_element_type=jnp.float32)

        if do_mm:
            dw[prev] = mm(5376, 896)
        if do_pre:
            pre(5376, 7)

        def chunk(i, carry):
            base = pl.multiple_of(i * 1792, 1792)
            if do_mm:
                pl.when(i == 1)(stages)
            if do_mm:
                dw[prev] += mm(base, 1792)
            if do_pre:
                pre(base, 14)
            return carry
        lax.fori_loop(0, 3, chunk, 0)
        if do_mm:
            core_copy(j - 1).start()

    @pl.when(j == 0)
    def _():
        step(True, False)

    @pl.when(jnp.logical_and(j > 0, j < NB))
    def _():
        step(True, True)

    @pl.when(j == NB)
    def _():
        step(False, True)

    @pl.when(j == NB + BTAIL - 1)
    def _():
        for k in range(1, 8):
            db_copy(k).wait()
        acc = dball[0]
        for k in range(1, 8):
            acc = acc + dball[k]
        dbo_ref[...] = acc

        def drain(b, carry):
            for c in gather_copies(gfull, gs, gr, b):
                c.wait_send()
            out_copy(b).wait()
            return carry
        lax.fori_loop(0, NB, drain, 0)


def backward(at, z, s, sc, sh, bb, cc, da, dgb):
    f32 = jnp.float32
    cur = lambda j: (0, jnp.minimum(j, NB - 1))
    row = pl.BlockSpec((1, CB), cur)
    return pl.pallas_call(
        bwd_kernel,
        grid=(NB + BTAIL,),
        in_specs=[
            pl.BlockSpec((CIN, ROWS), lambda j: (0, 0), pipeline_mode=pl.Buffered(1)),
            pl.BlockSpec((None, ROWS, CB), lambda j: (jnp.minimum(j, NB - 1), 0, 0)),
            pl.BlockSpec((ROWS, CB), cur),
            row, row, row, row,
            pl.BlockSpec((IMG, CB), cur),
            pl.BlockSpec((2, COUT), lambda j: (0, 0)),
        ],
        out_specs=[pl.BlockSpec(memory_space=pl.ANY), pl.BlockSpec((2, COUT), lambda j: (0, 0)), pl.BlockSpec((8, CB), lambda j: (0, 0))],
        out_shape=[jax.ShapeDtypeStruct((2, 2, 2, QR, COUT), f32), jax.ShapeDtypeStruct((2, COUT), f32), jax.ShapeDtypeStruct((8, CB), f32)],
        scratch_shapes=[
            pltpu.VMEM((2, ROWS, CB), jnp.bfloat16),
            pltpu.VMEM((2, CIN, CB), f32),
            pltpu.VMEM((NB, CIN // 2, CB), f32),
            pltpu.VMEM((2, 2, 2, QR, CB // 2), f32),
            pltpu.VMEM((2, 2, 2, QR, CB // 2), f32),
            pltpu.VMEM((NB, 2, QR, CB // 2), f32),
            pltpu.VMEM((NB, 2, QR, CB // 2), f32),
            pltpu.VMEM((2, 2, QR, CB // 2), f32),
            pltpu.VMEM((2, 2, QR, CB // 2), f32),
            pltpu.VMEM((NB, QR, CB // 2), f32),
            pltpu.VMEM((NB, QR, CB // 2), f32),
            pltpu.VMEM((2, 2, 2, QR, COUT), f32),
            pltpu.VMEM((8, 2, COUT), f32),
            pltpu.SemaphoreType.DMA((5, NB)),
            pltpu.SemaphoreType.DMA((5, NB)),
            pltpu.SemaphoreType.DMA((5, NB)),
            pltpu.SemaphoreType.DMA((5, NB)),
            pltpu.SemaphoreType.DMA((8,)),
            pltpu.SemaphoreType.DMA((8,)),
            pltpu.SemaphoreType.DMA((NB,)),
        ],
        compiler_params=pltpu.CompilerParams(vmem_limit_bytes=63 * 1024 * 1024, collective_id=1, has_side_effects=True),
        cost_estimate=pl.CostEstimate(flops=2 * ROWS * CIN * COUT, bytes_accessed=120_000_000, transcendentals=0),
        name="bwd_conv",
    )(at, z, s, sc, sh, bb, cc, da, dgb)


SMOOTHING = 0.1
MOMENTUM = 0.9
TRUST_COEF = 0.001
WEIGHT_DECAY = 5e-5
CLASSES = 1000
KP = 1024
UB = 128
FB = 200
NU = CIN // UB
NF = CLASSES // FB
TOTAL = 8 * IMG


def trust_of(wsq, gsq):
    total = lambda v: jnp.sum(jnp.sum(v, axis=0, keepdims=True), axis=1, keepdims=True)
    wn = jnp.sqrt(total(wsq))
    gn = jnp.sqrt(total(gsq))
    return TRUST_COEF * wn / (gn + WEIGHT_DECAY * wn)


def update_kernel(lr_ref, w_ref, v_ref, g_ref, wsq_ref, gsq_ref, wt_hbm, vt_ref, pall_hbm, lab_ref, bias_ref, vbias_ref,
                  gam_ref, bet_ref, vgam_ref, vbet_ref, dgb_ref,
                  wo_ref, vo_ref, wto_ref, vto_ref, bo_ref, vbo_ref, go_ref, vgo_ref, beo_ref, vbeo_ref, loss_ref,
                  wt, wtb, pall, dlt, gfc, fsq, gb, ls, sem):
    j = pl.program_id(0)
    f32 = jnp.float32
    lr = lr_ref[0]

    def wt_copy():
        return pltpu.make_async_copy(wt_hbm, wt, sem.at[0])

    def pall_copy():
        return pltpu.make_async_copy(pall_hbm, pall, sem.at[1])

    @pl.when(j == 0)
    def _():
        wt_copy().start()
        pall_copy().start()
        gb[...] = jnp.zeros_like(gb)
        ls[...] = jnp.zeros_like(ls)
        fsq[...] = jnp.zeros_like(fsq)
        for (p, v, po, vo, g) in ((gam_ref, vgam_ref, go_ref, vgo_ref, dgb_ref[0:1, :]), (bet_ref, vbet_ref, beo_ref, vbeo_ref, dgb_ref[1:2, :])):
            nv = MOMENTUM * v[...] + lr * g
            vo[...] = nv
            po[...] = p[...] - nv

    @pl.when(j < NU)
    def _():
        rate = jnp.broadcast_to(lr * trust_of(wsq_ref[...], gsq_ref[...]), (8, CB))

        def row(i, carry):
            r = pl.ds(pl.multiple_of(i * 8, 8), 8)
            for c in range(0, COUT, CB):
                cc = slice(c, c + CB)
                w = w_ref[r, cc]
                nv = MOMENTUM * v_ref[r, cc] + rate * (g_ref[r, cc] + WEIGHT_DECAY * w)
                vo_ref[r, cc] = nv
                wo_ref[r, cc] = w - nv
            return carry
        lax.fori_loop(0, UB // 8, row, 0)

    @pl.when(j == 1)
    def _():
        wt_copy().wait()
        pall_copy().wait()

        def row(i, acc):
            r = pl.ds(pl.multiple_of(i * 40, 40), 40)
            w = wt[r, :]
            wtb[r, :] = w.astype(jnp.bfloat16)
            return acc + jnp.sum((w * w).reshape(5, 8, COUT), axis=0)
        fsq[0] = lax.fori_loop(0, CLASSES // 40, row, jnp.zeros((8, COUT), f32))
        wtb[CLASSES:KP, :] = jnp.zeros((KP - CLASSES, COUT), jnp.bfloat16)

    def logits_block(i):
        rows = pl.ds(pl.multiple_of(i * IMG, IMG), IMG)
        lg = lax.dot_general(pall[rows, :], wtb[...], (((1,), (1,)), ((), ())), preferred_element_type=f32)
        cls = lax.broadcasted_iota(jnp.int32, (IMG, KP), 1)
        valid = cls < CLASSES
        lg = jnp.where(valid, lg + bias_ref[...], -1e30)
        mx = jnp.max(lg, axis=1, keepdims=True)
        sh = lg - mx
        ex = jnp.exp(sh)
        lse = jnp.log(jnp.sum(ex, axis=1, keepdims=True))
        lp = sh - lse
        tg = jnp.where(valid, SMOOTHING / CLASSES + jnp.where(lab_ref[rows, :] == cls, 1.0 - SMOOTHING, 0.0), 0.0)
        ls[...] += jnp.sum((tg * lp).reshape(IMG // 8, 8, KP), axis=0)
        dl = (jnp.exp(lp) - tg) * (1.0 / TOTAL)
        gb[...] += jnp.sum(dl.reshape(IMG // 8, 8, KP), axis=0)
        dlt[:, rows] = dl.T.astype(jnp.bfloat16)

    @pl.when(jnp.logical_and(j >= 2, j < 6))
    def _():
        logits_block((j - 2) * 2)
        logits_block((j - 2) * 2 + 1)

    @pl.when(jnp.logical_and(j >= 6, j < 8))
    def _():
        rows = pl.ds(pl.multiple_of((j - 6) * 512, 512), 512)

        def col(i, carry):
            cc = pl.ds(pl.multiple_of(i * 256, 256), 256)
            g = jnp.dot(dlt[rows, :], pall[:, cc], preferred_element_type=f32)
            gfc[rows, cc] = g
            fsq[1, :, cc] += jnp.sum((g * g).reshape(64, 8, 256), axis=0)
            return carry
        lax.fori_loop(0, COUT // 256, col, 0)

    @pl.when(j >= NU)
    def _():
        rate = jnp.broadcast_to(lr * trust_of(fsq[0], fsq[1]), (8, CB))
        base = pl.multiple_of((j - NU) * FB, 8)

        def row(i, carry):
            o = pl.multiple_of(i * 8, 8)
            r = pl.ds(o, 8)
            a = pl.ds(pl.multiple_of(base + o, 8), 8)
            for c in range(0, COUT, CB):
                cc = slice(c, c + CB)
                w = wt[a, cc]
                nv = MOMENTUM * vt_ref[r, cc] + rate * (gfc[a, cc] + WEIGHT_DECAY * w)
                vto_ref[r, cc] = nv
                wto_ref[r, cc] = w - nv
            return carry
        lax.fori_loop(0, FB // 8, row, 0)

    @pl.when(j == NU)
    def _():
        g = jnp.sum(gb[...], axis=0, keepdims=True)
        nv = MOMENTUM * vbias_ref[...] + lr * g
        vbo_ref[...] = nv
        bo_ref[...] = bias_ref[...] - nv
        tot = jnp.sum(jnp.sum(ls[...], axis=0, keepdims=True), axis=1, keepdims=True)
        loss_ref[...] = jnp.broadcast_to(tot * (-1.0 / TOTAL), (8, 128))


def update_all(lr, w, v, g, wsq, gsq, wt, vt, pall, lab, bias, vbias, gamma, beta, vgamma, vbeta, dgb):
    f32 = jnp.float32
    S = jax.ShapeDtypeStruct
    conv = pl.BlockSpec((UB, COUT), lambda j: (jnp.minimum(j, NU - 1), 0))
    fc = pl.BlockSpec((FB, COUT), lambda j: (jnp.clip(j - NU, 0, NF - 1), 0))
    full = lambda *sh: pl.BlockSpec(sh, lambda j: (0,) * len(sh))
    hbm = pl.BlockSpec(memory_space=pl.ANY)
    vec = full(1, COUT)
    bvec = full(1, KP)
    return pl.pallas_call(
        update_kernel,
        grid=(NU + NF,),
        in_specs=[pl.BlockSpec(memory_space=pltpu.SMEM), conv, conv, conv, full(8, CB), full(8, CB), hbm, fc, hbm, full(TOTAL, 1), bvec, bvec,
                  vec, vec, vec, vec, full(2, COUT)],
        out_specs=[conv, conv, fc, fc, bvec, bvec, vec, vec, vec, vec, full(8, 128)],
        out_shape=[S((CIN, COUT), f32), S((CIN, COUT), f32), S((CLASSES, COUT), f32), S((CLASSES, COUT), f32), S((1, KP), f32), S((1, KP), f32),
                   S((1, COUT), f32), S((1, COUT), f32), S((1, COUT), f32), S((1, COUT), f32), S((8, 128), f32)],
        scratch_shapes=[
            pltpu.VMEM((CLASSES, COUT), f32),
            pltpu.VMEM((KP, COUT), jnp.bfloat16),
            pltpu.VMEM((TOTAL, COUT), jnp.bfloat16),
            pltpu.VMEM((KP, TOTAL), jnp.bfloat16),
            pltpu.VMEM((KP, COUT), f32),
            pltpu.VMEM((2, 8, COUT), f32),
            pltpu.VMEM((8, KP), f32),
            pltpu.VMEM((8, KP), f32),
            pltpu.SemaphoreType.DMA((2,)),
        ],
        compiler_params=pltpu.CompilerParams(vmem_limit_bytes=63 * 1024 * 1024),
        cost_estimate=pl.CostEstimate(flops=9_000_000_000, bytes_accessed=80_000_000, transcendentals=0),
        name="update",
    )(lr, w, v, g, wsq, gsq, wt, vt, pall, lab, bias, vbias, gamma, beta, vgamma, vbeta, dgb)


from jax.sharding import PartitionSpec as P


def head(pb, labels, w_fc_t, fc_bias, total):
    bf = jnp.bfloat16
    f32 = jnp.float32
    classes = w_fc_t.shape[0]
    wb = w_fc_t.astype(bf)
    logits = jnp.einsum('nc,kc->nk', pb, wb, preferred_element_type=f32) + fc_bias
    log_prob = jax.nn.log_softmax(logits, axis=-1)
    one_hot = (labels[:, None] == jnp.arange(classes, dtype=jnp.int32)[None, :]).astype(f32)
    target = SMOOTHING / classes + (1.0 - SMOOTHING) * one_hot
    loss = -jnp.sum(target * log_prob) / total
    dl = (jnp.exp(log_prob) - target) / total
    return pb, wb, dl, dl.astype(bf), loss


def solution(mesh):
    groups = mesh.shape['dp']

    def local_step(act_in, shortcut, labels, w_conv, gamma, beta, w_fc, fc_bias, vel_conv, vel_gamma, vel_beta, vel_fc, vel_bias, lr):
        f32 = jnp.float32
        total = IMG * groups
        a = act_in.transpose(1, 2, 0, 3).reshape(ROWS, CIN)
        s = shortcut.transpose(1, 2, 0, 3).reshape(ROWS, COUT)
        w_fc_t = w_fc.T
        lab8 = jnp.broadcast_to(labels[None], (8, IMG))
        z, at, pooled, cnt, sx, st, pall, lall, wsq = forward(a, w_conv, s, gamma[None], beta[None], lab8)
        _, wb, _, dlb, _ = head(pooled.astype(jnp.bfloat16), labels, w_fc_t, fc_bias, total)
        dpool = jnp.einsum('nk,kc->nc', dlb, wb, preferred_element_type=f32) / POS
        mean = st[0:1]
        inv = st[1:2]
        gam = gamma[None]
        d_beta = jnp.sum(dpool * cnt, axis=0, keepdims=True)
        d_gamma = jnp.sum(dpool * sx, axis=0, keepdims=True)
        sc = gam * inv
        sh = beta[None] - mean * sc
        cc = -(sc * inv) * (d_gamma / ROWS)
        bb = -sc * (d_beta / ROWS) - mean * cc
        dgb = jnp.concatenate([d_gamma, d_beta])
        g8, dgb, gsq = backward(at, z, s, sc, sh, bb, cc, dpool * sc, dgb)
        pad = lambda b: jnp.pad(b, (0, KP - CLASSES))[None]
        wo, vo, wto, vto, bo, vbo, go, vgo, beo, vbeo, loss = update_all(
            lr.reshape(1), w_conv, vel_conv, g8.reshape(CIN, COUT), wsq, gsq, w_fc_t, vel_fc.T, pall, lall[:, :, :, 0].reshape(total, 1),
            pad(fc_bias), pad(vel_bias), gamma[None], beta[None], vel_gamma[None], vel_beta[None], dgb)
        return (wo, go[0], beo[0], wto.T, bo[0, :CLASSES], vo, vgo[0], vbeo[0], vto.T, vbo[0, :CLASSES], loss[0, 0])

    return jax.shard_map(local_step, mesh=mesh, in_specs=(P('dp'),) * 3 + (P(),) * 11, out_specs=(P(),) * 11, check_vma=False)
```

```python
import functools
import jax
import jax.numpy as jnp
from jax import lax
from jax.experimental import pallas as pl
from jax.experimental.pallas import tpu as pltpu
from jax.sharding import PartitionSpec as P

BN_EPS = 1e-5
SMOOTHING = 0.1
MOMENTUM = 0.9
TRUST_COEF = 0.001
WEIGHT_DECAY = 5e-5

LANES = 128
SUB = 8
IMG = 128
POS = 49
ROWS = IMG * POS
CIN = 1024
COUT = 2048
CLASSES = 1000
KP = 1024
DEVS = 8
TOTAL = DEVS * IMG
CB = 256
HC = CB // 2
NB = COUT // CB
CH = 7
NCH = POS // CH
NT = 16
APAD = CIN + LANES
TAIL = 3
BTAIL = 7
QR = CIN // DEVS
HALF = CIN // 2
BIG = 1792
BTILE = BIG // IMG
NBIG = ROWS // BIG
UB = 128
FB = 208
NU = CIN // UB
NF = pl.cdiv(CLASSES, FB)
LB = 256
MIB = 1024 * 1024
F32 = jnp.float32
BF16 = jnp.bfloat16
MESH = pl.DeviceIdType.MESH
XN, YN, PN = 'x', 'y', 'core'


def dot(a, b):
    return jnp.dot(a, b, preferred_element_type=F32)


def dot_t(a, b):
    return lax.dot_general(a, b, (((1,), (1,)), ((), ())), preferred_element_type=F32)


def fold(v, axis=0):
    return jnp.sum(v.reshape(v.shape[0] // SUB, SUB, v.shape[1]), axis=axis)


def rowsum(v, axis=0):
    return jnp.sum(v, axis=axis, keepdims=True)


def lanesum(v, axis=1):
    return jnp.sum(v, axis=axis, keepdims=True)


def cols(b, size=CB, at=0):
    return pl.ds(pl.multiple_of(b * CB + at, LANES), size)


def span(i, size):
    return pl.ds(pl.multiple_of(i * size, SUB), size)


def position():
    me = lax.axis_index('dp')
    return me, lax.rem(me, 2), lax.rem(me // 2, 2), me // 4


def dev(core, x, y):
    return (y * 2 + x) * 2 + core


def neighbour(name):
    me, core, x, y = position()
    flip = lambda v, k: 1 - v if k == name else v
    return dev(flip(core, PN), flip(x, XN), flip(y, YN))


def enter_all():
    me = lax.axis_index('dp')
    bar = pltpu.get_barrier_semaphore()
    for k in range(1, DEVS):
        pl.semaphore_signal(bar, inc=1, device_id=(lax.rem(me + k, DEVS),), device_id_type=MESH)
    pl.semaphore_wait(bar, DEVS - 1)


def rcopy(src, dst, send, recv, target):
    return pltpu.make_async_remote_copy(src_ref=src, dst_ref=dst, send_sem=send, recv_sem=recv, device_id=(target,), device_id_type=MESH)


def each(fn, copies):
    for c in copies:
        fn(c)


def start(c):
    c.start()


def wait(c):
    c.wait()


def wait_send(c):
    c.wait_send()


def wait_recv(c):
    c.wait_recv()


def gather_own(buf, send, recv, b, ka=0, kb=1):
    me, core, x, y = position()
    a, c = buf.at[core, y, x, :, cols(b, HC)], buf.at[core, y, x, :, cols(b, HC, HC)]
    return rcopy(a, a, send.at[ka, b], recv.at[ka, b], neighbour(YN)), rcopy(c, c, send.at[kb, b], recv.at[kb, b], neighbour(XN))


def gather_on(buf, send, recv, b, ka=2, kb=3):
    me, core, x, y = position()
    a, c = buf.at[core, :, x, :, cols(b, HC)], buf.at[core, y, :, :, cols(b, HC, HC)]
    return rcopy(a, a, send.at[ka, b], recv.at[ka, b], neighbour(XN)), rcopy(c, c, send.at[kb, b], recv.at[kb, b], neighbour(YN))


def gather_core(buf, send, recv, b, k=4):
    me, core, x, y = position()
    a = buf.at[core, :, :, :, cols(b)]
    return (rcopy(a, a, send.at[k, b], recv.at[k, b], neighbour(PN)),)


def gather_all(*a):
    return gather_own(*a) + gather_on(*a) + gather_core(*a)


def when_block(b, fn):
    @pl.when(jnp.logical_and(b >= 0, b < NB))
    def _():
        fn(b)


def stage_list(j, fns, lag=2):
    for k, fn in enumerate(fns):
        when_block(j - lag - k, fn)


def pieces():
    return [(c, y, x) for c in range(2) for y in range(2) for x in range(2)]


def softmax_terms(logits, bias, labels):
    n = logits.shape[0]
    cls = lax.broadcasted_iota(jnp.int32, (n, KP), 1)
    valid = cls < CLASSES
    lg = jnp.where(valid, logits + bias, -1e30)
    sh = lg - jnp.max(lg, axis=1, keepdims=True)
    lp = sh - jnp.log(lanesum(jnp.exp(sh)))
    lab = jnp.concatenate([labels] * (KP // LANES), axis=1)
    hit = lab == cls.astype(F32)
    tg = jnp.where(valid, SMOOTHING / CLASSES + jnp.where(hit, 1.0 - SMOOTHING, 0.0), 0.0)
    return tg * lp, (jnp.exp(lp) - tg) * (1.0 / TOTAL)


def label_rows(row):
    return jnp.broadcast_to(row.astype(F32), (IMG, IMG)).T


def set_bias(bpad, bias_ref):
    bpad[:] = jnp.zeros_like(bpad)
    bpad[:, :CLASSES] = bias_ref[:]


def fwd_kernel(a_hbm, w_ref, s_ref, g_ref, b_ref, lab_ref, bias_ref, wt_hbm,
               z_hbm, at_ref, pall_ref, lall_ref, wsq_ref, fsq_ref, wtb_hbm, da_ref, sc_ref, sh_ref, bb_ref, cc_ref, db_ref,
               abf, zbuf, wbf, stat, pfull, lfull, pool, cnt, sx, sv, wtb, bpad, asem, zsem, wsem, osem, gs, gr, ls, lr):
    j = pl.program_id(0)
    slot = lax.rem(j, 2)
    prev = 1 - slot
    me, core, x, y = position()
    crow = CH * IMG

    def a_copy(i):
        r = span(i, crow)
        return pltpu.make_async_copy(a_hbm.at[r, :], abf.at[r, :CIN], asem.at[i])

    def z_copy(jj):
        sl = lax.rem(jj, 2)
        return pltpu.make_async_copy(zbuf.at[sl], z_hbm.at[jj], zsem.at[sl])

    def wt_view(b):
        return zbuf.at[b // 6, pl.ds((b % 6) * CLASSES, CLASSES), :]

    def wt_copy(b):
        return pltpu.make_async_copy(wt_hbm.at[:, pl.ds(b * CB, CB)], wt_view(b), wsem.at[b])

    def wtb_copy():
        return pltpu.make_async_copy(wtb, wtb_hbm, osem)

    def label_copy(k):
        return rcopy(lab_ref, lfull.at[core, y, x], ls.at[k], lr.at[k], lax.rem(me + k, DEVS))

    labels = [label_copy(k) for k in range(1, DEVS)]

    @pl.when(j == 0)
    def _():
        for i in range(NCH):
            a_copy(i).start()
        enter_all()
        each(start, labels)
        lfull[core, y, x] = lab_ref[:]
        wsq_ref[:] = jnp.zeros_like(wsq_ref)
        set_bias(bpad, bias_ref)

    def second(b):
        each(wait_recv, gather_own(pfull, gs, gr, b))
        each(start, gather_on(pfull, gs, gr, b))

    def third(b):
        each(wait_recv, gather_on(pfull, gs, gr, b))
        each(start, gather_core(pfull, gs, gr, b))

    def last(b):
        each(wait_recv, gather_core(pfull, gs, gr, b))
        for q, (c, py, px) in enumerate(pieces()):
            pall_ref[span(q, IMG), :] = pfull[c, py, px, :, cols(b)].astype(BF16)

    def stages():
        stage_list(j, (second, third, last))

    @pl.when(jnp.logical_and(j >= 2, j < NB + 2))
    def _():
        z_copy(j - 2).wait()

    def step(first, do_mm, do_post):
        if do_mm:
            wf = w_ref[:]
            wsq_ref[:] += fold(wf * wf)
            w = wf.astype(BF16)
            wbf[:] = w
            if first:
                a_copy(0).wait()
            m0 = rowsum(dot(abf[:IMG, :CIN], w)) * (1.0 / IMG)
            stat[:2 * SUB] = jnp.zeros((2 * SUB, CB), F32)
        if do_post:
            mean = stat[2 * SUB:2 * SUB + 1]
            inv = stat[3 * SUB:3 * SUB + 1]
            sc = g_ref[:] * inv
            sh = b_ref[:] - mean * sc
            pool[:] = jnp.zeros_like(pool)
            pc = cols(j - 1)
            cnt[:, pc] = jnp.zeros((IMG, CB), F32)
            sx[:, pc] = jnp.zeros((IMG, CB), F32)

        def chunk(i, carry):
            base = pl.multiple_of(i * crow, crow)
            if do_post:
                pl.when(i == 4)(stages)
            if do_mm:
                if first:
                    pl.when(i > 0)(lambda: a_copy(i).wait())
                r = pl.ds(base, crow)
                zc = dot(abf[r, :CIN], wbf[:])
                zbuf[slot, r, :] = zc
                d = zc - m0
                stat[:SUB] += fold(d)
                stat[SUB:2 * SUB] += fold(d * d)
                at_ref[:, r] = abf[r, pl.ds(pl.multiple_of(j * IMG, IMG), IMG)].astype(F32).T.astype(BF16)
            if do_post:
                for n in range(0, IMG, NT):
                    nr = slice(n, n + NT)
                    pa, ca, xa = pool[nr], cnt[nr, pc], sx[nr, pc]
                    for p in range(CH):
                        r = pl.ds(base + p * IMG + n, NT)
                        zz = zbuf[prev, r, :]
                        u = zz * sc + sh + s_ref[r, :].astype(F32)
                        mk = u > 0
                        pa = pa + jnp.maximum(u, 0.0)
                        ca = ca + jnp.where(mk, 1.0, 0.0)
                        xa = xa + jnp.where(mk, zz, 0.0)
                    pool[nr], cnt[nr, pc], sx[nr, pc] = pa, ca, xa
            return carry

        lax.fori_loop(0, NCH, chunk, 0)
        if do_post:
            pfull[core, y, x, :, pc] = pool[:] * (1.0 / POS)
            sx[:, pc] = (sx[:, pc] - mean * cnt[:, pc]) * inv
            sv[:1, pc] = mean
            sv[SUB:SUB + 1, pc] = inv
            sc_ref[:, pc] = sc
            sh_ref[:, pc] = sh
            each(start, gather_own(pfull, gs, gr, j - 1))
        if do_mm:
            dm = rowsum(stat[:SUB]) * (1.0 / ROWS)
            q = rowsum(stat[SUB:2 * SUB]) * (1.0 / ROWS)
            stat[2 * SUB:2 * SUB + 1] = m0 + dm
            stat[3 * SUB:3 * SUB + 1] = lax.rsqrt(jnp.maximum(q - dm * dm, 0.0) + BN_EPS)
            z_copy(j).start()

    @pl.when(j == 0)
    def _():
        step(True, True, False)

    @pl.when(jnp.logical_and(j > 0, j < NB))
    def _():
        step(False, True, True)

    @pl.when(j == NB)
    def _():
        for b in range(6):
            wt_copy(b).start()
        step(False, False, True)

    @pl.when(j == NB + 1)
    def _():
        for b in range(6, NB):
            wt_copy(b).start()
        stages()
        wtb[CLASSES:] = jnp.zeros((KP - CLASSES, COUT), BF16)
        for b in range(NB):
            wt_copy(b).wait()
            view = wt_view(b)

            def cast(i, acc):
                w = view[span(i, 40), :]
                wtb[span(i, 40), b * CB:(b + 1) * CB] = w.astype(BF16)
                return acc + fold(w * w)
            fsq_ref[:, b * CB:(b + 1) * CB] = lax.fori_loop(0, CLASSES // 40, cast, jnp.zeros((SUB, CB), F32))
        wtb_copy().start()

    @pl.when(j == NB + 2)
    def _():
        stages()
        own = pfull[core, y, x].astype(BF16)
        lg = dot_t(own, wtb[:])
        _, dl = softmax_terms(lg, bpad[:], label_rows(lab_ref[:]))
        dlb = dl.astype(BF16)

        def col(b, carry):
            c = cols(b)
            dp = dot(dlb, wtb[:, c]) * (1.0 / POS)
            dbeta = rowsum(dp * cnt[:, c])
            dgamma = rowsum(dp * sx[:, c])
            sc = sc_ref[:, c]
            cc = -(sc * sv[SUB:SUB + 1, c]) * (dgamma * (1.0 / ROWS))
            cc_ref[:, c] = cc
            bb_ref[:, c] = -sc * (dbeta * (1.0 / ROWS)) - sv[:1, c] * cc
            da_ref[:, c] = dp * sc
            db_ref[:1, c] = dgamma
            db_ref[1:, c] = dbeta
            return carry
        lax.fori_loop(0, NB, col, 0)

    @pl.when(j == NB + TAIL)
    def _():
        stages()
        each(wait, labels)
        lall_ref[:] = lfull[:]
        wtb_copy().wait()

        def drain(b, carry):
            each(wait_send, gather_all(pfull, gs, gr, b))
            return carry
        lax.fori_loop(0, NB, drain, 0)


def whole(*shape):
    return pl.BlockSpec(shape, lambda j: (0,) * len(shape))


def struct(shape, dtype=F32):
    return jax.ShapeDtypeStruct(shape, dtype)


def fvmem(*shape):
    return pltpu.VMEM(shape, F32)


def bvmem(*shape):
    return pltpu.VMEM(shape, BF16)


def dma(*shape):
    return pltpu.SemaphoreType.DMA(shape)


HBM = pl.BlockSpec(memory_space=pl.ANY)
QUAD = (2, 2, 2)


def forward(a, w, s, gamma, beta, labels, bias, wt):
    prev = lambda j: (0, jnp.clip(j - 1, 0, NB - 1))
    cur = lambda j: (0, jnp.minimum(j, NB - 1))
    late = lambda j: (0, jnp.clip(j - 4, 0, NB - 1))
    vec, lab = (1, COUT), QUAD + (1, IMG)
    return pl.pallas_call(
        fwd_kernel,
        grid=(NB + 1 + TAIL,),
        in_specs=[HBM, pl.BlockSpec((CIN, CB), cur), pl.BlockSpec((ROWS, CB), prev), pl.BlockSpec((1, CB), prev), pl.BlockSpec((1, CB), prev),
                  whole(1, IMG), whole(1, CLASSES), HBM],
        out_specs=[HBM, pl.BlockSpec((IMG, ROWS), lambda j: (jnp.minimum(j, NB - 1), 0)), pl.BlockSpec((TOTAL, CB), late), whole(*lab),
                   whole(SUB, CB), whole(SUB, COUT), HBM, whole(IMG, COUT)] + [whole(*vec)] * 4 + [whole(2, COUT)],
        out_shape=[struct((NB, ROWS, CB)), struct((CIN, ROWS), BF16), struct((TOTAL, COUT), BF16), struct(lab, jnp.int32),
                   struct((SUB, CB)), struct((SUB, COUT)), struct((KP, COUT), BF16), struct((IMG, COUT))] + [struct(vec)] * 4 + [struct((2, COUT))],
        scratch_shapes=[bvmem(ROWS, APAD), fvmem(2, ROWS, CB), bvmem(CIN, CB), fvmem(4 * SUB, CB), fvmem(*QUAD, IMG, COUT), pltpu.VMEM(lab, jnp.int32),
                        fvmem(IMG, CB), fvmem(IMG, COUT), fvmem(IMG, COUT), fvmem(2 * SUB, COUT), bvmem(KP, COUT), fvmem(1, KP),
                        dma(NCH), dma(2), dma(NB), pltpu.SemaphoreType.DMA, dma(5, NB), dma(5, NB), dma(DEVS), dma(DEVS)],
        compiler_params=pltpu.CompilerParams(vmem_limit_bytes=63 * MIB, collective_id=0, has_side_effects=True),
        cost_estimate=pl.CostEstimate(flops=2 * ROWS * CIN * COUT, bytes_accessed=2 * ROWS * COUT * 4, transcendentals=0),
        name="fwd_conv",
    )(a, w, s, gamma, beta, labels, bias, wt)


def bwd_kernel(at_hbm, z_ref, s_ref, sc_ref, sh_ref, bb_ref, cc_ref, da_ref, db_ref, pall_hbm, wtb_hbm, lab_ref, bias_ref,
               g_hbm, dbo_ref, gsq_ref, gfc_hbm, fsq_ref, gb_ref, loss_ref,
               atv, dz, dw, rd, ha, hb, ra, rb, ka, kb, r2a, r2b, gfull, dball, bpad, ss, rs, gs, gr, bs, br, osem, isem, fsem):
    j = pl.program_id(0)
    slot = lax.rem(j, 2)
    prev = 1 - slot
    me, core, x, y = position()
    plan = pl.ds(0, COUT)
    pall = atv.at[:, plan]
    wtb = atv.at[:, pl.ds(COUT, COUT)]
    dlt = atv.at[:, pl.ds(2 * COUT, TOTAL)]

    at_copy = pltpu.make_async_copy(at_hbm, atv, isem.at[0])
    pall_copy = pltpu.make_async_copy(pall_hbm, pall, isem.at[1])
    wtb_copy = pltpu.make_async_copy(wtb_hbm, wtb, isem.at[2])
    db_copies = [rcopy(db_ref, dball.at[me], bs.at[k], br.at[k], lax.rem(me + k, DEVS)) for k in range(1, DEVS)]

    @pl.when(j == 0)
    def _():
        at_copy.start()
        enter_all()
        each(start, db_copies)
        dball[me] = db_ref[:]
        for r in (gsq_ref, fsq_ref, gb_ref, loss_ref):
            r[:] = jnp.zeros_like(r)
        set_bias(bpad, bias_ref)

    @pl.when(j == 1)
    def _():
        at_copy.wait()

    def out_copy(b):
        c = cols(b)
        return pltpu.make_async_copy(gfull.at[:, :, :, :, c], g_hbm.at[:, :, :, :, c], osem.at[b])

    def core_copy(b, k=0):
        return rcopy(dw.at[lax.rem(b, 2), span(1 - core, HALF), :], rd.at[b], ss.at[k, b], rs.at[k, b], neighbour(PN))

    def first_copies(b, k=1, m=2):
        sl = lax.rem(b, 2)
        return (rcopy(ha.at[sl, 1 - x], ra.at[b], ss.at[k, b], rs.at[k, b], neighbour(XN)),
                rcopy(hb.at[sl, 1 - y], rb.at[b], ss.at[m, b], rs.at[m, b], neighbour(YN)))

    def second_copies(b, k=3, m=4):
        sl = lax.rem(b, 2)
        return (rcopy(ka.at[sl, 1 - y], r2a.at[b], ss.at[k, b], rs.at[k, b], neighbour(YN)),
                rcopy(kb.at[sl, 1 - x], r2b.at[b], ss.at[m, b], rs.at[m, b], neighbour(XN)))

    def stage1(b):
        core_copy(b).wait()
        sl = lax.rem(b, 2)
        for q, (py, px) in enumerate((py, px) for py in range(2) for px in range(2)):
            own = pl.ds(pl.multiple_of(core * HALF + q * QR, QR), QR)
            got = slice(q * QR, (q + 1) * QR)
            ha[sl, px, py] = dw[sl, own, :HC] + rd[b, got, :HC]
            hb[sl, py, px] = dw[sl, own, HC:] + rd[b, got, HC:]
        each(start, first_copies(b))

    def stage2(b):
        sl = lax.rem(b, 2)
        each(wait, first_copies(b))
        for k in range(2):
            ka[sl, k] = ha[sl, x, k] + ra[b, k]
            kb[sl, k] = hb[sl, y, k] + rb[b, k]
        each(start, second_copies(b))

    def stage3(b):
        sl = lax.rem(b, 2)
        each(wait, second_copies(b))
        gfull[core, y, x, :, cols(b, HC)] = ka[sl, y] + r2a[b]
        gfull[core, y, x, :, cols(b, HC, HC)] = kb[sl, x] + r2b[b]
        each(start, gather_own(gfull, gs, gr, b))

    def stage4(b):
        each(wait_recv, gather_own(gfull, gs, gr, b))
        each(start, gather_on(gfull, gs, gr, b))

    def stage5(b):
        each(wait_recv, gather_on(gfull, gs, gr, b))
        each(start, gather_core(gfull, gs, gr, b))

    def stage6(b):
        each(wait_recv, gather_core(gfull, gs, gr, b))
        out_copy(b).start()
        acc = gsq_ref[:]
        for q in pieces():
            gv = gfull[q + (slice(None), cols(b))]
            acc = acc + fold(gv * gv)
        gsq_ref[:] = acc

    def stages():
        stage_list(j, (stage1, stage2, stage3, stage4, stage5, stage6))

    def step(do_pre, do_mm):
        if do_pre:
            sc, sh, bb, cc = sc_ref[:], sh_ref[:], bb_ref[:], cc_ref[:]

        def pre(base, slabs):
            for n in range(0, IMG, NT):
                da = da_ref[n:n + NT, :]
                for p in range(slabs):
                    r = pl.ds(base + p * IMG + n, NT)
                    zz = z_ref[r, :]
                    u = zz * sc + sh + s_ref[r, :].astype(F32)
                    dz[slot, r, :] = (jnp.where(u > 0, da, 0.0) + (zz * cc + bb)).astype(BF16)

        def mm(base, size):
            return dot(atv[:, pl.ds(base, size)], dz[prev, pl.ds(base, size), :])

        rest = NBIG * BIG
        if do_mm:
            dw[prev] = mm(rest, ROWS - rest)
        if do_pre:
            pre(rest, POS - NBIG * BTILE)

        def chunk(i, carry):
            base = pl.multiple_of(i * BIG, BIG)
            if do_mm:
                pl.when(i == 1)(stages)
                dw[prev] += mm(base, BIG)
            if do_pre:
                pre(base, BTILE)
            return carry
        lax.fori_loop(0, NBIG, chunk, 0)
        if do_mm:
            core_copy(j - 1).start()

    @pl.when(j == 0)
    def _():
        step(True, False)

    @pl.when(jnp.logical_and(j > 0, j < NB))
    def _():
        step(True, True)

    def logits_unit(i):
        rows = span(i, LB)
        lg = dot_t(pall[rows, :], wtb[:])
        lab = jnp.concatenate([label_rows(lab_ref[i // 2, lax.rem(i, 2), k]) for k in range(2)])
        lterm, dl = softmax_terms(lg, bpad[:], lab)
        loss_ref[:] += fold(lterm)
        gb_ref[:] += fold(dl)
        dlt[:, pl.ds(pl.multiple_of(i * LB, LB), LB)] = dl.T.astype(BF16)

    def fc_copies(c):
        sl = lax.rem(c, 4)
        return [pltpu.make_async_copy(rd.at[sl * 2 + h], gfc_hbm.at[pl.ds(h * HALF, HALF), cols(c)], fsem.at[h, c]) for h in range(2)]

    def dfc_unit(c):
        pl.when(c >= 4)(lambda: each(wait, fc_copies(c - 4)))
        acc = jnp.zeros((SUB, CB), F32)
        for h in range(2):
            g = dot(dlt[pl.ds(h * HALF, HALF), :], pall[:, cols(c)])
            rd[lax.rem(c, 4) * 2 + h] = g
            acc = acc + fold(g * g)
        fsq_ref[:, cols(c)] = acc
        each(start, fc_copies(c))

    def loop(lo, hi, fn):
        def body(i, carry):
            fn(i)
            return carry
        lax.fori_loop(lo, hi, body, 0)

    @pl.when(j == NB)
    def _():
        step(False, True)
        pall_copy.start()
        wtb_copy.start()

    @pl.when(j > NB)
    def _():
        stages()
        k = j - NB - 1

        @pl.when(k == 0)
        def _():
            pall_copy.wait()
            wtb_copy.wait()

        loop(jnp.minimum(k * 3, 4), jnp.minimum(k * 3 + 3, 4), logits_unit)
        loop(jnp.clip(k * 3 - 3, 0, NB), jnp.clip(k * 3, 0, NB), dfc_unit)

    @pl.when(j == NB + BTAIL - 1)
    def _():
        each(wait, db_copies)
        acc = dball[0]
        for k in range(1, DEVS):
            acc = acc + dball[k]
        dbo_ref[:] = acc
        for c in range(4, NB):
            each(wait, fc_copies(c))

        def drain(b):
            each(wait_send, gather_all(gfull, gs, gr, b))
            out_copy(b).wait()
        loop(0, NB, drain)


def backward(at, z, s, sc, sh, bb, cc, da, dgb, pall, wtb, lab, bias):
    cur = lambda j: (0, jnp.minimum(j, NB - 1))
    row = pl.BlockSpec((1, CB), cur)
    pair, quad, side = (2, QR, HC), (2, 2, 2, QR, HC), (NB, QR, HC)
    return pl.pallas_call(
        bwd_kernel,
        grid=(NB + BTAIL,),
        in_specs=[HBM, pl.BlockSpec((None, ROWS, CB), lambda j: (jnp.minimum(j, NB - 1), 0, 0)), pl.BlockSpec((ROWS, CB), cur), row, row, row, row,
                  pl.BlockSpec((IMG, CB), cur), whole(2, COUT), HBM, HBM, whole(2, 2, 2, 1, IMG), whole(1, CLASSES)],
        out_specs=[HBM, whole(2, COUT), whole(SUB, CB), HBM, whole(SUB, COUT), whole(SUB, KP), whole(SUB, KP)],
        out_shape=[struct(QUAD + (QR, COUT)), struct((2, COUT)), struct((SUB, CB)), struct((KP, COUT)), struct((SUB, COUT)), struct((SUB, KP)), struct((SUB, KP))],
        scratch_shapes=[bvmem(CIN, ROWS), bvmem(2, ROWS, CB), fvmem(2, CIN, CB), fvmem(NB, HALF, CB), fvmem(*quad), fvmem(*quad),
                        fvmem(NB, *pair), fvmem(NB, *pair), fvmem(2, *pair), fvmem(2, *pair), fvmem(*side), fvmem(*side),
                        fvmem(*QUAD, QR, COUT), fvmem(DEVS, 2, COUT), fvmem(1, KP),
                        dma(5, NB), dma(5, NB), dma(5, NB), dma(5, NB), dma(DEVS), dma(DEVS), dma(NB), dma(3), dma(2, NB)],
        compiler_params=pltpu.CompilerParams(vmem_limit_bytes=63 * MIB, collective_id=1, has_side_effects=True),
        cost_estimate=pl.CostEstimate(flops=2 * ROWS * CIN * COUT, bytes_accessed=2 * ROWS * COUT * 4, transcendentals=0),
        name="bwd_conv",
    )(at, z, s, sc, sh, bb, cc, da, dgb, pall, wtb, lab, bias)


def trust_of(wsq, gsq):
    wn = jnp.sqrt(lanesum(rowsum(wsq)))
    gn = jnp.sqrt(lanesum(rowsum(gsq)))
    return TRUST_COEF * wn / (gn + WEIGHT_DECAY * wn)


def update_kernel(lr_ref, w_ref, v_ref, g_ref, wsq_ref, gsq_ref, wt_ref, vt_ref, gt_ref, tsq_ref, fsq_ref, bias_ref, vbias_ref, gb_ref, ls_ref,
                  gam_ref, bet_ref, vgam_ref, vbet_ref, dgb_ref,
                  wo_ref, vo_ref, wto_ref, vto_ref, bo_ref, vbo_ref, go_ref, vgo_ref, beo_ref, vbeo_ref, loss_ref):
    j = pl.program_id(0)
    lr = lr_ref[0]

    def plain(p, v, g, po, vo):
        nv = MOMENTUM * v[:] + lr * g
        vo[:] = nv
        po[:] = p[:] - nv

    @pl.when(j == 0)
    def _():
        plain(gam_ref, vgam_ref, dgb_ref[:1], go_ref, vgo_ref)
        plain(bet_ref, vbet_ref, dgb_ref[1:], beo_ref, vbeo_ref)
        plain(bias_ref, vbias_ref, rowsum(gb_ref[:])[:, :CLASSES], bo_ref, vbo_ref)
        loss_ref[:] = lanesum(rowsum(ls_ref[:])) * (-1.0 / TOTAL)

    def lars(w_ref, v_ref, g_ref, wsq, gsq, wo, vo, rows):
        rate = jnp.broadcast_to(lr * trust_of(wsq[:], gsq[:]), (SUB, CB))

        def row(i, carry):
            for q in range(2):
                r = pl.ds(pl.multiple_of(i * 2 * SUB + q * SUB, SUB), SUB)
                for c in range(0, COUT, CB):
                    cc = slice(c, c + CB)
                    w = w_ref[r, cc]
                    nv = MOMENTUM * v_ref[r, cc] + rate * (g_ref[r, cc] + WEIGHT_DECAY * w)
                    vo[r, cc] = nv
                    wo[r, cc] = w - nv
            return carry
        lax.fori_loop(0, rows // (2 * SUB), row, 0)

    @pl.when(j < NU)
    def _():
        lars(w_ref, v_ref, g_ref, wsq_ref, gsq_ref, wo_ref, vo_ref, UB)

    @pl.when(j >= NU)
    def _():
        lars(wt_ref, vt_ref, gt_ref, tsq_ref, fsq_ref, wto_ref, vto_ref, FB)


def update_all(*args):
    conv = pl.BlockSpec((UB, COUT), lambda j: (jnp.minimum(j, NU - 1), 0))
    fc = pl.BlockSpec((FB, COUT), lambda j: (jnp.clip(j - NU, 0, NF - 1), 0))
    vec, bvec, one = (1, COUT), (1, CLASSES), (1, 1)
    vs, bs = whole(*vec), whole(*bvec)
    big, fcs = struct((CIN, COUT)), struct((CLASSES, COUT))
    return pl.pallas_call(
        update_kernel,
        grid=(NU + NF,),
        in_specs=[pl.BlockSpec(memory_space=pltpu.SMEM), conv, conv, conv, whole(SUB, CB), whole(SUB, CB), fc, fc, fc, whole(SUB, COUT), whole(SUB, COUT),
                  bs, bs, whole(SUB, KP), whole(SUB, KP), vs, vs, vs, vs, whole(2, COUT)],
        out_specs=[conv, conv, fc, fc, bs, bs, vs, vs, vs, vs, whole(*one)],
        out_shape=[big, big, fcs, fcs] + [struct(bvec)] * 2 + [struct(vec)] * 4 + [struct(one)],
        compiler_params=pltpu.CompilerParams(vmem_limit_bytes=63 * MIB),
        cost_estimate=pl.CostEstimate(flops=CIN * COUT * 16, bytes_accessed=10 * CIN * COUT * 4, transcendentals=0),
        name="update",
    )(*args)


def solution(mesh):
    def local_step(act_in, shortcut, labels, w_conv, gamma, beta, w_fc, fc_bias, vel_conv, vel_gamma, vel_beta, vel_fc, vel_bias, lr):
        a = act_in.transpose(1, 2, 0, 3).reshape(ROWS, CIN)
        s = shortcut.transpose(1, 2, 0, 3).reshape(ROWS, COUT)
        wt = w_fc.T
        bias = fc_bias[None]
        z, at, pall, lab, wsq, tsq, wtb, da, sc, sh, bb, cc, dgb = forward(a, w_conv, s, gamma[None], beta[None], labels[None], bias, wt)
        g8, dgb, gsq, gfc, fsq, gb, ls = backward(at, z, s, sc, sh, bb, cc, da, dgb, pall, wtb, lab, bias)
        wo, vo, wto, vto, bo, vbo, go, vgo, beo, vbeo, loss = update_all(
            lr.reshape(1), w_conv, vel_conv, g8.reshape(CIN, COUT), wsq, gsq, wt, vel_fc.T, gfc, tsq, fsq, bias, vel_bias[None], gb, ls,
            gamma[None], beta[None], vel_gamma[None], vel_beta[None], dgb)
        return (wo, go[0], beo[0], wto.T, bo[0], vo, vgo[0], vbeo[0], vto.T, vbo[0], loss[0, 0])

    return jax.shard_map(local_step, mesh=mesh, in_specs=(P('dp'),) * 3 + (P(),) * 11, out_specs=(P(),) * 11, check_vma=False)
```

```python
import functools
import jax
import jax.numpy as jnp
from jax import lax
from jax.experimental import pallas as pl
from jax.experimental.pallas import tpu as pltpu
from jax.sharding import PartitionSpec as P

BN_EPS = 1e-5
SMOOTHING = 0.1
MOMENTUM = 0.9
TRUST_COEF = 0.001
WEIGHT_DECAY = 5e-5

LANES = 128
SUB = 8
IMG = 128
POS = 49
ROWS = IMG * POS
CIN = 1024
COUT = 2048
CLASSES = 1000
KP = 1024
DEVS = 8
TOTAL = DEVS * IMG
CB = 256
HC = CB // 2
NB = COUT // CB
CH = 7
NCH = POS // CH
NT = 16
PIECES = 8
BPIECES = 4
APAD = CIN + LANES
TAIL = 3
BTAIL = 7
QR = CIN // DEVS
HALF = CIN // 2
BIG = 1792
BTILE = BIG // IMG
NBIG = ROWS // BIG
UB = 128
FB = 208
NU = CIN // UB
NF = pl.cdiv(CLASSES, FB)
LB = 256
MIB = 1024 * 1024
F32 = jnp.float32
BF16 = jnp.bfloat16
MESH = pl.DeviceIdType.MESH
XN, YN, PN = 'x', 'y', 'core'


def dot(a, b):
    return jnp.dot(a, b, preferred_element_type=F32)


def dot_t(a, b):
    return lax.dot_general(a, b, (((1,), (1,)), ((), ())), preferred_element_type=F32)


def fold(v, axis=0):
    return jnp.sum(v.reshape(v.shape[0] // SUB, SUB, v.shape[1]), axis=axis)


def rowsum(v, axis=0):
    return jnp.sum(v, axis=axis, keepdims=True)


def lanesum(v, axis=1):
    return jnp.sum(v, axis=axis, keepdims=True)


def cols(b, size=CB, at=0):
    return pl.ds(pl.multiple_of(b * CB + at, LANES), size)


def span(i, size):
    return pl.ds(pl.multiple_of(i * size, SUB), size)


def position():
    me = lax.axis_index('dp')
    return me, lax.rem(me, 2), lax.rem(me // 2, 2), me // 4


def dev(core, x, y):
    return (y * 2 + x) * 2 + core


def neighbour(name):
    me, core, x, y = position()
    flip = lambda v, k: 1 - v if k == name else v
    return dev(flip(core, PN), flip(x, XN), flip(y, YN))


def enter_all():
    me = lax.axis_index('dp')
    bar = pltpu.get_barrier_semaphore()
    for k in range(1, DEVS):
        pl.semaphore_signal(bar, inc=1, device_id=(lax.rem(me + k, DEVS),), device_id_type=MESH)
    pl.semaphore_wait(bar, DEVS - 1)


def rcopy(src, dst, send, recv, target):
    return pltpu.make_async_remote_copy(src_ref=src, dst_ref=dst, send_sem=send, recv_sem=recv, device_id=(target,), device_id_type=MESH)


def each(fn, copies):
    for c in copies:
        fn(c)


def start(c):
    c.start()


def wait(c):
    c.wait()


def wait_send(c):
    c.wait_send()


def wait_recv(c):
    c.wait_recv()


def gather_own(buf, send, recv, b, ka=0, kb=1):
    me, core, x, y = position()
    a, c = buf.at[core, y, x, :, cols(b, HC)], buf.at[core, y, x, :, cols(b, HC, HC)]
    return rcopy(a, a, send.at[ka, b], recv.at[ka, b], neighbour(YN)), rcopy(c, c, send.at[kb, b], recv.at[kb, b], neighbour(XN))


def gather_on(buf, send, recv, b, ka=2, kb=3):
    me, core, x, y = position()
    a, c = buf.at[core, :, x, :, cols(b, HC)], buf.at[core, y, :, :, cols(b, HC, HC)]
    return rcopy(a, a, send.at[ka, b], recv.at[ka, b], neighbour(XN)), rcopy(c, c, send.at[kb, b], recv.at[kb, b], neighbour(YN))


def gather_core(buf, send, recv, b, k=4):
    me, core, x, y = position()
    a = buf.at[core, :, :, :, cols(b)]
    return (rcopy(a, a, send.at[k, b], recv.at[k, b], neighbour(PN)),)


def gather_all(*a):
    return gather_own(*a) + gather_on(*a) + gather_core(*a)


def when_block(b, fn):
    @pl.when(jnp.logical_and(b >= 0, b < NB))
    def _():
        fn(b)


def stage_list(j, fns, lag=2):
    for k, fn in enumerate(fns):
        when_block(j - lag - k, fn)


def pieces():
    return [(c, y, x) for c in range(2) for y in range(2) for x in range(2)]


def softmax_terms(logits, bias, labels):
    n = logits.shape[0]
    cls = lax.broadcasted_iota(jnp.int32, (n, KP), 1)
    valid = cls < CLASSES
    lg = jnp.where(valid, logits + bias, -1e30)
    sh = lg - jnp.max(lg, axis=1, keepdims=True)
    lp = sh - jnp.log(lanesum(jnp.exp(sh)))
    lab = jnp.concatenate([labels] * (KP // LANES), axis=1)
    hit = lab == cls.astype(F32)
    tg = jnp.where(valid, SMOOTHING / CLASSES + jnp.where(hit, 1.0 - SMOOTHING, 0.0), 0.0)
    return tg * lp, (jnp.exp(lp) - tg) * (1.0 / TOTAL)


def label_rows(row):
    return jnp.broadcast_to(row.astype(F32), (IMG, IMG)).T


def set_bias(bpad, bias_ref):
    bpad[:] = jnp.zeros_like(bpad)
    bpad[:, :CLASSES] = bias_ref[:]


def fwd_kernel(a_hbm, w_ref, s_ref, g_ref, b_ref, lab_ref, bias_ref, wt_hbm,
               z_hbm, at_ref, pall_ref, lall_ref, wsq_ref, fsq_ref, wtb_hbm, da_ref, sc_ref, sh_ref, bb_ref, cc_ref, db_ref,
               abf, z0, z1, wbf, stat, pfull, lfull, pool, cnt, sx, sv, wtb, bpad, asem, zsem, wsem, osem, gs, gr, ls, lr):
    j = pl.program_id(0)
    zs = (z0, z1)
    me, core, x, y = position()
    crow = CH * IMG

    def a_copy(i):
        r = span(i, crow)
        return pltpu.make_async_copy(a_hbm.at[r, :], abf.at[r, :CIN], asem.at[i])

    def z_copy(jj, par):
        return pltpu.make_async_copy(zs[par], z_hbm.at[jj], zsem.at[par])

    def wt_view(b):
        return zs[b // 6].at[pl.ds((b % 6) * CLASSES, CLASSES), :]

    def wt_copy(b):
        return pltpu.make_async_copy(wt_hbm.at[:, pl.ds(b * CB, CB)], wt_view(b), wsem.at[b])

    def wtb_copy():
        return pltpu.make_async_copy(wtb, wtb_hbm, osem)

    def label_copy(k):
        return rcopy(lab_ref, lfull.at[core, y, x], ls.at[k], lr.at[k], lax.rem(me + k, DEVS))

    labels = [label_copy(k) for k in range(1, DEVS)]

    @pl.when(j == 0)
    def _():
        for i in range(NCH):
            a_copy(i).start()
        enter_all()
        each(start, labels)
        lfull[core, y, x] = lab_ref[:]
        wsq_ref[:] = jnp.zeros_like(wsq_ref)
        set_bias(bpad, bias_ref)

    def second(b):
        each(wait_recv, gather_own(pfull, gs, gr, b))
        each(start, gather_on(pfull, gs, gr, b))

    def third(b):
        each(wait_recv, gather_on(pfull, gs, gr, b))
        each(start, gather_core(pfull, gs, gr, b))

    def last(b):
        each(wait_recv, gather_core(pfull, gs, gr, b))
        for q, (c, py, px) in enumerate(pieces()):
            pall_ref[span(q, IMG), :] = pfull[c, py, px, :, cols(b)].astype(BF16)

    def stages():
        stage_list(j, (second, third, last))

    def step(par, do_mm, do_post):
        first = not do_post
        slot, prev = zs[par], zs[1 - par]
        if do_post:
            pl.when(j >= 2)(lambda: z_copy(j - 2, par).wait())
        if do_mm:
            wf = w_ref[:]
            wsq_ref[:] += fold(wf * wf)
            w = wf.astype(BF16)
            wbf[:] = w
            if first:
                a_copy(0).wait()
            m0 = rowsum(dot(abf[:IMG, :CIN], w)) * (1.0 / IMG)
            stat[:2 * SUB] = jnp.zeros((2 * SUB, CB), F32)
        if do_post and not do_mm:
            for b in range(6):
                wt_copy(b).start()
        if do_post:
            mean = stat[2 * SUB:2 * SUB + 1]
            inv = stat[3 * SUB:3 * SUB + 1]
            sc = g_ref[:] * inv
            sh = b_ref[:] - mean * sc
            pool[:] = jnp.zeros_like(pool)
            pc = cols(j - 1)
            cnt[:, pc] = jnp.zeros((IMG, CB), F32)
            sx[:, pc] = jnp.zeros((IMG, CB), F32)

        def post(base, n, slabs):
            nr = slice(n, n + NT)
            pa, ca, xa = pool[nr], cnt[nr, pc], sx[nr, pc]
            for p in range(slabs):
                r = pl.ds(base + p * IMG + n, NT)
                zz = prev[r, :]
                u = zz * sc + sh + s_ref[r, :].astype(F32)
                mk = u > 0
                pa = pa + jnp.maximum(u, 0.0)
                ca = ca + jnp.where(mk, 1.0, 0.0)
                xa = xa + jnp.where(mk, zz, 0.0)
            pool[nr], cnt[nr, pc], sx[nr, pc] = pa, ca, xa

        def flip(base, rows):
            r = pl.ds(base, rows)
            at_ref[:, r] = abf[r, pl.ds(pl.multiple_of(j * IMG, IMG), IMG)].astype(F32).T.astype(BF16)

        def region(base, slabs, parts):
            size = slabs * IMG // parts
            for k in range(parts):
                if do_mm:
                    r = pl.ds(base + k * size, size)
                    zc = dot(abf[r, :CIN], wbf[:])
                if do_post:
                    for n in range(k * IMG // parts, (k + 1) * IMG // parts, NT):
                        post(base, n, slabs)
                if do_mm:
                    slot[r, :] = zc
                    d = zc - m0
                    stat[:SUB] += fold(d)
                    stat[SUB:2 * SUB] += fold(d * d)

            if do_mm:
                flip(base, slabs * IMG)

        def chunk(i, carry):
            if first:
                pl.when(i > 0)(lambda: a_copy(i).wait())
            region(pl.multiple_of(i * crow, crow), CH, 4)
            return carry

        def chunk2(i, carry):
            pl.when(i == 2)(stages)
            region(pl.multiple_of(i * 2 * crow, 2 * crow), 2 * CH, PIECES)
            return carry

        if first:
            lax.fori_loop(0, NCH, chunk, 0)
        else:
            lax.fori_loop(0, NCH // 2, chunk2, 0)
            region(pl.multiple_of((jnp.minimum(me, 0) + NCH - 1) * crow, crow), CH, 4)
        if do_post:
            pfull[core, y, x, :, pc] = pool[:] * (1.0 / POS)
            sx[:, pc] = (sx[:, pc] - mean * cnt[:, pc]) * inv
            sv[:1, pc] = mean
            sv[SUB:SUB + 1, pc] = inv
            sc_ref[:, pc] = sc
            sh_ref[:, pc] = sh
            each(start, gather_own(pfull, gs, gr, j - 1))
        if do_mm:
            dm = rowsum(stat[:SUB]) * (1.0 / ROWS)
            q = rowsum(stat[SUB:2 * SUB]) * (1.0 / ROWS)
            stat[2 * SUB:2 * SUB + 1] = m0 + dm
            stat[3 * SUB:3 * SUB + 1] = lax.rsqrt(jnp.maximum(q - dm * dm, 0.0) + BN_EPS)
            z_copy(j, par).start()

    @pl.when(j == 0)
    def _():
        step(0, True, False)

    for par in range(2):
        @pl.when(jnp.logical_and(jnp.logical_and(j > 0, j < NB), lax.rem(j, 2) == par))
        def _():
            step(par, True, True)

    @pl.when(j == NB)
    def _():
        step(0, False, True)

    @pl.when(j == NB + 1)
    def _():
        z_copy(NB - 1, 1).wait()
        for b in range(6, NB):
            wt_copy(b).start()
        stages()
        wtb[CLASSES:] = jnp.zeros((KP - CLASSES, COUT), BF16)
        for b in range(NB):
            wt_copy(b).wait()
            view = wt_view(b)

            def cast(i, acc):
                w = view[span(i, 40), :]
                wtb[span(i, 40), b * CB:(b + 1) * CB] = w.astype(BF16)
                return acc + fold(w * w)
            fsq_ref[:, b * CB:(b + 1) * CB] = lax.fori_loop(0, CLASSES // 40, cast, jnp.zeros((SUB, CB), F32))
        wtb_copy().start()

    @pl.when(j == NB + 2)
    def _():
        stages()
        own = pfull[core, y, x].astype(BF16)
        lg = dot_t(own, wtb[:])
        _, dl = softmax_terms(lg, bpad[:], label_rows(lab_ref[:]))
        dlb = dl.astype(BF16)

        def col(b, carry):
            c = cols(b)
            dp = dot(dlb, wtb[:, c]) * (1.0 / POS)
            dbeta = rowsum(dp * cnt[:, c])
            dgamma = rowsum(dp * sx[:, c])
            sc = sc_ref[:, c]
            cc = -(sc * sv[SUB:SUB + 1, c]) * (dgamma * (1.0 / ROWS))
            cc_ref[:, c] = cc
            bb_ref[:, c] = -sc * (dbeta * (1.0 / ROWS)) - sv[:1, c] * cc
            da_ref[:, c] = dp * sc
            db_ref[:1, c] = dgamma
            db_ref[1:, c] = dbeta
            return carry
        lax.fori_loop(0, NB, col, 0)

    @pl.when(j == NB + TAIL)
    def _():
        stages()
        each(wait, labels)
        lall_ref[:] = lfull[:]
        wtb_copy().wait()

        def drain(b, carry):
            each(wait_send, gather_all(pfull, gs, gr, b))
            return carry
        lax.fori_loop(0, NB, drain, 0)


def whole(*shape):
    return pl.BlockSpec(shape, lambda j: (0,) * len(shape))


def struct(shape, dtype=F32):
    return jax.ShapeDtypeStruct(shape, dtype)


def fvmem(*shape):
    return pltpu.VMEM(shape, F32)


def bvmem(*shape):
    return pltpu.VMEM(shape, BF16)


def dma(*shape):
    return pltpu.SemaphoreType.DMA(shape)


HBM = pl.BlockSpec(memory_space=pl.ANY)
QUAD = (2, 2, 2)


def forward(a, w, s, gamma, beta, labels, bias, wt):
    prev = lambda j: (0, jnp.clip(j - 1, 0, NB - 1))
    cur = lambda j: (0, jnp.minimum(j, NB - 1))
    late = lambda j: (0, jnp.clip(j - 4, 0, NB - 1))
    vec, lab = (1, COUT), QUAD + (1, IMG)
    return pl.pallas_call(
        fwd_kernel,
        grid=(NB + 1 + TAIL,),
        in_specs=[HBM, pl.BlockSpec((CIN, CB), cur), pl.BlockSpec((ROWS, CB), prev), pl.BlockSpec((1, CB), prev), pl.BlockSpec((1, CB), prev),
                  whole(1, IMG), whole(1, CLASSES), HBM],
        out_specs=[HBM, pl.BlockSpec((IMG, ROWS), lambda j: (jnp.minimum(j, NB - 1), 0)), pl.BlockSpec((TOTAL, CB), late), whole(*lab),
                   whole(SUB, CB), whole(SUB, COUT), HBM, whole(IMG, COUT)] + [whole(*vec)] * 4 + [whole(2, COUT)],
        out_shape=[struct((NB, ROWS, CB)), struct((CIN, ROWS), BF16), struct((TOTAL, COUT), BF16), struct(lab, jnp.int32),
                   struct((SUB, CB)), struct((SUB, COUT)), struct((KP, COUT), BF16), struct((IMG, COUT))] + [struct(vec)] * 4 + [struct((2, COUT))],
        scratch_shapes=[bvmem(ROWS, APAD), fvmem(ROWS, CB), fvmem(ROWS, CB), bvmem(CIN, CB), fvmem(4 * SUB, CB), fvmem(*QUAD, IMG, COUT), pltpu.VMEM(lab, jnp.int32),
                        fvmem(IMG, CB), fvmem(IMG, COUT), fvmem(IMG, COUT), fvmem(2 * SUB, COUT), bvmem(KP, COUT), fvmem(1, KP),
                        dma(NCH), dma(2), dma(NB), pltpu.SemaphoreType.DMA, dma(5, NB), dma(5, NB), dma(DEVS), dma(DEVS)],
        compiler_params=pltpu.CompilerParams(vmem_limit_bytes=63 * MIB, collective_id=0, has_side_effects=True),
        cost_estimate=pl.CostEstimate(flops=2 * ROWS * CIN * COUT, bytes_accessed=2 * ROWS * COUT * 4, transcendentals=0),
        name="fwd_conv",
    )(a, w, s, gamma, beta, labels, bias, wt)


def bwd_kernel(at_hbm, z_ref, s_ref, sc_ref, sh_ref, bb_ref, cc_ref, da_ref, db_ref, pall_hbm, wtb_hbm, lab_ref, bias_ref,
               g_hbm, dbo_ref, gsq_ref, gfc_hbm, fsq_ref, gb_ref, loss_ref,
               atv, dz0, dz1, dw, rd, ha, hb, ra, rb, ka, kb, r2a, r2b, gfull, dball, bpad, ss, rs, gs, gr, bs, br, osem, isem, fsem):
    j = pl.program_id(0)
    dzs = (dz0, dz1)
    me, core, x, y = position()
    plan = pl.ds(0, COUT)
    pall = atv.at[:, plan]
    wtb = atv.at[:, pl.ds(COUT, COUT)]
    dlt = atv.at[:, pl.ds(2 * COUT, TOTAL)]

    at_copy = pltpu.make_async_copy(at_hbm, atv, isem.at[0])
    pall_copy = pltpu.make_async_copy(pall_hbm, pall, isem.at[1])
    wtb_copy = pltpu.make_async_copy(wtb_hbm, wtb, isem.at[2])
    db_copies = [rcopy(db_ref, dball.at[me], bs.at[k], br.at[k], lax.rem(me + k, DEVS)) for k in range(1, DEVS)]

    @pl.when(j == 0)
    def _():
        at_copy.start()
        enter_all()
        each(start, db_copies)
        dball[me] = db_ref[:]
        for r in (gsq_ref, fsq_ref, gb_ref, loss_ref):
            r[:] = jnp.zeros_like(r)
        set_bias(bpad, bias_ref)

    @pl.when(j == 1)
    def _():
        at_copy.wait()

    def out_copy(b):
        c = cols(b)
        return pltpu.make_async_copy(gfull.at[:, :, :, :, c], g_hbm.at[:, :, :, :, c], osem.at[b])

    def core_copy(b, k=0):
        return rcopy(dw.at[lax.rem(b, 2), span(1 - core, HALF), :], rd.at[b], ss.at[k, b], rs.at[k, b], neighbour(PN))

    def first_copies(b, k=1, m=2):
        sl = lax.rem(b, 2)
        return (rcopy(ha.at[sl, 1 - x], ra.at[b], ss.at[k, b], rs.at[k, b], neighbour(XN)),
                rcopy(hb.at[sl, 1 - y], rb.at[b], ss.at[m, b], rs.at[m, b], neighbour(YN)))

    def second_copies(b, k=3, m=4):
        sl = lax.rem(b, 2)
        return (rcopy(ka.at[sl, 1 - y], r2a.at[b], ss.at[k, b], rs.at[k, b], neighbour(YN)),
                rcopy(kb.at[sl, 1 - x], r2b.at[b], ss.at[m, b], rs.at[m, b], neighbour(XN)))

    def stage1(b):
        core_copy(b).wait()
        sl = lax.rem(b, 2)
        for q, (py, px) in enumerate((py, px) for py in range(2) for px in range(2)):
            own = pl.ds(pl.multiple_of(core * HALF + q * QR, QR), QR)
            got = slice(q * QR, (q + 1) * QR)
            ha[sl, px, py] = dw[sl, own, :HC] + rd[b, got, :HC]
            hb[sl, py, px] = dw[sl, own, HC:] + rd[b, got, HC:]
        each(start, first_copies(b))

    def stage2(b):
        sl = lax.rem(b, 2)
        each(wait, first_copies(b))
        for k in range(2):
            ka[sl, k] = ha[sl, x, k] + ra[b, k]
            kb[sl, k] = hb[sl, y, k] + rb[b, k]
        each(start, second_copies(b))

    def stage3(b):
        sl = lax.rem(b, 2)
        each(wait, second_copies(b))
        gfull[core, y, x, :, cols(b, HC)] = ka[sl, y] + r2a[b]
        gfull[core, y, x, :, cols(b, HC, HC)] = kb[sl, x] + r2b[b]
        each(start, gather_own(gfull, gs, gr, b))

    def stage4(b):
        each(wait_recv, gather_own(gfull, gs, gr, b))
        each(start, gather_on(gfull, gs, gr, b))

    def stage5(b):
        each(wait_recv, gather_on(gfull, gs, gr, b))
        each(start, gather_core(gfull, gs, gr, b))

    def stage6(b):
        each(wait_recv, gather_core(gfull, gs, gr, b))
        out_copy(b).start()
        acc = gsq_ref[:]
        for q in pieces():
            gv = gfull[q + (slice(None), cols(b))]
            acc = acc + fold(gv * gv)
        gsq_ref[:] = acc

    def stages():
        stage_list(j, (stage1, stage2, stage3, stage4, stage5, stage6))

    def step(par, do_pre, do_mm):
        slot, prev = dzs[par], dzs[1 - par]
        out = dw.at[1 - par]
        if do_pre:
            sc, sh, bb, cc = sc_ref[:], sh_ref[:], bb_ref[:], cc_ref[:]

        def pre(base, n):
            da = da_ref[n:n + NT, :]
            for p in range(CH):
                r = pl.ds(base + p * IMG + n, NT)
                zz = z_ref[r, :]
                u = zz * sc + sh + s_ref[r, :].astype(F32)
                slot[r, :] = (jnp.where(u > 0, da, 0.0) + (zz * cc + bb)).astype(BF16)

        def body(base, slabs, add):
            work = [functools.partial(pre, base + p * IMG, n) for p in range(0, slabs, CH) for n in range(0, IMG, NT)]
            size = slabs * IMG
            for k in range(BPIECES):
                m = slice(k * CIN // BPIECES, (k + 1) * CIN // BPIECES)
                if do_mm:
                    g = dot(atv[m, pl.ds(base, size)], prev[pl.ds(base, size), :])
                if do_pre:
                    n = len(work)
                    for f in work[k * n // BPIECES:(k + 1) * n // BPIECES]:
                        f()
                if do_mm:
                    out[m] = out[m] + g if add else g

        rest = NBIG * BIG
        body(rest, POS - NBIG * BTILE, False)

        def chunk(i, carry):
            base = pl.multiple_of(i * BIG, BIG)
            if do_mm:
                pl.when(i == 1)(stages)
            body(base, BTILE, True)
            return carry
        lax.fori_loop(0, NBIG, chunk, 0)
        if do_mm:
            core_copy(j - 1).start()

    @pl.when(j == 0)
    def _():
        step(0, True, False)

    for par in range(2):
        @pl.when(jnp.logical_and(jnp.logical_and(j > 0, j < NB), lax.rem(j, 2) == par))
        def _():
            step(par, True, True)

    def logits_unit(i):
        rows = span(i, LB)
        lg = dot_t(pall[rows, :], wtb[:])
        lab = jnp.concatenate([label_rows(lab_ref[i // 2, lax.rem(i, 2), k]) for k in range(2)])
        lterm, dl = softmax_terms(lg, bpad[:], lab)
        loss_ref[:] += fold(lterm)
        gb_ref[:] += fold(dl)
        dlt[:, pl.ds(pl.multiple_of(i * LB, LB), LB)] = dl.T.astype(BF16)

    def fc_copies(c):
        sl = lax.rem(c, 4)
        return [pltpu.make_async_copy(rd.at[sl * 2 + h], gfc_hbm.at[pl.ds(h * HALF, HALF), cols(c)], fsem.at[h, c]) for h in range(2)]

    def dfc_unit(c):
        pl.when(c >= 4)(lambda: each(wait, fc_copies(c - 4)))
        acc = jnp.zeros((SUB, CB), F32)
        for h in range(2):
            g = dot(dlt[pl.ds(h * HALF, HALF), :], pall[:, cols(c)])
            rd[lax.rem(c, 4) * 2 + h] = g
            acc = acc + fold(g * g)
        fsq_ref[:, cols(c)] = acc
        each(start, fc_copies(c))

    def loop(lo, hi, fn):
        def body(i, carry):
            fn(i)
            return carry
        lax.fori_loop(lo, hi, body, 0)

    @pl.when(j == NB)
    def _():
        step(0, False, True)
        pall_copy.start()
        wtb_copy.start()

    @pl.when(j > NB)
    def _():
        stages()
        k = j - NB - 1

        @pl.when(k == 0)
        def _():
            pall_copy.wait()
            wtb_copy.wait()

        loop(jnp.minimum(k * 3, 4), jnp.minimum(k * 3 + 3, 4), logits_unit)
        loop(jnp.clip(k * 3 - 3, 0, NB), jnp.clip(k * 3, 0, NB), dfc_unit)

    @pl.when(j == NB + BTAIL - 1)
    def _():
        each(wait, db_copies)
        acc = dball[0]
        for k in range(1, DEVS):
            acc = acc + dball[k]
        dbo_ref[:] = acc
        for c in range(4, NB):
            each(wait, fc_copies(c))

        def drain(b):
            each(wait_send, gather_all(gfull, gs, gr, b))
            out_copy(b).wait()
        loop(0, NB, drain)


def backward(at, z, s, sc, sh, bb, cc, da, dgb, pall, wtb, lab, bias):
    cur = lambda j: (0, jnp.minimum(j, NB - 1))
    row = pl.BlockSpec((1, CB), cur)
    pair, quad, side = (2, QR, HC), (2, 2, 2, QR, HC), (NB, QR, HC)
    return pl.pallas_call(
        bwd_kernel,
        grid=(NB + BTAIL,),
        in_specs=[HBM, pl.BlockSpec((None, ROWS, CB), lambda j: (jnp.minimum(j, NB - 1), 0, 0)), pl.BlockSpec((ROWS, CB), cur), row, row, row, row,
                  pl.BlockSpec((IMG, CB), cur), whole(2, COUT), HBM, HBM, whole(2, 2, 2, 1, IMG), whole(1, CLASSES)],
        out_specs=[HBM, whole(2, COUT), whole(SUB, CB), HBM, whole(SUB, COUT), whole(SUB, KP), whole(SUB, KP)],
        out_shape=[struct(QUAD + (QR, COUT)), struct((2, COUT)), struct((SUB, CB)), struct((KP, COUT)), struct((SUB, COUT)), struct((SUB, KP)), struct((SUB, KP))],
        scratch_shapes=[bvmem(CIN, ROWS), bvmem(ROWS, CB), bvmem(ROWS, CB), fvmem(2, CIN, CB), fvmem(NB, HALF, CB), fvmem(*quad), fvmem(*quad),
                        fvmem(NB, *pair), fvmem(NB, *pair), fvmem(2, *pair), fvmem(2, *pair), fvmem(*side), fvmem(*side),
                        fvmem(*QUAD, QR, COUT), fvmem(DEVS, 2, COUT), fvmem(1, KP),
                        dma(5, NB), dma(5, NB), dma(5, NB), dma(5, NB), dma(DEVS), dma(DEVS), dma(NB), dma(3), dma(2, NB)],
        compiler_params=pltpu.CompilerParams(vmem_limit_bytes=63 * MIB, collective_id=1, has_side_effects=True),
        cost_estimate=pl.CostEstimate(flops=2 * ROWS * CIN * COUT, bytes_accessed=2 * ROWS * COUT * 4, transcendentals=0),
        name="bwd_conv",
    )(at, z, s, sc, sh, bb, cc, da, dgb, pall, wtb, lab, bias)


def trust_of(wsq, gsq):
    wn = jnp.sqrt(lanesum(rowsum(wsq)))
    gn = jnp.sqrt(lanesum(rowsum(gsq)))
    return TRUST_COEF * wn / (gn + WEIGHT_DECAY * wn)


def update_kernel(lr_ref, w_ref, v_ref, g_ref, wsq_ref, gsq_ref, wt_ref, vt_ref, gt_ref, tsq_ref, fsq_ref, bias_ref, vbias_ref, gb_ref, ls_ref,
                  gam_ref, bet_ref, vgam_ref, vbet_ref, dgb_ref,
                  wo_ref, vo_ref, wto_ref, vto_ref, bo_ref, vbo_ref, go_ref, vgo_ref, beo_ref, vbeo_ref, loss_ref):
    j = pl.program_id(0)
    lr = lr_ref[0]

    def plain(p, v, g, po, vo):
        nv = MOMENTUM * v[:] + lr * g
        vo[:] = nv
        po[:] = p[:] - nv

    @pl.when(j == 0)
    def _():
        plain(gam_ref, vgam_ref, dgb_ref[:1], go_ref, vgo_ref)
        plain(bet_ref, vbet_ref, dgb_ref[1:], beo_ref, vbeo_ref)
        plain(bias_ref, vbias_ref, rowsum(gb_ref[:])[:, :CLASSES], bo_ref, vbo_ref)
        loss_ref[:] = lanesum(rowsum(ls_ref[:])) * (-1.0 / TOTAL)

    def lars(w_ref, v_ref, g_ref, wsq, gsq, wo, vo, rows):
        rate = jnp.broadcast_to(lr * trust_of(wsq[:], gsq[:]), (SUB, CB))

        def row(i, carry):
            for q in range(2):
                r = pl.ds(pl.multiple_of(i * 2 * SUB + q * SUB, SUB), SUB)
                for c in range(0, COUT, CB):
                    cc = slice(c, c + CB)
                    w = w_ref[r, cc]
                    nv = MOMENTUM * v_ref[r, cc] + rate * (g_ref[r, cc] + WEIGHT_DECAY * w)
                    vo[r, cc] = nv
                    wo[r, cc] = w - nv
            return carry
        lax.fori_loop(0, rows // (2 * SUB), row, 0)

    @pl.when(j < NU)
    def _():
        lars(w_ref, v_ref, g_ref, wsq_ref, gsq_ref, wo_ref, vo_ref, UB)

    @pl.when(j >= NU)
    def _():
        lars(wt_ref, vt_ref, gt_ref, tsq_ref, fsq_ref, wto_ref, vto_ref, FB)


def update_all(*args):
    conv = pl.BlockSpec((UB, COUT), lambda j: (jnp.minimum(j, NU - 1), 0))
    fc = pl.BlockSpec((FB, COUT), lambda j: (jnp.clip(j - NU, 0, NF - 1), 0))
    vec, bvec, one = (1, COUT), (1, CLASSES), (1, 1)
    vs, bs = whole(*vec), whole(*bvec)
    big, fcs = struct((CIN, COUT)), struct((CLASSES, COUT))
    return pl.pallas_call(
        update_kernel,
        grid=(NU + NF,),
        in_specs=[pl.BlockSpec(memory_space=pltpu.SMEM), conv, conv, conv, whole(SUB, CB), whole(SUB, CB), fc, fc, fc, whole(SUB, COUT), whole(SUB, COUT),
                  bs, bs, whole(SUB, KP), whole(SUB, KP), vs, vs, vs, vs, whole(2, COUT)],
        out_specs=[conv, conv, fc, fc, bs, bs, vs, vs, vs, vs, whole(*one)],
        out_shape=[big, big, fcs, fcs] + [struct(bvec)] * 2 + [struct(vec)] * 4 + [struct(one)],
        compiler_params=pltpu.CompilerParams(vmem_limit_bytes=63 * MIB),
        cost_estimate=pl.CostEstimate(flops=CIN * COUT * 16, bytes_accessed=10 * CIN * COUT * 4, transcendentals=0),
        name="update",
    )(*args)


def solution(mesh):
    def local_step(act_in, shortcut, labels, w_conv, gamma, beta, w_fc, fc_bias, vel_conv, vel_gamma, vel_beta, vel_fc, vel_bias, lr):
        a = act_in.transpose(1, 2, 0, 3).reshape(ROWS, CIN)
        s = shortcut.transpose(1, 2, 0, 3).reshape(ROWS, COUT)
        wt = w_fc.T
        bias = fc_bias[None]
        z, at, pall, lab, wsq, tsq, wtb, da, sc, sh, bb, cc, dgb = forward(a, w_conv, s, gamma[None], beta[None], labels[None], bias, wt)
        g8, dgb, gsq, gfc, fsq, gb, ls = backward(at, z, s, sc, sh, bb, cc, da, dgb, pall, wtb, lab, bias)
        wo, vo, wto, vto, bo, vbo, go, vgo, beo, vbeo, loss = update_all(
            lr.reshape(1), w_conv, vel_conv, g8.reshape(CIN, COUT), wsq, gsq, wt, vel_fc.T, gfc, tsq, fsq, bias, vel_bias[None], gb, ls,
            gamma[None], beta[None], vel_gamma[None], vel_beta[None], dgb)
        return (wo, go[0], beo[0], wto.T, bo[0], vo, vgo[0], vbeo[0], vto.T, vbo[0], loss[0, 0])

    return jax.shard_map(local_step, mesh=mesh, in_specs=(P('dp'),) * 3 + (P(),) * 11, out_specs=(P(),) * 11, check_vma=False)
```

```python
import functools
import jax
import jax.numpy as jnp
from jax import lax
from jax.experimental import pallas as pl
from jax.experimental.pallas import tpu as pltpu
from jax.sharding import PartitionSpec as P

BN_EPS = 1e-5
SMOOTHING = 0.1
MOMENTUM = 0.9
TRUST_COEF = 0.001
WEIGHT_DECAY = 5e-5

LANES = 128
SUB = 8
IMG = 128
POS = 49
ROWS = IMG * POS
CIN = 1024
COUT = 2048
CLASSES = 1000
KP = 1024
DEVS = 8
TOTAL = DEVS * IMG
CB = 256
HC = CB // 2
NB = COUT // CB
CH = 7
NCH = POS // CH
NT = 16
PIECES = 8
BPIECES = 4
APAD = CIN + LANES
TAIL = 1
NG = 6
NP = NB - NG
PG, PT = NG * CB, NP * CB
BTAIL = 7
QR = CIN // DEVS
HALF = CIN // 2
BIG = 1792
BTILE = BIG // IMG
NBIG = ROWS // BIG
UB = 128
FB = 208
NU = CIN // UB
NF = pl.cdiv(CLASSES, FB)
LB = 256
MIB = 1024 * 1024
F32 = jnp.float32
BF16 = jnp.bfloat16
MESH = pl.DeviceIdType.MESH
XN, YN, PN = 'x', 'y', 'core'


def dot(a, b):
    return jnp.dot(a, b, preferred_element_type=F32)


def dot_t(a, b):
    return lax.dot_general(a, b, (((1,), (1,)), ((), ())), preferred_element_type=F32)


def fold(v, axis=0):
    return jnp.sum(v.reshape(v.shape[0] // SUB, SUB, v.shape[1]), axis=axis)


def rowsum(v, axis=0):
    return jnp.sum(v, axis=axis, keepdims=True)


def lanesum(v, axis=1):
    return jnp.sum(v, axis=axis, keepdims=True)


def cols(b, size=CB, at=0):
    return pl.ds(pl.multiple_of(b * CB + at, LANES), size)


def span(i, size):
    return pl.ds(pl.multiple_of(i * size, SUB), size)


def position():
    me = lax.axis_index('dp')
    return me, lax.rem(me, 2), lax.rem(me // 2, 2), me // 4


def dev(core, x, y):
    return (y * 2 + x) * 2 + core


def neighbour(name):
    me, core, x, y = position()
    flip = lambda v, k: 1 - v if k == name else v
    return dev(flip(core, PN), flip(x, XN), flip(y, YN))


def enter_all():
    me = lax.axis_index('dp')
    bar = pltpu.get_barrier_semaphore()
    for k in range(1, DEVS):
        pl.semaphore_signal(bar, inc=1, device_id=(lax.rem(me + k, DEVS),), device_id_type=MESH)
    pl.semaphore_wait(bar, DEVS - 1)


def rcopy(src, dst, send, recv, target):
    return pltpu.make_async_remote_copy(src_ref=src, dst_ref=dst, send_sem=send, recv_sem=recv, device_id=(target,), device_id_type=MESH)


def each(fn, copies):
    for c in copies:
        fn(c)


def start(c):
    c.start()


def wait(c):
    c.wait()


def wait_send(c):
    c.wait_send()


def wait_recv(c):
    c.wait_recv()


def gather_own(buf, send, recv, b, ka=0, kb=1):
    me, core, x, y = position()
    a, c = buf.at[core, y, x, :, cols(b, HC)], buf.at[core, y, x, :, cols(b, HC, HC)]
    return rcopy(a, a, send.at[ka, b], recv.at[ka, b], neighbour(YN)), rcopy(c, c, send.at[kb, b], recv.at[kb, b], neighbour(XN))


def gather_on(buf, send, recv, b, ka=2, kb=3):
    me, core, x, y = position()
    a, c = buf.at[core, :, x, :, cols(b, HC)], buf.at[core, y, :, :, cols(b, HC, HC)]
    return rcopy(a, a, send.at[ka, b], recv.at[ka, b], neighbour(XN)), rcopy(c, c, send.at[kb, b], recv.at[kb, b], neighbour(YN))


def gather_core(buf, send, recv, b, k=4):
    me, core, x, y = position()
    a = buf.at[core, :, :, :, cols(b)]
    return (rcopy(a, a, send.at[k, b], recv.at[k, b], neighbour(PN)),)


def gather_all(*a):
    return gather_own(*a) + gather_on(*a) + gather_core(*a)


def stage_list(j, blocks, fns, lag=2):
    for k, fn in enumerate(fns):
        b = j - lag - k
        pl.when(jnp.logical_and(b >= 0, b < blocks))(functools.partial(fn, b))


def loop(lo, hi, fn):
    def body(i, carry):
        fn(i)
        return carry
    lax.fori_loop(lo, hi, body, 0)


def pieces():
    return [(c, y, x) for c in range(2) for y in range(2) for x in range(2)]


def softmax_terms(logits, bias, labels):
    n = logits.shape[0]
    cls = lax.broadcasted_iota(jnp.int32, (n, KP), 1)
    valid = cls < CLASSES
    lg = jnp.where(valid, logits + bias, -1e30)
    sh = lg - jnp.max(lg, axis=1, keepdims=True)
    lp = sh - jnp.log(lanesum(jnp.exp(sh)))
    lab = jnp.concatenate([labels] * (KP // LANES), axis=1)
    hit = lab == cls.astype(F32)
    tg = jnp.where(valid, SMOOTHING / CLASSES + jnp.where(hit, 1.0 - SMOOTHING, 0.0), 0.0)
    return tg * lp, (jnp.exp(lp) - tg) * (1.0 / TOTAL)


def label_rows(row):
    return jnp.broadcast_to(row.astype(F32), (IMG, IMG)).T


def set_bias(bpad, bias_ref):
    bpad[:] = jnp.zeros_like(bpad)
    bpad[:, :CLASSES] = bias_ref[:]


def fwd_kernel(a_hbm, w_ref, s_ref, g_ref, b_ref, lab_ref, bias_ref, wt_ref,
               z_hbm, at_ref, pall_ref, ptail_ref, lall_ref, wsq_ref, fsq_ref, wtb_hbm, da_ref, sc_ref, sh_ref, bb_ref, cc_ref, db_ref,
               abf, z0, z1, wbf, stat, pfull, lfull, pool, cnt, sx, sv, wtb, bpad, asem, zsem, osem, gs, gr, ls, lr):
    j = pl.program_id(0)
    zs = (z0, z1)
    me, core, x, y = position()
    crow = CH * IMG

    def a_copy(i):
        r = span(i, crow)
        return pltpu.make_async_copy(a_hbm.at[r, :], abf.at[r, :CIN], asem.at[i])

    def z_copy(jj, par):
        return pltpu.make_async_copy(zs[par], z_hbm.at[jj], zsem.at[par])

    def wtb_copy():
        return pltpu.make_async_copy(wtb, wtb_hbm, osem)

    def label_copy(k):
        return rcopy(lab_ref, lfull.at[core, y, x], ls.at[k], lr.at[k], lax.rem(me + k, DEVS))

    labels = [label_copy(k) for k in range(1, DEVS)]

    @pl.when(j == 0)
    def _():
        for i in range(NCH):
            a_copy(i).start()
        enter_all()
        each(start, labels)
        lfull[core, y, x] = lab_ref[:]
        wsq_ref[:] = jnp.zeros_like(wsq_ref)
        wtb[CLASSES:] = jnp.zeros((KP - CLASSES, COUT), BF16)
        set_bias(bpad, bias_ref)

    def second(b):
        each(wait_recv, gather_own(pfull, gs, gr, b))
        each(start, gather_on(pfull, gs, gr, b))

    def third(b):
        each(wait_recv, gather_on(pfull, gs, gr, b))
        each(start, gather_core(pfull, gs, gr, b))

    def last(b):
        each(wait_recv, gather_core(pfull, gs, gr, b))
        for q, (c, py, px) in enumerate(pieces()):
            pall_ref[span(q, IMG), :] = pfull[c, py, px, :, cols(b)].astype(BF16)

    def stages():
        stage_list(j, NG, (second, third, last))

    def step(par, do_mm, do_post):
        first = not do_post
        slot, prev = zs[par], zs[1 - par]
        if do_post:
            pl.when(j >= 2)(lambda: z_copy(j - 2, par).wait())
        if do_mm:
            wf = w_ref[:]
            wsq_ref[:] += fold(wf * wf)
            wtf = wt_ref[:]
            fsq_ref[:, cols(j)] = fold(wtf * wtf)
            wtb[:CLASSES, cols(j)] = wtf.astype(BF16)
            w = wf.astype(BF16)
            wbf[:] = w
            if first:
                a_copy(0).wait()
            m0 = rowsum(dot(abf[:IMG, :CIN], w)) * (1.0 / IMG)
            stat[:2 * SUB] = jnp.zeros((2 * SUB, CB), F32)
        if do_post and not do_mm:
            wtb_copy().start()
        if do_post:
            mean = stat[2 * SUB:2 * SUB + 1]
            inv = stat[3 * SUB:3 * SUB + 1]
            sc = g_ref[:] * inv
            sh = b_ref[:] - mean * sc
            pool[:] = jnp.zeros_like(pool)
            pc = cols(j - 1)
            cnt[:, pc] = jnp.zeros((IMG, CB), F32)
            sx[:, pc] = jnp.zeros((IMG, CB), F32)

        def post(base, n, slabs):
            nr = slice(n, n + NT)
            pa, ca, xa = pool[nr], cnt[nr, pc], sx[nr, pc]
            for p in range(slabs):
                r = pl.ds(base + p * IMG + n, NT)
                zz = prev[r, :]
                u = zz * sc + sh + s_ref[r, :].astype(F32)
                mk = u > 0
                pa = pa + jnp.maximum(u, 0.0)
                ca = ca + jnp.where(mk, 1.0, 0.0)
                xa = xa + jnp.where(mk, zz, 0.0)
            pool[nr], cnt[nr, pc], sx[nr, pc] = pa, ca, xa

        def flip(base, rows):
            r = pl.ds(base, rows)
            at_ref[:, r] = abf[r, pl.ds(pl.multiple_of(j * IMG, IMG), IMG)].astype(F32).T.astype(BF16)

        def region(base, slabs, parts):
            size = slabs * IMG // parts
            for k in range(parts):
                if do_mm:
                    r = pl.ds(base + k * size, size)
                    zc = dot(abf[r, :CIN], wbf[:])
                if do_post:
                    for n in range(k * IMG // parts, (k + 1) * IMG // parts, NT):
                        post(base, n, slabs)
                if do_mm:
                    slot[r, :] = zc
                    d = zc - m0
                    stat[:SUB] += fold(d)
                    stat[SUB:2 * SUB] += fold(d * d)

            if do_mm:
                flip(base, slabs * IMG)

        def chunk(i, carry):
            if first:
                pl.when(i > 0)(lambda: a_copy(i).wait())
            region(pl.multiple_of(i * crow, crow), CH, 4)
            return carry

        def chunk2(i, carry):
            pl.when(i == 2)(stages)
            region(pl.multiple_of(i * 2 * crow, 2 * crow), 2 * CH, PIECES)
            return carry

        if first:
            lax.fori_loop(0, NCH, chunk, 0)
        else:
            lax.fori_loop(0, NCH // 2, chunk2, 0)
            region(pl.multiple_of((jnp.minimum(me, 0) + NCH - 1) * crow, crow), CH, 4)
        if do_post:
            pfull[core, y, x, :, pc] = pool[:] * (1.0 / POS)
            sx[:, pc] = (sx[:, pc] - mean * cnt[:, pc]) * inv
            sv[:1, pc] = mean
            sv[SUB:SUB + 1, pc] = inv
            sc_ref[:, pc] = sc
            sh_ref[:, pc] = sh
            pl.when(j - 1 < NG)(lambda: each(start, gather_own(pfull, gs, gr, j - 1)))
        if do_mm:
            dm = rowsum(stat[:SUB]) * (1.0 / ROWS)
            q = rowsum(stat[SUB:2 * SUB]) * (1.0 / ROWS)
            stat[2 * SUB:2 * SUB + 1] = m0 + dm
            stat[3 * SUB:3 * SUB + 1] = lax.rsqrt(jnp.maximum(q - dm * dm, 0.0) + BN_EPS)
            z_copy(j, par).start()

    @pl.when(j == 0)
    def _():
        step(0, True, False)

    for par in range(2):
        @pl.when(jnp.logical_and(jnp.logical_and(j > 0, j < NB), lax.rem(j, 2) == par))
        def _():
            step(par, True, True)

    @pl.when(j == NB)
    def _():
        step(0, False, True)

    @pl.when(j == NB + 1)
    def _():
        stages()
        ptail_ref[:] = pfull[core, y, x, :, PG:]
        lg = dot_t(pfull[core, y, x].astype(BF16), wtb[:])
        _, dl = softmax_terms(lg, bpad[:], label_rows(lab_ref[:]))
        dlb = dl.astype(BF16)

        def col(b, carry):
            c = cols(b)
            dp = dot(dlb, wtb[:, c]) * (1.0 / POS)
            dbeta = rowsum(dp * cnt[:, c])
            dgamma = rowsum(dp * sx[:, c])
            sc = sc_ref[:, c]
            cc = -(sc * sv[SUB:SUB + 1, c]) * (dgamma * (1.0 / ROWS))
            cc_ref[:, c] = cc
            bb_ref[:, c] = -sc * (dbeta * (1.0 / ROWS)) - sv[:1, c] * cc
            da_ref[:, c] = dp * sc
            db_ref[:1, c] = dgamma
            db_ref[1:, c] = dbeta
            return carry
        lax.fori_loop(0, NB, col, 0)

        each(wait, labels)
        lall_ref[:] = lfull[:]
        wtb_copy().wait()
        z_copy(NB - 1, 1).wait()
        loop(0, NG, lambda b: each(wait_send, gather_all(pfull, gs, gr, b)))


def whole(*shape):
    return pl.BlockSpec(shape, lambda j: (0,) * len(shape))


def struct(shape, dtype=F32):
    return jax.ShapeDtypeStruct(shape, dtype)


def fvmem(*shape):
    return pltpu.VMEM(shape, F32)


def bvmem(*shape):
    return pltpu.VMEM(shape, BF16)


def dma(*shape):
    return pltpu.SemaphoreType.DMA(shape)


HBM = pl.BlockSpec(memory_space=pl.ANY)
QUAD = (2, 2, 2)


def forward(a, w, s, gamma, beta, labels, bias, wt):
    prev = lambda j: (0, jnp.clip(j - 1, 0, NB - 1))
    cur = lambda j: (0, jnp.minimum(j, NB - 1))
    late = lambda j: (0, jnp.clip(j - 4, 0, NG - 1))
    vec, lab = (1, COUT), QUAD + (1, IMG)
    return pl.pallas_call(
        fwd_kernel,
        grid=(NB + 1 + TAIL,),
        in_specs=[HBM, pl.BlockSpec((CIN, CB), cur), pl.BlockSpec((ROWS, CB), prev), pl.BlockSpec((1, CB), prev), pl.BlockSpec((1, CB), prev),
                  whole(1, IMG), whole(1, CLASSES), pl.BlockSpec((CLASSES, CB), cur)],
        out_specs=[HBM, pl.BlockSpec((IMG, ROWS), lambda j: (jnp.minimum(j, NB - 1), 0)), pl.BlockSpec((TOTAL, CB), late), whole(IMG, PT), whole(*lab),
                   whole(SUB, CB), whole(SUB, COUT), HBM, whole(IMG, COUT)] + [whole(*vec)] * 4 + [whole(2, COUT)],
        out_shape=[struct((NB, ROWS, CB)), struct((CIN, ROWS), BF16), struct((TOTAL, PG), BF16), struct((IMG, PT)), struct(lab, jnp.int32),
                   struct((SUB, CB)), struct((SUB, COUT)), struct((KP, COUT), BF16), struct((IMG, COUT))] + [struct(vec)] * 4 + [struct((2, COUT))],
        scratch_shapes=[bvmem(ROWS, APAD), fvmem(ROWS, CB), fvmem(ROWS, CB), bvmem(CIN, CB), fvmem(4 * SUB, CB), fvmem(*QUAD, IMG, COUT), pltpu.VMEM(lab, jnp.int32),
                        fvmem(IMG, CB), fvmem(IMG, COUT), fvmem(IMG, COUT), fvmem(2 * SUB, COUT), bvmem(KP, COUT), fvmem(1, KP),
                        dma(NCH), dma(2), pltpu.SemaphoreType.DMA, dma(5, NG), dma(5, NG), dma(DEVS), dma(DEVS)],
        compiler_params=pltpu.CompilerParams(vmem_limit_bytes=63 * MIB, collective_id=0, has_side_effects=True),
        cost_estimate=pl.CostEstimate(flops=2 * ROWS * CIN * COUT, bytes_accessed=2 * ROWS * COUT * 4, transcendentals=0),
        name="fwd_conv",
    )(a, w, s, gamma, beta, labels, bias, wt)


def bwd_kernel(at_hbm, z_ref, s_ref, sc_ref, sh_ref, bb_ref, cc_ref, da_ref, db_ref, pall_hbm, ptail_hbm, wtb_hbm, lab_ref, bias_ref,
               g_hbm, dbo_ref, gsq_ref, gfc_hbm, fsq_ref, gb_ref, loss_ref,
               atv, dz0, dz1, dw, rd, ha, hb, ra, rb, ka, kb, r2a, r2b, gfull, dball, ptail, bpad, ps, pr, ss, rs, gs, gr, bs, br, osem, isem, fsem):
    j = pl.program_id(0)
    dzs = (dz0, dz1)
    me, core, x, y = position()
    plan = pl.ds(0, COUT)
    pall = atv.at[:, plan]
    wtb = atv.at[:, pl.ds(COUT, COUT)]
    dlt = atv.at[:, pl.ds(2 * COUT, TOTAL)]

    at_copy = pltpu.make_async_copy(at_hbm, atv, isem.at[0])
    pall_copy = pltpu.make_async_copy(pall_hbm, atv.at[:, pl.ds(0, PG)], isem.at[1])
    wtb_copy = pltpu.make_async_copy(wtb_hbm, wtb, isem.at[2])
    ptail_copy = pltpu.make_async_copy(ptail_hbm, ptail.at[core, y, x], isem.at[3])
    db_copies = [rcopy(db_ref, dball.at[me], bs.at[k], br.at[k], lax.rem(me + k, DEVS)) for k in range(1, DEVS)]

    @pl.when(j == 0)
    def _():
        ptail_copy.start()
        at_copy.start()
        enter_all()
        ptail_copy.wait()
        for b in range(NP):
            each(start, gather_own(ptail, ps, pr, b))
        each(start, db_copies)
        dball[me] = db_ref[:]
        for r in (gsq_ref, fsq_ref, gb_ref, loss_ref):
            r[:] = jnp.zeros_like(r)
        set_bias(bpad, bias_ref)

    @pl.when(j == 1)
    def _():
        at_copy.wait()

    def out_copy(b):
        c = cols(b)
        return pltpu.make_async_copy(gfull.at[:, :, :, :, c], g_hbm.at[:, :, :, :, c], osem.at[b])

    def core_copy(b, k=0):
        return rcopy(dw.at[lax.rem(b, 2), span(1 - core, HALF), :], rd.at[b], ss.at[k, b], rs.at[k, b], neighbour(PN))

    def first_copies(b, k=1, m=2):
        sl = lax.rem(b, 2)
        return (rcopy(ha.at[sl, 1 - x], ra.at[b], ss.at[k, b], rs.at[k, b], neighbour(XN)),
                rcopy(hb.at[sl, 1 - y], rb.at[b], ss.at[m, b], rs.at[m, b], neighbour(YN)))

    def second_copies(b, k=3, m=4):
        sl = lax.rem(b, 2)
        return (rcopy(ka.at[sl, 1 - y], r2a.at[b], ss.at[k, b], rs.at[k, b], neighbour(YN)),
                rcopy(kb.at[sl, 1 - x], r2b.at[b], ss.at[m, b], rs.at[m, b], neighbour(XN)))

    def stage1(b):
        core_copy(b).wait()
        sl = lax.rem(b, 2)
        for q, (py, px) in enumerate((py, px) for py in range(2) for px in range(2)):
            own = pl.ds(pl.multiple_of(core * HALF + q * QR, QR), QR)
            got = slice(q * QR, (q + 1) * QR)
            ha[sl, px, py] = dw[sl, own, :HC] + rd[b, got, :HC]
            hb[sl, py, px] = dw[sl, own, HC:] + rd[b, got, HC:]
        each(start, first_copies(b))

    def stage2(b):
        sl = lax.rem(b, 2)
        each(wait, first_copies(b))
        for k in range(2):
            ka[sl, k] = ha[sl, x, k] + ra[b, k]
            kb[sl, k] = hb[sl, y, k] + rb[b, k]
        each(start, second_copies(b))

    def stage3(b):
        sl = lax.rem(b, 2)
        each(wait, second_copies(b))
        gfull[core, y, x, :, cols(b, HC)] = ka[sl, y] + r2a[b]
        gfull[core, y, x, :, cols(b, HC, HC)] = kb[sl, x] + r2b[b]

    def stage4(b):
        each(wait_recv, gather_own(gfull, gs, gr, b))
        each(start, gather_on(gfull, gs, gr, b))

    def stage5(b):
        each(wait_recv, gather_on(gfull, gs, gr, b))
        each(start, gather_core(gfull, gs, gr, b))

    def stage6(b):
        each(wait_recv, gather_core(gfull, gs, gr, b))
        out_copy(b).start()
        acc = gsq_ref[:]
        for q in pieces():
            gv = gfull[q + (slice(None), cols(b))]
            acc = acc + fold(gv * gv)
        gsq_ref[:] = acc

    def pooled_on():
        for b in range(NP):
            each(wait_recv, gather_own(ptail, ps, pr, b))
            each(start, gather_on(ptail, ps, pr, b))

    def pooled_core():
        for b in range(NP):
            each(wait_recv, gather_on(ptail, ps, pr, b))
            each(start, gather_core(ptail, ps, pr, b))

    def stages():
        stage_list(j, NB, (stage1, stage2, stage3))
        pl.when(j == 1)(pooled_on)
        pl.when(j == 2)(pooled_core)

    def step(par, do_pre, do_mm):
        slot, prev = dzs[par], dzs[1 - par]
        out = dw.at[1 - par]
        if do_pre:
            sc, sh, bb, cc = sc_ref[:], sh_ref[:], bb_ref[:], cc_ref[:]

        def pre(base, n):
            da = da_ref[n:n + NT, :]
            for p in range(CH):
                r = pl.ds(base + p * IMG + n, NT)
                zz = z_ref[r, :]
                u = zz * sc + sh + s_ref[r, :].astype(F32)
                slot[r, :] = (jnp.where(u > 0, da, 0.0) + (zz * cc + bb)).astype(BF16)

        def body(base, slabs, add):
            work = [functools.partial(pre, base + p * IMG, n) for p in range(0, slabs, CH) for n in range(0, IMG, NT)]
            size = slabs * IMG
            for k in range(BPIECES):
                m = slice(k * CIN // BPIECES, (k + 1) * CIN // BPIECES)
                if do_mm:
                    g = dot(atv[m, pl.ds(base, size)], prev[pl.ds(base, size), :])
                if do_pre:
                    n = len(work)
                    for f in work[k * n // BPIECES:(k + 1) * n // BPIECES]:
                        f()
                if do_mm:
                    out[m] = out[m] + g if add else g

        rest = NBIG * BIG
        body(rest, POS - NBIG * BTILE, False)

        def chunk(i, carry):
            base = pl.multiple_of(i * BIG, BIG)
            if do_mm:
                pl.when(i == 1)(stages)
            body(base, BTILE, True)
            return carry
        lax.fori_loop(0, NBIG, chunk, 0)
        if do_mm:
            core_copy(j - 1).start()

    @pl.when(j == 0)
    def _():
        step(0, True, False)

    for par in range(2):
        @pl.when(jnp.logical_and(jnp.logical_and(j > 0, j < NB), lax.rem(j, 2) == par))
        def _():
            step(par, True, True)

    def logits_unit(i):
        rows = span(i, LB)
        lg = dot_t(pall[rows, :], wtb[:])
        lab = jnp.concatenate([label_rows(lab_ref[i // 2, lax.rem(i, 2), k]) for k in range(2)])
        lterm, dl = softmax_terms(lg, bpad[:], lab)
        loss_ref[:] += fold(lterm)
        gb_ref[:] += fold(dl)
        dlt[:, pl.ds(pl.multiple_of(i * LB, LB), LB)] = dl.T.astype(BF16)

    def fc_copies(c):
        sl = lax.rem(c, 4)
        return [pltpu.make_async_copy(rd.at[sl * 2 + h], gfc_hbm.at[pl.ds(h * HALF, HALF), cols(c)], fsem.at[h, c]) for h in range(2)]

    def dfc_unit(c):
        pl.when(c >= 4)(lambda: each(wait, fc_copies(c - 4)))
        acc = jnp.zeros((SUB, CB), F32)
        for h in range(2):
            g = dot(dlt[pl.ds(h * HALF, HALF), :], pall[:, cols(c)])
            rd[lax.rem(c, 4) * 2 + h] = g
            acc = acc + fold(g * g)
        fsq_ref[:, cols(c)] = acc
        each(start, fc_copies(c))

    @pl.when(j == NB)
    def _():
        step(0, False, True)
        pall_copy.start()
        wtb_copy.start()

    @pl.when(j > NB)
    def _():
        stages()
        k = j - NB - 1
        third = lambda n: jnp.clip(3 * n, 0, NB)
        loop(jnp.where(k == 0, 0, jnp.minimum(k + NB - 3, NB)), jnp.minimum(k + NB - 2, NB), lambda b: each(start, gather_own(gfull, gs, gr, b)))
        loop(third(k - 1), third(k), stage4)
        loop(third(k - 2), third(k - 1), stage5)
        loop(third(k - 3), third(k - 2), stage6)

        @pl.when(k == 0)
        def _():
            for b in range(NP):
                each(wait_recv, gather_core(ptail, ps, pr, b))
            for q, (c, py, px) in enumerate(pieces()):
                atv[span(q, IMG), PG:COUT] = ptail[c, py, px].astype(BF16)
            pall_copy.wait()
            wtb_copy.wait()

        loop(jnp.minimum(k * 3, 4), jnp.minimum(k * 3 + 3, 4), logits_unit)
        loop(jnp.clip(k * 3 - 3, 0, NB), jnp.clip(k * 3, 0, NB), dfc_unit)

    @pl.when(j == NB + BTAIL - 1)
    def _():
        each(wait, db_copies)
        acc = dball[0]
        for k in range(1, DEVS):
            acc = acc + dball[k]
        dbo_ref[:] = acc
        for c in range(4, NB):
            each(wait, fc_copies(c))

        def drain(b):
            each(wait_send, gather_all(gfull, gs, gr, b))
            out_copy(b).wait()
        loop(0, NB, drain)
        loop(0, NP, lambda b: each(wait_send, gather_all(ptail, ps, pr, b)))


def backward(*args):
    cur = lambda j: (0, jnp.minimum(j, NB - 1))
    row = pl.BlockSpec((1, CB), cur)
    pair, quad, side = (2, QR, HC), (2, 2, 2, QR, HC), (NB, QR, HC)
    return pl.pallas_call(
        bwd_kernel,
        grid=(NB + BTAIL,),
        in_specs=[HBM, pl.BlockSpec((None, ROWS, CB), lambda j: (jnp.minimum(j, NB - 1), 0, 0)), pl.BlockSpec((ROWS, CB), cur), row, row, row, row,
                  pl.BlockSpec((IMG, CB), cur), whole(2, COUT), HBM, HBM, HBM, whole(2, 2, 2, 1, IMG), whole(1, CLASSES)],
        out_specs=[HBM, whole(2, COUT), whole(SUB, CB), HBM, whole(SUB, COUT), whole(SUB, KP), whole(SUB, KP)],
        out_shape=[struct(QUAD + (QR, COUT)), struct((2, COUT)), struct((SUB, CB)), struct((KP, COUT)), struct((SUB, COUT)), struct((SUB, KP)), struct((SUB, KP))],
        scratch_shapes=[bvmem(CIN, ROWS), bvmem(ROWS, CB), bvmem(ROWS, CB), fvmem(2, CIN, CB), fvmem(NB, HALF, CB), fvmem(*quad), fvmem(*quad),
                        fvmem(NB, *pair), fvmem(NB, *pair), fvmem(2, *pair), fvmem(2, *pair), fvmem(*side), fvmem(*side),
                        fvmem(*QUAD, QR, COUT), fvmem(DEVS, 2, COUT), fvmem(*QUAD, IMG, PT), fvmem(1, KP),
                        dma(5, NP), dma(5, NP), dma(5, NB), dma(5, NB), dma(5, NB), dma(5, NB), dma(DEVS), dma(DEVS), dma(NB), dma(4), dma(2, NB)],
        compiler_params=pltpu.CompilerParams(vmem_limit_bytes=63 * MIB, collective_id=1, has_side_effects=True),
        cost_estimate=pl.CostEstimate(flops=2 * ROWS * CIN * COUT, bytes_accessed=2 * ROWS * COUT * 4, transcendentals=0),
        name="bwd_conv",
    )(*args)


def trust_of(wsq, gsq):
    wn = jnp.sqrt(lanesum(rowsum(wsq)))
    gn = jnp.sqrt(lanesum(rowsum(gsq)))
    return TRUST_COEF * wn / (gn + WEIGHT_DECAY * wn)


def update_kernel(lr_ref, w_ref, v_ref, g_ref, wsq_ref, gsq_ref, wt_ref, vt_ref, gt_ref, tsq_ref, fsq_ref, bias_ref, vbias_ref, gb_ref, ls_ref,
                  gam_ref, bet_ref, vgam_ref, vbet_ref, dgb_ref,
                  wo_ref, vo_ref, wto_ref, vto_ref, bo_ref, vbo_ref, go_ref, vgo_ref, beo_ref, vbeo_ref, loss_ref):
    j = pl.program_id(0)
    lr = lr_ref[0]

    def plain(p, v, g, po, vo):
        nv = MOMENTUM * v[:] + lr * g
        vo[:] = nv
        po[:] = p[:] - nv

    @pl.when(j == 0)
    def _():
        plain(gam_ref, vgam_ref, dgb_ref[:1], go_ref, vgo_ref)
        plain(bet_ref, vbet_ref, dgb_ref[1:], beo_ref, vbeo_ref)
        plain(bias_ref, vbias_ref, rowsum(gb_ref[:])[:, :CLASSES], bo_ref, vbo_ref)
        loss_ref[:] = lanesum(rowsum(ls_ref[:])) * (-1.0 / TOTAL)

    def lars(w_ref, v_ref, g_ref, wsq, gsq, wo, vo, rows):
        rate = jnp.broadcast_to(lr * trust_of(wsq[:], gsq[:]), (SUB, CB))

        def row(i, carry):
            for q in range(2):
                r = pl.ds(pl.multiple_of(i * 2 * SUB + q * SUB, SUB), SUB)
                for c in range(0, COUT, CB):
                    cc = slice(c, c + CB)
                    w = w_ref[r, cc]
                    nv = MOMENTUM * v_ref[r, cc] + rate * (g_ref[r, cc] + WEIGHT_DECAY * w)
                    vo[r, cc] = nv
                    wo[r, cc] = w - nv
            return carry
        lax.fori_loop(0, rows // (2 * SUB), row, 0)

    @pl.when(j < NU)
    def _():
        lars(w_ref, v_ref, g_ref, wsq_ref, gsq_ref, wo_ref, vo_ref, UB)

    @pl.when(j >= NU)
    def _():
        lars(wt_ref, vt_ref, gt_ref, tsq_ref, fsq_ref, wto_ref, vto_ref, FB)


def update_all(*args):
    conv = pl.BlockSpec((UB, COUT), lambda j: (jnp.minimum(j, NU - 1), 0))
    fc = pl.BlockSpec((FB, COUT), lambda j: (jnp.clip(j - NU, 0, NF - 1), 0))
    vec, bvec, one = (1, COUT), (1, CLASSES), (1, 1)
    vs, bs = whole(*vec), whole(*bvec)
    big, fcs = struct((CIN, COUT)), struct((CLASSES, COUT))
    return pl.pallas_call(
        update_kernel,
        grid=(NU + NF,),
        in_specs=[pl.BlockSpec(memory_space=pltpu.SMEM), conv, conv, conv, whole(SUB, CB), whole(SUB, CB), fc, fc, fc, whole(SUB, COUT), whole(SUB, COUT),
                  bs, bs, whole(SUB, KP), whole(SUB, KP), vs, vs, vs, vs, whole(2, COUT)],
        out_specs=[conv, conv, fc, fc, bs, bs, vs, vs, vs, vs, whole(*one)],
        out_shape=[big, big, fcs, fcs] + [struct(bvec)] * 2 + [struct(vec)] * 4 + [struct(one)],
        compiler_params=pltpu.CompilerParams(vmem_limit_bytes=63 * MIB),
        cost_estimate=pl.CostEstimate(flops=CIN * COUT * 16, bytes_accessed=10 * CIN * COUT * 4, transcendentals=0),
        name="update",
    )(*args)


def solution(mesh):
    def local_step(act_in, shortcut, labels, w_conv, gamma, beta, w_fc, fc_bias, vel_conv, vel_gamma, vel_beta, vel_fc, vel_bias, lr):
        a = act_in.transpose(1, 2, 0, 3).reshape(ROWS, CIN)
        s = shortcut.transpose(1, 2, 0, 3).reshape(ROWS, COUT)
        wt = w_fc.T
        bias = fc_bias[None]
        z, at, pall, ptail, lab, wsq, tsq, wtb, da, sc, sh, bb, cc, dgb = forward(a, w_conv, s, gamma[None], beta[None], labels[None], bias, wt)
        g8, dgb, gsq, gfc, fsq, gb, ls = backward(at, z, s, sc, sh, bb, cc, da, dgb, pall, ptail, wtb, lab, bias)
        wo, vo, wto, vto, bo, vbo, go, vgo, beo, vbeo, loss = update_all(
            lr.reshape(1), w_conv, vel_conv, g8.reshape(CIN, COUT), wsq, gsq, wt, vel_fc.T, gfc, tsq, fsq, bias, vel_bias[None], gb, ls,
            gamma[None], beta[None], vel_gamma[None], vel_beta[None], dgb)
        return (wo, go[0], beo[0], wto.T, bo[0], vo, vgo[0], vbeo[0], vto.T, vbo[0], loss[0, 0])

    return jax.shard_map(local_step, mesh=mesh, in_specs=(P('dp'),) * 3 + (P(),) * 11, out_specs=(P(),) * 11, check_vma=False)
```

```python
import functools
import jax
import jax.numpy as jnp
from jax import lax
from jax.experimental import pallas as pl
from jax.experimental.pallas import tpu as pltpu
from jax.sharding import PartitionSpec as P

BN_EPS = 1e-5
SMOOTHING = 0.1
MOMENTUM = 0.9
TRUST_COEF = 0.001
WEIGHT_DECAY = 5e-5

LANES = 128
SUB = 8
IMG = 128
POS = 49
ROWS = IMG * POS
CIN = 1024
COUT = 2048
CLASSES = 1000
KP = 1024
DEVS = 8
TOTAL = DEVS * IMG
CB = 256
HC = CB // 2
NB = COUT // CB
CH = 7
NCH = POS // CH
NT = 16
PIECES = 8
BPIECES = 4
APAD = CIN + LANES
TAIL = 1
NG = 6
NP = NB - NG
PG, PT = NG * CB, NP * CB
BTAIL = 7
QR = CIN // DEVS
HALF = CIN // 2
BIG = 1792
BTILE = BIG // IMG
NBIG = ROWS // BIG
UB = 128
FB = 208
NU = CIN // UB
NF = pl.cdiv(CLASSES, FB)
LB = 256
MIB = 1024 * 1024
F32 = jnp.float32
BF16 = jnp.bfloat16
MESH = pl.DeviceIdType.MESH
XN, YN, PN = 'x', 'y', 'core'


def dot(a, b):
    return jnp.dot(a, b, preferred_element_type=F32)


def dot_t(a, b):
    return lax.dot_general(a, b, (((1,), (1,)), ((), ())), preferred_element_type=F32)


def fold(v, axis=0):
    return jnp.sum(v.reshape(v.shape[0] // SUB, SUB, v.shape[1]), axis=axis)


def rowsum(v, axis=0):
    return jnp.sum(v, axis=axis, keepdims=True)


def lanesum(v, axis=1):
    return jnp.sum(v, axis=axis, keepdims=True)


def cols(b, size=CB, at=0):
    return pl.ds(pl.multiple_of(b * CB + at, LANES), size)


def span(i, size):
    return pl.ds(pl.multiple_of(i * size, SUB), size)


def position():
    me = lax.axis_index('dp')
    return me, lax.rem(me, 2), lax.rem(me // 2, 2), me // 4


def dev(core, x, y):
    return (y * 2 + x) * 2 + core


def neighbour(name):
    me, core, x, y = position()
    flip = lambda v, k: 1 - v if k == name else v
    return dev(flip(core, PN), flip(x, XN), flip(y, YN))


def enter_all():
    me = lax.axis_index('dp')
    bar = pltpu.get_barrier_semaphore()
    for k in range(1, DEVS):
        pl.semaphore_signal(bar, inc=1, device_id=(lax.rem(me + k, DEVS),), device_id_type=MESH)
    pl.semaphore_wait(bar, DEVS - 1)


def rcopy(src, dst, send, recv, target):
    return pltpu.make_async_remote_copy(src_ref=src, dst_ref=dst, send_sem=send, recv_sem=recv, device_id=(target,), device_id_type=MESH)


def each(fn, copies):
    for c in copies:
        fn(c)


def start(c):
    c.start()


def wait(c):
    c.wait()


def wait_send(c):
    c.wait_send()


def wait_recv(c):
    c.wait_recv()


def gather_own(buf, send, recv, b, ka=0, kb=1):
    me, core, x, y = position()
    a, c = buf.at[core, y, x, :, cols(b, HC)], buf.at[core, y, x, :, cols(b, HC, HC)]
    return rcopy(a, a, send.at[ka, b], recv.at[ka, b], neighbour(YN)), rcopy(c, c, send.at[kb, b], recv.at[kb, b], neighbour(XN))


def gather_on(buf, send, recv, b, ka=2, kb=3):
    me, core, x, y = position()
    a, c = buf.at[core, :, x, :, cols(b, HC)], buf.at[core, y, :, :, cols(b, HC, HC)]
    return rcopy(a, a, send.at[ka, b], recv.at[ka, b], neighbour(XN)), rcopy(c, c, send.at[kb, b], recv.at[kb, b], neighbour(YN))


def gather_core(buf, send, recv, b, k=4):
    me, core, x, y = position()
    a = buf.at[core, :, :, :, cols(b)]
    return (rcopy(a, a, send.at[k, b], recv.at[k, b], neighbour(PN)),)


def gather_all(*a):
    return gather_own(*a) + gather_on(*a) + gather_core(*a)


def stage_list(j, blocks, fns, lag=2):
    for k, fn in enumerate(fns):
        b = j - lag - k
        pl.when(jnp.logical_and(b >= 0, b < blocks))(functools.partial(fn, b))


def loop(lo, hi, fn):
    def body(i, carry):
        fn(i)
        return carry
    lax.fori_loop(lo, hi, body, 0)


def pieces():
    return [(c, y, x) for c in range(2) for y in range(2) for x in range(2)]


def softmax_terms(logits, bias, labels):
    n = logits.shape[0]
    cls = lax.broadcasted_iota(jnp.int32, (n, KP), 1)
    valid = cls < CLASSES
    lg = jnp.where(valid, logits + bias, -1e30)
    sh = lg - jnp.max(lg, axis=1, keepdims=True)
    lp = sh - jnp.log(lanesum(jnp.exp(sh)))
    lab = jnp.concatenate([labels] * (KP // LANES), axis=1)
    hit = lab == cls.astype(F32)
    tg = jnp.where(valid, SMOOTHING / CLASSES + jnp.where(hit, 1.0 - SMOOTHING, 0.0), 0.0)
    return tg * lp, (jnp.exp(lp) - tg) * (1.0 / TOTAL)


def label_rows(row):
    return jnp.broadcast_to(row.astype(F32), (IMG, IMG)).T


def set_bias(bpad, bias_ref):
    bpad[:] = jnp.zeros_like(bpad)
    bpad[:, :CLASSES] = bias_ref[:]


def fwd_kernel(a_hbm, w_ref, s_ref, g_ref, b_ref, lab_ref, bias_ref, wt_ref,
               z_hbm, at_ref, pall_ref, ptail_ref, lall_ref, wsq_ref, fsq_ref, wtb_hbm, da_ref, sc_ref, sh_ref, bb_ref, cc_ref, db_ref,
               abf, z0, z1, wbf, stat, pfull, lfull, pool, cnt, sx, sv, wtb, bpad, asem, zsem, osem, gs, gr, ls, lr):
    j = pl.program_id(0)
    zs = (z0, z1)
    me, core, x, y = position()
    crow = CH * IMG

    def a_copy(i):
        r = span(i, crow)
        return pltpu.make_async_copy(a_hbm.at[r, :], abf.at[r, :CIN], asem.at[i])

    def z_copy(jj, par):
        return pltpu.make_async_copy(zs[par], z_hbm.at[jj], zsem.at[par])

    def wtb_copy():
        return pltpu.make_async_copy(wtb, wtb_hbm, osem)

    def label_copy(k):
        return rcopy(lab_ref, lfull.at[core, y, x], ls.at[k], lr.at[k], lax.rem(me + k, DEVS))

    labels = [label_copy(k) for k in range(1, DEVS)]

    @pl.when(j == 0)
    def _():
        for i in range(NCH):
            a_copy(i).start()
        enter_all()
        each(start, labels)
        lfull[core, y, x] = lab_ref[:]
        wsq_ref[:] = jnp.zeros_like(wsq_ref)
        wtb[CLASSES:] = jnp.zeros((KP - CLASSES, COUT), BF16)
        set_bias(bpad, bias_ref)

    def second(b):
        each(wait_recv, gather_own(pfull, gs, gr, b))
        each(start, gather_on(pfull, gs, gr, b))

    def third(b):
        each(wait_recv, gather_on(pfull, gs, gr, b))
        each(start, gather_core(pfull, gs, gr, b))

    def last(b):
        each(wait_recv, gather_core(pfull, gs, gr, b))
        for q, (c, py, px) in enumerate(pieces()):
            pall_ref[span(q, IMG), :] = pfull[c, py, px, :, cols(b)].astype(BF16)

    def stages():
        stage_list(j, NG, (second, third, last))

    def step(par, do_mm, do_post):
        first = not do_post
        slot, prev = zs[par], zs[1 - par]
        if do_post:
            pl.when(j >= 2)(lambda: z_copy(j - 2, par).wait())
        if do_mm:
            wf = w_ref[:]
            wsq_ref[:] += fold(wf * wf)
            wtf = wt_ref[:]
            fsq_ref[:, cols(j)] = fold(wtf * wtf)
            wtb[:CLASSES, cols(j)] = wtf.astype(BF16)
            w = wf.astype(BF16)
            wbf[:] = w
            if first:
                a_copy(0).wait()
            m0 = rowsum(dot(abf[:IMG, :CIN], w)) * (1.0 / IMG)
            stat[:2 * SUB] = jnp.zeros((2 * SUB, CB), F32)
        if do_post and not do_mm:
            wtb_copy().start()
        if do_post:
            mean = stat[2 * SUB:2 * SUB + 1]
            inv = stat[3 * SUB:3 * SUB + 1]
            sc = g_ref[:] * inv
            sh = b_ref[:] - mean * sc
            pool[:] = jnp.zeros_like(pool)
            pc = cols(j - 1)
            cnt[:, pc] = jnp.zeros((IMG, CB), F32)
            sx[:, pc] = jnp.zeros((IMG, CB), F32)

        def post(base, n, slabs):
            nr = slice(n, n + NT)
            pa, ca, xa = pool[nr], cnt[nr, pc], sx[nr, pc]
            for p in range(slabs):
                r = pl.ds(base + p * IMG + n, NT)
                zz = prev[r, :]
                u = zz * sc + sh + s_ref[r, :].astype(F32)
                mk = u > 0
                pa = pa + jnp.maximum(u, 0.0)
                ca = ca + jnp.where(mk, 1.0, 0.0)
                xa = xa + jnp.where(mk, zz, 0.0)
            pool[nr], cnt[nr, pc], sx[nr, pc] = pa, ca, xa

        def flip(base, rows):
            r = pl.ds(base, rows)
            at_ref[:, r] = abf[r, pl.ds(pl.multiple_of(j * IMG, IMG), IMG)].astype(F32).T.astype(BF16)

        def region(base, slabs, parts):
            size = slabs * IMG // parts
            for k in range(parts):
                if do_mm:
                    r = pl.ds(base + k * size, size)
                    zc = dot(abf[r, :CIN], wbf[:])
                if do_post:
                    for n in range(k * IMG // parts, (k + 1) * IMG // parts, NT):
                        post(base, n, slabs)
                if do_mm:
                    slot[r, :] = zc
                    d = zc - m0
                    stat[:SUB] += fold(d)
                    stat[SUB:2 * SUB] += fold(d * d)

            if do_mm:
                flip(base, slabs * IMG)

        def chunk(i, carry):
            if first:
                pl.when(i > 0)(lambda: a_copy(i).wait())
            region(pl.multiple_of(i * crow, crow), CH, 4)
            return carry

        def chunk2(i, carry):
            pl.when(i == 2)(stages)
            region(pl.multiple_of(i * 2 * crow, 2 * crow), 2 * CH, PIECES)
            return carry

        if first:
            lax.fori_loop(0, NCH, chunk, 0)
        else:
            lax.fori_loop(0, NCH // 2, chunk2, 0)
            region(pl.multiple_of((jnp.minimum(me, 0) + NCH - 1) * crow, crow), CH, 4)
        if do_post:
            pfull[core, y, x, :, pc] = pool[:] * (1.0 / POS)
            sx[:, pc] = (sx[:, pc] - mean * cnt[:, pc]) * inv
            sv[:1, pc] = mean
            sv[SUB:SUB + 1, pc] = inv
            sc_ref[:, pc] = sc
            sh_ref[:, pc] = sh
            pl.when(j - 1 < NG)(lambda: each(start, gather_own(pfull, gs, gr, j - 1)))
        if do_mm:
            dm = rowsum(stat[:SUB]) * (1.0 / ROWS)
            q = rowsum(stat[SUB:2 * SUB]) * (1.0 / ROWS)
            stat[2 * SUB:2 * SUB + 1] = m0 + dm
            stat[3 * SUB:3 * SUB + 1] = lax.rsqrt(jnp.maximum(q - dm * dm, 0.0) + BN_EPS)
            z_copy(j, par).start()

    @pl.when(j == 0)
    def _():
        step(0, True, False)

    for par in range(2):
        @pl.when(jnp.logical_and(jnp.logical_and(j > 0, j < NB), lax.rem(j, 2) == par))
        def _():
            step(par, True, True)

    @pl.when(j == NB)
    def _():
        step(0, False, True)

    @pl.when(j == NB + 1)
    def _():
        stages()
        ptail_ref[:] = pfull[core, y, x, :, PG:]
        lg = dot_t(pfull[core, y, x].astype(BF16), wtb[:])
        _, dl = softmax_terms(lg, bpad[:], label_rows(lab_ref[:]))
        dlb = dl.astype(BF16)

        def col(b, carry):
            c = cols(b)
            dp = dot(dlb, wtb[:, c]) * (1.0 / POS)
            dbeta = rowsum(dp * cnt[:, c])
            dgamma = rowsum(dp * sx[:, c])
            sc = sc_ref[:, c]
            cc = -(sc * sv[SUB:SUB + 1, c]) * (dgamma * (1.0 / ROWS))
            cc_ref[:, c] = cc
            bb_ref[:, c] = -sc * (dbeta * (1.0 / ROWS)) - sv[:1, c] * cc
            da_ref[:, c] = dp * sc
            db_ref[:1, c] = dgamma
            db_ref[1:, c] = dbeta
            return carry
        lax.fori_loop(0, NB, col, 0)

        each(wait, labels)
        lall_ref[:] = lfull[:]
        wtb_copy().wait()
        z_copy(NB - 1, 1).wait()
        loop(0, NG, lambda b: each(wait_send, gather_all(pfull, gs, gr, b)))


def whole(*shape):
    return pl.BlockSpec(shape, lambda j: (0,) * len(shape))


def struct(shape, dtype=F32):
    return jax.ShapeDtypeStruct(shape, dtype)


def fvmem(*shape):
    return pltpu.VMEM(shape, F32)


def bvmem(*shape):
    return pltpu.VMEM(shape, BF16)


def dma(*shape):
    return pltpu.SemaphoreType.DMA(shape)


HBM = pl.BlockSpec(memory_space=pl.ANY)
QUAD = (2, 2, 2)


def forward(a, w, s, gamma, beta, labels, bias, wt):
    prev = lambda j: (0, jnp.clip(j - 1, 0, NB - 1))
    cur = lambda j: (0, jnp.minimum(j, NB - 1))
    late = lambda j: (0, jnp.clip(j - 4, 0, NG - 1))
    vec, lab = (1, COUT), QUAD + (1, IMG)
    return pl.pallas_call(
        fwd_kernel,
        grid=(NB + 1 + TAIL,),
        in_specs=[HBM, pl.BlockSpec((CIN, CB), cur), pl.BlockSpec((ROWS, CB), prev), pl.BlockSpec((1, CB), prev), pl.BlockSpec((1, CB), prev),
                  whole(1, IMG), whole(1, CLASSES), pl.BlockSpec((CLASSES, CB), cur)],
        out_specs=[HBM, pl.BlockSpec((IMG, ROWS), lambda j: (jnp.minimum(j, NB - 1), 0)), pl.BlockSpec((TOTAL, CB), late), whole(IMG, PT), whole(*lab),
                   whole(SUB, CB), whole(SUB, COUT), HBM, whole(IMG, COUT)] + [whole(*vec)] * 4 + [whole(2, COUT)],
        out_shape=[struct((NB, ROWS, CB)), struct((CIN, ROWS), BF16), struct((TOTAL, PG), BF16), struct((IMG, PT)), struct(lab, jnp.int32),
                   struct((SUB, CB)), struct((SUB, COUT)), struct((KP, COUT), BF16), struct((IMG, COUT))] + [struct(vec)] * 4 + [struct((2, COUT))],
        scratch_shapes=[bvmem(ROWS, APAD), fvmem(ROWS, CB), fvmem(ROWS, CB), bvmem(CIN, CB), fvmem(4 * SUB, CB), fvmem(*QUAD, IMG, COUT), pltpu.VMEM(lab, jnp.int32),
                        fvmem(IMG, CB), fvmem(IMG, COUT), fvmem(IMG, COUT), fvmem(2 * SUB, COUT), bvmem(KP, COUT), fvmem(1, KP),
                        dma(NCH), dma(2), pltpu.SemaphoreType.DMA, dma(5, NG), dma(5, NG), dma(DEVS), dma(DEVS)],
        compiler_params=pltpu.CompilerParams(vmem_limit_bytes=63 * MIB, collective_id=0, has_side_effects=True),
        cost_estimate=pl.CostEstimate(flops=2 * ROWS * CIN * COUT, bytes_accessed=2 * ROWS * COUT * 4, transcendentals=0),
        name="fwd_conv",
    )(a, w, s, gamma, beta, labels, bias, wt)


def bwd_kernel(at_hbm, z_ref, s_ref, sc_ref, sh_ref, bb_ref, cc_ref, da_ref, db_ref, pall_hbm, ptail_hbm, wtb_hbm, lab_ref, bias_ref,
               g_hbm, dbo_ref, gsq_ref, gfc_hbm, fsq_ref, gb_ref, loss_ref,
               atv, dz0, dz1, dw, rd, ha, hb, ra, rb, ka, kb, r2a, r2b, gfull, dball, ptail, bpad, ps, pr, ss, rs, gs, gr, bs, br, osem, isem, fsem):
    j = pl.program_id(0)
    dzs = (dz0, dz1)
    me, core, x, y = position()
    plan = pl.ds(0, COUT)
    pall = atv.at[:, plan]
    wtb = atv.at[:, pl.ds(COUT, COUT)]
    dlt = atv.at[:, pl.ds(2 * COUT, TOTAL)]

    at_copy = pltpu.make_async_copy(at_hbm, atv, isem.at[0])
    pall_copy = pltpu.make_async_copy(pall_hbm, atv.at[:, pl.ds(0, PG)], isem.at[1])
    wtb_copy = pltpu.make_async_copy(wtb_hbm, wtb, isem.at[2])
    ptail_copy = pltpu.make_async_copy(ptail_hbm, ptail.at[core, y, x], isem.at[3])
    db_copies = [rcopy(db_ref, dball.at[me], bs.at[k], br.at[k], lax.rem(me + k, DEVS)) for k in range(1, DEVS)]

    @pl.when(j == 0)
    def _():
        ptail_copy.start()
        at_copy.start()
        enter_all()
        ptail_copy.wait()
        for b in range(NP):
            each(start, gather_own(ptail, ps, pr, b))
        each(start, db_copies)
        dball[me] = db_ref[:]
        for r in (gsq_ref, fsq_ref, gb_ref, loss_ref):
            r[:] = jnp.zeros_like(r)
        set_bias(bpad, bias_ref)

    @pl.when(j == 1)
    def _():
        at_copy.wait()

    def out_copy(b):
        c = cols(b)
        return pltpu.make_async_copy(gfull.at[:, :, :, :, c], g_hbm.at[:, :, :, :, c], osem.at[b])

    def core_copy(b, k=0):
        return rcopy(dw.at[lax.rem(b, 2), span(1 - core, HALF), :], rd.at[b], ss.at[k, b], rs.at[k, b], neighbour(PN))

    def first_copies(b, k=1, m=2):
        sl = lax.rem(b, 2)
        return (rcopy(ha.at[sl, 1 - x], ra.at[b], ss.at[k, b], rs.at[k, b], neighbour(XN)),
                rcopy(hb.at[sl, 1 - y], rb.at[b], ss.at[m, b], rs.at[m, b], neighbour(YN)))

    def second_copies(b, k=3, m=4):
        sl = lax.rem(b, 2)
        return (rcopy(ka.at[sl, 1 - y], r2a.at[b], ss.at[k, b], rs.at[k, b], neighbour(YN)),
                rcopy(kb.at[sl, 1 - x], r2b.at[b], ss.at[m, b], rs.at[m, b], neighbour(XN)))

    def stage1(b):
        core_copy(b).wait()
        sl = lax.rem(b, 2)
        for q, (py, px) in enumerate((py, px) for py in range(2) for px in range(2)):
            own = pl.ds(pl.multiple_of(core * HALF + q * QR, QR), QR)
            got = slice(q * QR, (q + 1) * QR)
            ha[sl, px, py] = dw[sl, own, :HC] + rd[b, got, :HC]
            hb[sl, py, px] = dw[sl, own, HC:] + rd[b, got, HC:]
        each(start, first_copies(b))

    def stage2(b):
        sl = lax.rem(b, 2)
        each(wait, first_copies(b))
        for k in range(2):
            ka[sl, k] = ha[sl, x, k] + ra[b, k]
            kb[sl, k] = hb[sl, y, k] + rb[b, k]
        each(start, second_copies(b))

    def stage3(b):
        sl = lax.rem(b, 2)
        each(wait, second_copies(b))
        gfull[core, y, x, :, cols(b, HC)] = ka[sl, y] + r2a[b]
        gfull[core, y, x, :, cols(b, HC, HC)] = kb[sl, x] + r2b[b]
        each(start, gather_own(gfull, gs, gr, b))

    def stage4(b):
        each(wait_recv, gather_own(gfull, gs, gr, b))
        each(start, gather_on(gfull, gs, gr, b))

    def stage5(b):
        each(wait_recv, gather_on(gfull, gs, gr, b))
        each(start, gather_core(gfull, gs, gr, b))

    def stage6(b):
        each(wait_recv, gather_core(gfull, gs, gr, b))
        out_copy(b).start()
        acc = gsq_ref[:]
        for q in pieces():
            gv = gfull[q + (slice(None), cols(b))]
            acc = acc + fold(gv * gv)
        gsq_ref[:] = acc

    def pooled_on():
        for b in range(NP):
            each(wait_recv, gather_own(ptail, ps, pr, b))
            each(start, gather_on(ptail, ps, pr, b))

    def pooled_core():
        for b in range(NP):
            each(wait_recv, gather_on(ptail, ps, pr, b))
            each(start, gather_core(ptail, ps, pr, b))

    def stages():
        stage_list(j, NB, (stage1, stage2, stage3, stage4, stage5, stage6))
        pl.when(j == 1)(pooled_on)
        pl.when(j == 2)(pooled_core)

    def step(par, do_pre, do_mm):
        slot, prev = dzs[par], dzs[1 - par]
        out = dw.at[1 - par]
        if do_pre:
            sc, sh, bb, cc = sc_ref[:], sh_ref[:], bb_ref[:], cc_ref[:]

        def pre(base, n):
            da = da_ref[n:n + NT, :]
            for p in range(CH):
                r = pl.ds(base + p * IMG + n, NT)
                zz = z_ref[r, :]
                u = zz * sc + sh + s_ref[r, :].astype(F32)
                slot[r, :] = (jnp.where(u > 0, da, 0.0) + (zz * cc + bb)).astype(BF16)

        def body(base, slabs, add):
            work = [functools.partial(pre, base + p * IMG, n) for p in range(0, slabs, CH) for n in range(0, IMG, NT)]
            size = slabs * IMG
            for k in range(BPIECES):
                m = slice(k * CIN // BPIECES, (k + 1) * CIN // BPIECES)
                if do_mm:
                    g = dot(atv[m, pl.ds(base, size)], prev[pl.ds(base, size), :])
                if do_pre:
                    n = len(work)
                    for f in work[k * n // BPIECES:(k + 1) * n // BPIECES]:
                        f()
                if do_mm:
                    out[m] = out[m] + g if add else g

        rest = NBIG * BIG
        body(rest, POS - NBIG * BTILE, False)

        def chunk(i, carry):
            base = pl.multiple_of(i * BIG, BIG)
            if do_mm:
                pl.when(i == 1)(stages)
            body(base, BTILE, True)
            return carry
        lax.fori_loop(0, NBIG, chunk, 0)
        if do_mm:
            core_copy(j - 1).start()

    @pl.when(j == 0)
    def _():
        step(0, True, False)

    for par in range(2):
        @pl.when(jnp.logical_and(jnp.logical_and(j > 0, j < NB), lax.rem(j, 2) == par))
        def _():
            step(par, True, True)

    def logits_unit(i):
        rows = span(i, LB)
        lg = dot_t(pall[rows, :], wtb[:])
        lab = jnp.concatenate([label_rows(lab_ref[i // 2, lax.rem(i, 2), k]) for k in range(2)])
        lterm, dl = softmax_terms(lg, bpad[:], lab)
        loss_ref[:] += fold(lterm)
        gb_ref[:] += fold(dl)
        dlt[:, pl.ds(pl.multiple_of(i * LB, LB), LB)] = dl.T.astype(BF16)

    def fc_copies(c):
        sl = lax.rem(c, 4)
        return [pltpu.make_async_copy(rd.at[sl * 2 + h], gfc_hbm.at[pl.ds(h * HALF, HALF), cols(c)], fsem.at[h, c]) for h in range(2)]

    def dfc_unit(c):
        pl.when(c >= 4)(lambda: each(wait, fc_copies(c - 4)))
        acc = jnp.zeros((SUB, CB), F32)
        for h in range(2):
            g = dot(dlt[pl.ds(h * HALF, HALF), :], pall[:, cols(c)])
            rd[lax.rem(c, 4) * 2 + h] = g
            acc = acc + fold(g * g)
        fsq_ref[:, cols(c)] = acc
        each(start, fc_copies(c))

    @pl.when(j == NB)
    def _():
        step(0, False, True)
        pall_copy.start()
        wtb_copy.start()

    @pl.when(j > NB)
    def _():
        stages()
        k = j - NB - 1

        @pl.when(k == 0)
        def _():
            for b in range(NP):
                each(wait_recv, gather_core(ptail, ps, pr, b))
            for q, (c, py, px) in enumerate(pieces()):
                atv[span(q, IMG), PG:COUT] = ptail[c, py, px].astype(BF16)
            pall_copy.wait()
            wtb_copy.wait()

        loop(jnp.minimum(k * 3, 4), jnp.minimum(k * 3 + 3, 4), logits_unit)
        loop(jnp.clip(k * 3 - 3, 0, NB), jnp.clip(k * 3, 0, NB), dfc_unit)

    @pl.when(j == NB + BTAIL - 1)
    def _():
        each(wait, db_copies)
        acc = dball[0]
        for k in range(1, DEVS):
            acc = acc + dball[k]
        dbo_ref[:] = acc
        for c in range(4, NB):
            each(wait, fc_copies(c))

        def drain(b):
            each(wait_send, gather_all(gfull, gs, gr, b))
            out_copy(b).wait()
        loop(0, NB, drain)
        loop(0, NP, lambda b: each(wait_send, gather_all(ptail, ps, pr, b)))


def backward(*args):
    cur = lambda j: (0, jnp.minimum(j, NB - 1))
    row = pl.BlockSpec((1, CB), cur)
    pair, quad, side = (2, QR, HC), (2, 2, 2, QR, HC), (NB, QR, HC)
    return pl.pallas_call(
        bwd_kernel,
        grid=(NB + BTAIL,),
        in_specs=[HBM, pl.BlockSpec((None, ROWS, CB), lambda j: (jnp.minimum(j, NB - 1), 0, 0)), pl.BlockSpec((ROWS, CB), cur), row, row, row, row,
                  pl.BlockSpec((IMG, CB), cur), whole(2, COUT), HBM, HBM, HBM, whole(2, 2, 2, 1, IMG), whole(1, CLASSES)],
        out_specs=[HBM, whole(2, COUT), whole(SUB, CB), HBM, whole(SUB, COUT), whole(SUB, KP), whole(SUB, KP)],
        out_shape=[struct(QUAD + (QR, COUT)), struct((2, COUT)), struct((SUB, CB)), struct((KP, COUT)), struct((SUB, COUT)), struct((SUB, KP)), struct((SUB, KP))],
        scratch_shapes=[bvmem(CIN, ROWS), bvmem(ROWS, CB), bvmem(ROWS, CB), fvmem(2, CIN, CB), fvmem(NB, HALF, CB), fvmem(*quad), fvmem(*quad),
                        fvmem(NB, *pair), fvmem(NB, *pair), fvmem(2, *pair), fvmem(2, *pair), fvmem(*side), fvmem(*side),
                        fvmem(*QUAD, QR, COUT), fvmem(DEVS, 2, COUT), fvmem(*QUAD, IMG, PT), fvmem(1, KP),
                        dma(5, NP), dma(5, NP), dma(5, NB), dma(5, NB), dma(5, NB), dma(5, NB), dma(DEVS), dma(DEVS), dma(NB), dma(4), dma(2, NB)],
        compiler_params=pltpu.CompilerParams(vmem_limit_bytes=63 * MIB, collective_id=1, has_side_effects=True),
        cost_estimate=pl.CostEstimate(flops=2 * ROWS * CIN * COUT, bytes_accessed=2 * ROWS * COUT * 4, transcendentals=0),
        name="bwd_conv",
    )(*args)


def trust_of(wsq, gsq):
    wn = jnp.sqrt(lanesum(rowsum(wsq)))
    gn = jnp.sqrt(lanesum(rowsum(gsq)))
    return TRUST_COEF * wn / (gn + WEIGHT_DECAY * wn)


def update_kernel(lr_ref, w_ref, v_ref, g_ref, wsq_ref, gsq_ref, wt_ref, vt_ref, gt_ref, tsq_ref, fsq_ref, bias_ref, vbias_ref, gb_ref, ls_ref,
                  gam_ref, bet_ref, vgam_ref, vbet_ref, dgb_ref,
                  wo_ref, vo_ref, wto_ref, vto_ref, bo_ref, vbo_ref, go_ref, vgo_ref, beo_ref, vbeo_ref, loss_ref):
    j = pl.program_id(0)
    lr = lr_ref[0]

    def plain(p, v, g, po, vo):
        nv = MOMENTUM * v[:] + lr * g
        vo[:] = nv
        po[:] = p[:] - nv

    @pl.when(j == 0)
    def _():
        plain(gam_ref, vgam_ref, dgb_ref[:1], go_ref, vgo_ref)
        plain(bet_ref, vbet_ref, dgb_ref[1:], beo_ref, vbeo_ref)
        plain(bias_ref, vbias_ref, rowsum(gb_ref[:])[:, :CLASSES], bo_ref, vbo_ref)
        loss_ref[:] = lanesum(rowsum(ls_ref[:])) * (-1.0 / TOTAL)

    def lars(w_ref, v_ref, g_ref, wsq, gsq, wo, vo, rows):
        rate = jnp.broadcast_to(lr * trust_of(wsq[:], gsq[:]), (SUB, CB))

        def row(i, carry):
            for q in range(2):
                r = pl.ds(pl.multiple_of(i * 2 * SUB + q * SUB, SUB), SUB)
                for c in range(0, COUT, CB):
                    cc = slice(c, c + CB)
                    w = w_ref[r, cc]
                    nv = MOMENTUM * v_ref[r, cc] + rate * (g_ref[r, cc] + WEIGHT_DECAY * w)
                    vo[r, cc] = nv
                    wo[r, cc] = w - nv
            return carry
        lax.fori_loop(0, rows // (2 * SUB), row, 0)

    @pl.when(j < NU)
    def _():
        lars(w_ref, v_ref, g_ref, wsq_ref, gsq_ref, wo_ref, vo_ref, UB)

    @pl.when(j >= NU)
    def _():
        lars(wt_ref, vt_ref, gt_ref, tsq_ref, fsq_ref, wto_ref, vto_ref, FB)


def update_all(*args):
    conv = pl.BlockSpec((UB, COUT), lambda j: (jnp.minimum(j, NU - 1), 0))
    fc = pl.BlockSpec((FB, COUT), lambda j: (jnp.clip(j - NU, 0, NF - 1), 0))
    vec, bvec, one = (1, COUT), (1, CLASSES), (1, 1)
    vs, bs = whole(*vec), whole(*bvec)
    big, fcs = struct((CIN, COUT)), struct((CLASSES, COUT))
    return pl.pallas_call(
        update_kernel,
        grid=(NU + NF,),
        in_specs=[pl.BlockSpec(memory_space=pltpu.SMEM), conv, conv, conv, whole(SUB, CB), whole(SUB, CB), fc, fc, fc, whole(SUB, COUT), whole(SUB, COUT),
                  bs, bs, whole(SUB, KP), whole(SUB, KP), vs, vs, vs, vs, whole(2, COUT)],
        out_specs=[conv, conv, fc, fc, bs, bs, vs, vs, vs, vs, whole(*one)],
        out_shape=[big, big, fcs, fcs] + [struct(bvec)] * 2 + [struct(vec)] * 4 + [struct(one)],
        compiler_params=pltpu.CompilerParams(vmem_limit_bytes=63 * MIB),
        cost_estimate=pl.CostEstimate(flops=CIN * COUT * 16, bytes_accessed=10 * CIN * COUT * 4, transcendentals=0),
        name="update",
    )(*args)


def solution(mesh):
    def local_step(act_in, shortcut, labels, w_conv, gamma, beta, w_fc, fc_bias, vel_conv, vel_gamma, vel_beta, vel_fc, vel_bias, lr):
        a = act_in.transpose(1, 2, 0, 3).reshape(ROWS, CIN)
        s = shortcut.transpose(1, 2, 0, 3).reshape(ROWS, COUT)
        wt = w_fc.T
        bias = fc_bias[None]
        z, at, pall, ptail, lab, wsq, tsq, wtb, da, sc, sh, bb, cc, dgb = forward(a, w_conv, s, gamma[None], beta[None], labels[None], bias, wt)
        g8, dgb, gsq, gfc, fsq, gb, ls = backward(at, z, s, sc, sh, bb, cc, da, dgb, pall, ptail, wtb, lab, bias)
        wo, vo, wto, vto, bo, vbo, go, vgo, beo, vbeo, loss = update_all(
            lr.reshape(1), w_conv, vel_conv, g8.reshape(CIN, COUT), wsq, gsq, wt, vel_fc.T, gfc, tsq, fsq, bias, vel_bias[None], gb, ls,
            gamma[None], beta[None], vel_gamma[None], vel_beta[None], dgb)
        return (wo, go[0], beo[0], wto.T, bo[0], vo, vgo[0], vbeo[0], vto.T, vbo[0], loss[0, 0])

    return jax.shard_map(local_step, mesh=mesh, in_specs=(P('dp'),) * 3 + (P(),) * 11, out_specs=(P(),) * 11, check_vma=False)
```

```python
import functools
import jax
import jax.numpy as jnp
from jax import lax
from jax.experimental import pallas as pl
from jax.experimental.pallas import tpu as pltpu
from jax.sharding import PartitionSpec as P

BN_EPS = 1e-5
SMOOTHING = 0.1
MOMENTUM = 0.9
TRUST_COEF = 0.001
WEIGHT_DECAY = 5e-5

LANES = 128
SUB = 8
IMG = 128
POS = 49
ROWS = IMG * POS
CIN = 1024
COUT = 2048
CLASSES = 1000
KP = 1024
DEVS = 8
TOTAL = DEVS * IMG
CB = 256
HC = CB // 2
NB = COUT // CB
CH = 7
NCH = POS // CH
NT = 16
PIECES = 8
BPIECES = 4
APAD = CIN + LANES
TAIL = 1
NG = 6
NP = NB - NG
PG, PT = NG * CB, NP * CB
LAGS = (2, 3, 4, 6, 8, 9)
BTAIL = LAGS[-1]
QR = CIN // DEVS
HALF = CIN // 2
BIG = 1792
BTILE = BIG // IMG
NBIG = ROWS // BIG
UB = 128
FB = 208
NU = CIN // UB
NF = pl.cdiv(CLASSES, FB)
LB = 256
MIB = 1024 * 1024
F32 = jnp.float32
BF16 = jnp.bfloat16
MESH = pl.DeviceIdType.MESH
XN, YN, PN = 'x', 'y', 'core'


def dot(a, b):
    return jnp.dot(a, b, preferred_element_type=F32)


def dot_t(a, b):
    return lax.dot_general(a, b, (((1,), (1,)), ((), ())), preferred_element_type=F32)


def fold(v, axis=0):
    return jnp.sum(v.reshape(v.shape[0] // SUB, SUB, v.shape[1]), axis=axis)


def rowsum(v, axis=0):
    return jnp.sum(v, axis=axis, keepdims=True)


def lanesum(v, axis=1):
    return jnp.sum(v, axis=axis, keepdims=True)


def cols(b, size=CB, at=0):
    return pl.ds(pl.multiple_of(b * CB + at, LANES), size)


def span(i, size):
    return pl.ds(pl.multiple_of(i * size, SUB), size)


def position():
    me = lax.axis_index('dp')
    return me, lax.rem(me, 2), lax.rem(me // 2, 2), me // 4


def dev(core, x, y):
    return (y * 2 + x) * 2 + core


def neighbour(name):
    me, core, x, y = position()
    flip = lambda v, k: 1 - v if k == name else v
    return dev(flip(core, PN), flip(x, XN), flip(y, YN))


def enter_all():
    me = lax.axis_index('dp')
    bar = pltpu.get_barrier_semaphore()
    for k in range(1, DEVS):
        pl.semaphore_signal(bar, inc=1, device_id=(lax.rem(me + k, DEVS),), device_id_type=MESH)
    pl.semaphore_wait(bar, DEVS - 1)


def rcopy(src, dst, send, recv, target):
    return pltpu.make_async_remote_copy(src_ref=src, dst_ref=dst, send_sem=send, recv_sem=recv, device_id=(target,), device_id_type=MESH)


def each(fn, copies):
    for c in copies:
        fn(c)


def start(c):
    c.start()


def wait(c):
    c.wait()


def wait_send(c):
    c.wait_send()


def wait_recv(c):
    c.wait_recv()


def gather_own(buf, send, recv, b, ka=0, kb=1):
    me, core, x, y = position()
    a, c = buf.at[core, y, x, :, cols(b, HC)], buf.at[core, y, x, :, cols(b, HC, HC)]
    return rcopy(a, a, send.at[ka, b], recv.at[ka, b], neighbour(YN)), rcopy(c, c, send.at[kb, b], recv.at[kb, b], neighbour(XN))


def gather_on(buf, send, recv, b, ka=2, kb=3):
    me, core, x, y = position()
    a, c = buf.at[core, :, x, :, cols(b, HC)], buf.at[core, y, :, :, cols(b, HC, HC)]
    return rcopy(a, a, send.at[ka, b], recv.at[ka, b], neighbour(XN)), rcopy(c, c, send.at[kb, b], recv.at[kb, b], neighbour(YN))


def gather_core(buf, send, recv, b, k=4):
    me, core, x, y = position()
    a = buf.at[core, :, :, :, cols(b)]
    return (rcopy(a, a, send.at[k, b], recv.at[k, b], neighbour(PN)),)


def gather_all(*a):
    return gather_own(*a) + gather_on(*a) + gather_core(*a)


def stage_list(j, blocks, fns, lags):
    for fn, lag in zip(fns, lags):
        b = j - lag
        pl.when(jnp.logical_and(b >= 0, b < blocks))(functools.partial(fn, b))


def loop(lo, hi, fn):
    def body(i, carry):
        fn(i)
        return carry
    lax.fori_loop(lo, hi, body, 0)


def pieces():
    return [(c, y, x) for c in range(2) for y in range(2) for x in range(2)]


def softmax_terms(logits, bias, labels):
    n = logits.shape[0]
    cls = lax.broadcasted_iota(jnp.int32, (n, KP), 1)
    valid = cls < CLASSES
    lg = jnp.where(valid, logits + bias, -1e30)
    sh = lg - jnp.max(lg, axis=1, keepdims=True)
    lp = sh - jnp.log(lanesum(jnp.exp(sh)))
    lab = jnp.concatenate([labels] * (KP // LANES), axis=1)
    hit = lab == cls.astype(F32)
    tg = jnp.where(valid, SMOOTHING / CLASSES + jnp.where(hit, 1.0 - SMOOTHING, 0.0), 0.0)
    return tg * lp, (jnp.exp(lp) - tg) * (1.0 / TOTAL)


def label_rows(row):
    return jnp.broadcast_to(row.astype(F32), (IMG, IMG)).T


def set_bias(bpad, bias_ref):
    bpad[:] = jnp.zeros_like(bpad)
    bpad[:, :CLASSES] = bias_ref[:]


def fwd_kernel(a_hbm, w_ref, s_ref, g_ref, b_ref, lab_ref, bias_ref, wt_ref,
               z_hbm, at_ref, pall_ref, ptail_ref, lall_ref, wsq_ref, fsq_ref, wtb_hbm, da_ref, sc_ref, sh_ref, bb_ref, cc_ref, db_ref,
               abf, z0, z1, wbf, stat, pfull, lfull, pool, cnt, sx, sv, wtb, bpad, asem, zsem, osem, gs, gr, ls, lr):
    j = pl.program_id(0)
    zs = (z0, z1)
    me, core, x, y = position()
    crow = CH * IMG

    def a_copy(i):
        r = span(i, crow)
        return pltpu.make_async_copy(a_hbm.at[r, :], abf.at[r, :CIN], asem.at[i])

    def z_copy(jj, par):
        return pltpu.make_async_copy(zs[par], z_hbm.at[jj], zsem.at[par])

    def wtb_copy():
        return pltpu.make_async_copy(wtb, wtb_hbm, osem)

    def label_copy(k):
        return rcopy(lab_ref, lfull.at[core, y, x], ls.at[k], lr.at[k], lax.rem(me + k, DEVS))

    labels = [label_copy(k) for k in range(1, DEVS)]

    @pl.when(j == 0)
    def _():
        for i in range(NCH):
            a_copy(i).start()
        enter_all()
        each(start, labels)
        lfull[core, y, x] = lab_ref[:]
        wsq_ref[:] = jnp.zeros_like(wsq_ref)
        wtb[CLASSES:] = jnp.zeros((KP - CLASSES, COUT), BF16)
        set_bias(bpad, bias_ref)

    def second(b):
        each(wait_recv, gather_own(pfull, gs, gr, b))
        each(start, gather_on(pfull, gs, gr, b))

    def third(b):
        each(wait_recv, gather_on(pfull, gs, gr, b))
        each(start, gather_core(pfull, gs, gr, b))

    def last(b):
        each(wait_recv, gather_core(pfull, gs, gr, b))
        for q, (c, py, px) in enumerate(pieces()):
            pall_ref[span(q, IMG), :] = pfull[c, py, px, :, cols(b)].astype(BF16)

    def stages():
        stage_list(j, NG, (second, third, last), (2, 3, 4))

    def step(par, do_mm, do_post):
        first = not do_post
        slot, prev = zs[par], zs[1 - par]
        if do_post:
            pl.when(j >= 2)(lambda: z_copy(j - 2, par).wait())
        if do_mm:
            wf = w_ref[:]
            wsq_ref[:] += fold(wf * wf)
            wtf = wt_ref[:]
            fsq_ref[:, cols(j)] = fold(wtf * wtf)
            wtb[:CLASSES, cols(j)] = wtf.astype(BF16)
            w = wf.astype(BF16)
            wbf[:] = w
            if first:
                a_copy(0).wait()
            m0 = rowsum(dot(abf[:IMG, :CIN], w)) * (1.0 / IMG)
            stat[:2 * SUB] = jnp.zeros((2 * SUB, CB), F32)
        if do_post and not do_mm:
            wtb_copy().start()
        if do_post:
            mean = stat[2 * SUB:2 * SUB + 1]
            inv = stat[3 * SUB:3 * SUB + 1]
            sc = g_ref[:] * inv
            sh = b_ref[:] - mean * sc
            pool[:] = jnp.zeros_like(pool)
            pc = cols(j - 1)
            cnt[:, pc] = jnp.zeros((IMG, CB), F32)
            sx[:, pc] = jnp.zeros((IMG, CB), F32)

        def post(base, n, slabs):
            nr = slice(n, n + NT)
            pa, ca, xa = pool[nr], cnt[nr, pc], sx[nr, pc]
            for p in range(slabs):
                r = pl.ds(base + p * IMG + n, NT)
                zz = prev[r, :]
                u = zz * sc + sh + s_ref[r, :].astype(F32)
                mk = u > 0
                pa = pa + jnp.maximum(u, 0.0)
                ca = ca + jnp.where(mk, 1.0, 0.0)
                xa = xa + jnp.where(mk, zz, 0.0)
            pool[nr], cnt[nr, pc], sx[nr, pc] = pa, ca, xa

        def flip(base, rows):
            r = pl.ds(base, rows)
            at_ref[:, r] = abf[r, pl.ds(pl.multiple_of(j * IMG, IMG), IMG)].astype(F32).T.astype(BF16)

        def region(base, slabs, parts):
            size = slabs * IMG // parts
            for k in range(parts):
                if do_mm:
                    r = pl.ds(base + k * size, size)
                    zc = dot(abf[r, :CIN], wbf[:])
                if do_post:
                    for n in range(k * IMG // parts, (k + 1) * IMG // parts, NT):
                        post(base, n, slabs)
                if do_mm:
                    slot[r, :] = zc
                    d = zc - m0
                    stat[:SUB] += fold(d)
                    stat[SUB:2 * SUB] += fold(d * d)

            if do_mm:
                flip(base, slabs * IMG)

        def chunk(i, carry):
            if first:
                pl.when(i > 0)(lambda: a_copy(i).wait())
            region(pl.multiple_of(i * crow, crow), CH, 4)
            return carry

        def chunk2(i, carry):
            pl.when(i == 2)(stages)
            region(pl.multiple_of(i * 2 * crow, 2 * crow), 2 * CH, PIECES)
            return carry

        if first:
            lax.fori_loop(0, NCH, chunk, 0)
        else:
            lax.fori_loop(0, NCH // 2, chunk2, 0)
            region(pl.multiple_of((jnp.minimum(me, 0) + NCH - 1) * crow, crow), CH, 4)
        if do_post:
            pfull[core, y, x, :, pc] = pool[:] * (1.0 / POS)
            sx[:, pc] = (sx[:, pc] - mean * cnt[:, pc]) * inv
            sv[:1, pc] = mean
            sv[SUB:SUB + 1, pc] = inv
            sc_ref[:, pc] = sc
            sh_ref[:, pc] = sh
            pl.when(j - 1 < NG)(lambda: each(start, gather_own(pfull, gs, gr, j - 1)))
        if do_mm:
            dm = rowsum(stat[:SUB]) * (1.0 / ROWS)
            q = rowsum(stat[SUB:2 * SUB]) * (1.0 / ROWS)
            stat[2 * SUB:2 * SUB + 1] = m0 + dm
            stat[3 * SUB:3 * SUB + 1] = lax.rsqrt(jnp.maximum(q - dm * dm, 0.0) + BN_EPS)
            z_copy(j, par).start()

    @pl.when(j == 0)
    def _():
        step(0, True, False)

    for par in range(2):
        @pl.when(jnp.logical_and(jnp.logical_and(j > 0, j < NB), lax.rem(j, 2) == par))
        def _():
            step(par, True, True)

    @pl.when(j == NB)
    def _():
        step(0, False, True)

    @pl.when(j == NB + 1)
    def _():
        stages()
        ptail_ref[:] = pfull[core, y, x, :, PG:]
        lg = dot_t(pfull[core, y, x].astype(BF16), wtb[:])
        _, dl = softmax_terms(lg, bpad[:], label_rows(lab_ref[:]))
        dlb = dl.astype(BF16)

        def col(b, carry):
            c = cols(b)
            dp = dot(dlb, wtb[:, c]) * (1.0 / POS)
            dbeta = rowsum(dp * cnt[:, c])
            dgamma = rowsum(dp * sx[:, c])
            sc = sc_ref[:, c]
            cc = -(sc * sv[SUB:SUB + 1, c]) * (dgamma * (1.0 / ROWS))
            cc_ref[:, c] = cc
            bb_ref[:, c] = -sc * (dbeta * (1.0 / ROWS)) - sv[:1, c] * cc
            da_ref[:, c] = dp * sc
            db_ref[:1, c] = dgamma
            db_ref[1:, c] = dbeta
            return carry
        lax.fori_loop(0, NB, col, 0)

        each(wait, labels)
        lall_ref[:] = lfull[:]
        wtb_copy().wait()
        z_copy(NB - 1, 1).wait()
        loop(0, NG, lambda b: each(wait_send, gather_all(pfull, gs, gr, b)))


def whole(*shape):
    return pl.BlockSpec(shape, lambda j: (0,) * len(shape))


def struct(shape, dtype=F32):
    return jax.ShapeDtypeStruct(shape, dtype)


def fvmem(*shape):
    return pltpu.VMEM(shape, F32)


def bvmem(*shape):
    return pltpu.VMEM(shape, BF16)


def dma(*shape):
    return pltpu.SemaphoreType.DMA(shape)


HBM = pl.BlockSpec(memory_space=pl.ANY)
QUAD = (2, 2, 2)


def forward(a, w, s, gamma, beta, labels, bias, wt):
    prev = lambda j: (0, jnp.clip(j - 1, 0, NB - 1))
    cur = lambda j: (0, jnp.minimum(j, NB - 1))
    late = lambda j: (0, jnp.clip(j - 4, 0, NG - 1))
    vec, lab = (1, COUT), QUAD + (1, IMG)
    return pl.pallas_call(
        fwd_kernel,
        grid=(NB + 1 + TAIL,),
        in_specs=[HBM, pl.BlockSpec((CIN, CB), cur), pl.BlockSpec((ROWS, CB), prev), pl.BlockSpec((1, CB), prev), pl.BlockSpec((1, CB), prev),
                  whole(1, IMG), whole(1, CLASSES), pl.BlockSpec((CLASSES, CB), cur)],
        out_specs=[HBM, pl.BlockSpec((IMG, ROWS), lambda j: (jnp.minimum(j, NB - 1), 0)), pl.BlockSpec((TOTAL, CB), late), whole(IMG, PT), whole(*lab),
                   whole(SUB, CB), whole(SUB, COUT), HBM, whole(IMG, COUT)] + [whole(*vec)] * 4 + [whole(2, COUT)],
        out_shape=[struct((NB, ROWS, CB)), struct((CIN, ROWS), BF16), struct((TOTAL, PG), BF16), struct((IMG, PT)), struct(lab, jnp.int32),
                   struct((SUB, CB)), struct((SUB, COUT)), struct((KP, COUT), BF16), struct((IMG, COUT))] + [struct(vec)] * 4 + [struct((2, COUT))],
        scratch_shapes=[bvmem(ROWS, APAD), fvmem(ROWS, CB), fvmem(ROWS, CB), bvmem(CIN, CB), fvmem(4 * SUB, CB), fvmem(*QUAD, IMG, COUT), pltpu.VMEM(lab, jnp.int32),
                        fvmem(IMG, CB), fvmem(IMG, COUT), fvmem(IMG, COUT), fvmem(2 * SUB, COUT), bvmem(KP, COUT), fvmem(1, KP),
                        dma(NCH), dma(2), pltpu.SemaphoreType.DMA, dma(5, NG), dma(5, NG), dma(DEVS), dma(DEVS)],
        compiler_params=pltpu.CompilerParams(vmem_limit_bytes=63 * MIB, collective_id=0, has_side_effects=True),
        cost_estimate=pl.CostEstimate(flops=2 * ROWS * CIN * COUT, bytes_accessed=2 * ROWS * COUT * 4, transcendentals=0),
        name="fwd_conv",
    )(a, w, s, gamma, beta, labels, bias, wt)


def bwd_kernel(at_hbm, z_ref, s_ref, sc_ref, sh_ref, bb_ref, cc_ref, da_ref, db_ref, pall_hbm, ptail_hbm, wtb_hbm, lab_ref, bias_ref,
               g_hbm, dbo_ref, gsq_ref, gfc_hbm, fsq_ref, gb_ref, loss_ref,
               atv, dz0, dz1, dw, rd, ha, hb, ra, rb, ka, kb, r2a, r2b, gfull, dball, ptail, bpad, ps, pr, ss, rs, gs, gr, bs, br, osem, isem, fsem):
    j = pl.program_id(0)
    dzs = (dz0, dz1)
    me, core, x, y = position()
    plan = pl.ds(0, COUT)
    pall = atv.at[:, plan]
    wtb = atv.at[:, pl.ds(COUT, COUT)]
    dlt = atv.at[:, pl.ds(2 * COUT, TOTAL)]

    at_copy = pltpu.make_async_copy(at_hbm, atv, isem.at[0])
    pall_copy = pltpu.make_async_copy(pall_hbm, atv.at[:, pl.ds(0, PG)], isem.at[1])
    wtb_copy = pltpu.make_async_copy(wtb_hbm, wtb, isem.at[2])
    ptail_copy = pltpu.make_async_copy(ptail_hbm, ptail.at[core, y, x], isem.at[3])
    db_copies = [rcopy(db_ref, dball.at[me], bs.at[k], br.at[k], lax.rem(me + k, DEVS)) for k in range(1, DEVS)]

    @pl.when(j == 0)
    def _():
        ptail_copy.start()
        at_copy.start()
        enter_all()
        ptail_copy.wait()
        for b in range(NP):
            each(start, gather_own(ptail, ps, pr, b))
        each(start, db_copies)
        dball[me] = db_ref[:]
        for r in (gsq_ref, fsq_ref, gb_ref, loss_ref):
            r[:] = jnp.zeros_like(r)
        set_bias(bpad, bias_ref)

    @pl.when(j == 1)
    def _():
        at_copy.wait()

    def out_copy(b):
        c = cols(b)
        return pltpu.make_async_copy(gfull.at[:, :, :, :, c], g_hbm.at[:, :, :, :, c], osem.at[b])

    def core_copy(b, k=0):
        return rcopy(dw.at[lax.rem(b, 2), span(1 - core, HALF), :], rd.at[b], ss.at[k, b], rs.at[k, b], neighbour(PN))

    def first_copies(b, k=1, m=2):
        sl = lax.rem(b, 2)
        return (rcopy(ha.at[sl, 1 - x], ra.at[b], ss.at[k, b], rs.at[k, b], neighbour(XN)),
                rcopy(hb.at[sl, 1 - y], rb.at[b], ss.at[m, b], rs.at[m, b], neighbour(YN)))

    def second_copies(b, k=3, m=4):
        sl = lax.rem(b, 2)
        return (rcopy(ka.at[sl, 1 - y], r2a.at[b], ss.at[k, b], rs.at[k, b], neighbour(YN)),
                rcopy(kb.at[sl, 1 - x], r2b.at[b], ss.at[m, b], rs.at[m, b], neighbour(XN)))

    def stage1(b):
        core_copy(b).wait()
        sl = lax.rem(b, 2)
        for q, (py, px) in enumerate((py, px) for py in range(2) for px in range(2)):
            own = pl.ds(pl.multiple_of(core * HALF + q * QR, QR), QR)
            got = slice(q * QR, (q + 1) * QR)
            ha[sl, px, py] = dw[sl, own, :HC] + rd[b, got, :HC]
            hb[sl, py, px] = dw[sl, own, HC:] + rd[b, got, HC:]
        each(start, first_copies(b))

    def stage2(b):
        sl = lax.rem(b, 2)
        each(wait, first_copies(b))
        for k in range(2):
            ka[sl, k] = ha[sl, x, k] + ra[b, k]
            kb[sl, k] = hb[sl, y, k] + rb[b, k]
        each(start, second_copies(b))

    def stage3(b):
        sl = lax.rem(b, 2)
        each(wait, second_copies(b))
        gfull[core, y, x, :, cols(b, HC)] = ka[sl, y] + r2a[b]
        gfull[core, y, x, :, cols(b, HC, HC)] = kb[sl, x] + r2b[b]
        each(start, gather_own(gfull, gs, gr, b))

    def stage4(b):
        each(wait_recv, gather_own(gfull, gs, gr, b))
        each(start, gather_on(gfull, gs, gr, b))

    def stage5(b):
        each(wait_recv, gather_on(gfull, gs, gr, b))
        each(start, gather_core(gfull, gs, gr, b))

    def stage6(b):
        each(wait_recv, gather_core(gfull, gs, gr, b))
        out_copy(b).start()
        acc = gsq_ref[:]
        for q in pieces():
            gv = gfull[q + (slice(None), cols(b))]
            acc = acc + fold(gv * gv)
        gsq_ref[:] = acc

    def pooled_on():
        for b in range(NP):
            each(wait_recv, gather_own(ptail, ps, pr, b))
            each(start, gather_on(ptail, ps, pr, b))

    def pooled_core():
        for b in range(NP):
            each(wait_recv, gather_on(ptail, ps, pr, b))
            each(start, gather_core(ptail, ps, pr, b))

    def stages():
        stage_list(j, NB, (stage1, stage2, stage3, stage4, stage5, stage6), LAGS)
        pl.when(j == 1)(pooled_on)
        pl.when(j == 2)(pooled_core)

    def step(par, do_pre, do_mm):
        slot, prev = dzs[par], dzs[1 - par]
        out = dw.at[1 - par]
        if do_pre:
            sc, sh, bb, cc = sc_ref[:], sh_ref[:], bb_ref[:], cc_ref[:]

        def pre(base, n):
            da = da_ref[n:n + NT, :]
            for p in range(CH):
                r = pl.ds(base + p * IMG + n, NT)
                zz = z_ref[r, :]
                u = zz * sc + sh + s_ref[r, :].astype(F32)
                slot[r, :] = (jnp.where(u > 0, da, 0.0) + (zz * cc + bb)).astype(BF16)

        def body(base, slabs, add):
            work = [functools.partial(pre, base + p * IMG, n) for p in range(0, slabs, CH) for n in range(0, IMG, NT)]
            size = slabs * IMG
            for k in range(BPIECES):
                m = slice(k * CIN // BPIECES, (k + 1) * CIN // BPIECES)
                if do_mm:
                    g = dot(atv[m, pl.ds(base, size)], prev[pl.ds(base, size), :])
                if do_pre:
                    n = len(work)
                    for f in work[k * n // BPIECES:(k + 1) * n // BPIECES]:
                        f()
                if do_mm:
                    out[m] = out[m] + g if add else g

        rest = NBIG * BIG
        body(rest, POS - NBIG * BTILE, False)

        def chunk(i, carry):
            base = pl.multiple_of(i * BIG, BIG)
            if do_mm:
                pl.when(i == 1)(stages)
            body(base, BTILE, True)
            return carry
        lax.fori_loop(0, NBIG, chunk, 0)
        if do_mm:
            core_copy(j - 1).start()

    @pl.when(j == 0)
    def _():
        step(0, True, False)

    for par in range(2):
        @pl.when(jnp.logical_and(jnp.logical_and(j > 0, j < NB), lax.rem(j, 2) == par))
        def _():
            step(par, True, True)

    def logits_unit(i):
        rows = span(i, LB)
        lg = dot_t(pall[rows, :], wtb[:])
        lab = jnp.concatenate([label_rows(lab_ref[i // 2, lax.rem(i, 2), k]) for k in range(2)])
        lterm, dl = softmax_terms(lg, bpad[:], lab)
        loss_ref[:] += fold(lterm)
        gb_ref[:] += fold(dl)
        dlt[:, pl.ds(pl.multiple_of(i * LB, LB), LB)] = dl.T.astype(BF16)

    def fc_copies(c):
        sl = lax.rem(c, 4)
        return [pltpu.make_async_copy(rd.at[sl * 2 + h], gfc_hbm.at[pl.ds(h * HALF, HALF), cols(c)], fsem.at[h, c]) for h in range(2)]

    def dfc_unit(c):
        pl.when(c >= 4)(lambda: each(wait, fc_copies(c - 4)))
        acc = jnp.zeros((SUB, CB), F32)
        for h in range(2):
            g = dot(dlt[pl.ds(h * HALF, HALF), :], pall[:, cols(c)])
            rd[lax.rem(c, 4) * 2 + h] = g
            acc = acc + fold(g * g)
        fsq_ref[:, cols(c)] = acc
        each(start, fc_copies(c))

    @pl.when(j == NB)
    def _():
        step(0, False, True)
        pall_copy.start()
        wtb_copy.start()

    @pl.when(j > NB)
    def _():
        stages()
        k = j - NB - 1

        @pl.when(k == 0)
        def _():
            for b in range(NP):
                each(wait_recv, gather_core(ptail, ps, pr, b))
            for q, (c, py, px) in enumerate(pieces()):
                atv[span(q, IMG), PG:COUT] = ptail[c, py, px].astype(BF16)
            pall_copy.wait()
            wtb_copy.wait()

        loop(jnp.minimum(k * 3, 4), jnp.minimum(k * 3 + 3, 4), logits_unit)
        loop(jnp.clip(k * 3 - 3, 0, NB), jnp.clip(k * 3, 0, NB), dfc_unit)

    @pl.when(j == NB + BTAIL - 1)
    def _():
        each(wait, db_copies)
        acc = dball[0]
        for k in range(1, DEVS):
            acc = acc + dball[k]
        dbo_ref[:] = acc
        for c in range(4, NB):
            each(wait, fc_copies(c))

        def drain(b):
            each(wait_send, gather_all(gfull, gs, gr, b))
            out_copy(b).wait()
        loop(0, NB, drain)
        loop(0, NP, lambda b: each(wait_send, gather_all(ptail, ps, pr, b)))


def backward(*args):
    cur = lambda j: (0, jnp.minimum(j, NB - 1))
    row = pl.BlockSpec((1, CB), cur)
    pair, quad, side = (2, QR, HC), (2, 2, 2, QR, HC), (NB, QR, HC)
    return pl.pallas_call(
        bwd_kernel,
        grid=(NB + BTAIL,),
        in_specs=[HBM, pl.BlockSpec((None, ROWS, CB), lambda j: (jnp.minimum(j, NB - 1), 0, 0)), pl.BlockSpec((ROWS, CB), cur), row, row, row, row,
                  pl.BlockSpec((IMG, CB), cur), whole(2, COUT), HBM, HBM, HBM, whole(2, 2, 2, 1, IMG), whole(1, CLASSES)],
        out_specs=[HBM, whole(2, COUT), whole(SUB, CB), HBM, whole(SUB, COUT), whole(SUB, KP), whole(SUB, KP)],
        out_shape=[struct(QUAD + (QR, COUT)), struct((2, COUT)), struct((SUB, CB)), struct((KP, COUT)), struct((SUB, COUT)), struct((SUB, KP)), struct((SUB, KP))],
        scratch_shapes=[bvmem(CIN, ROWS), bvmem(ROWS, CB), bvmem(ROWS, CB), fvmem(2, CIN, CB), fvmem(NB, HALF, CB), fvmem(*quad), fvmem(*quad),
                        fvmem(NB, *pair), fvmem(NB, *pair), fvmem(2, *pair), fvmem(2, *pair), fvmem(*side), fvmem(*side),
                        fvmem(*QUAD, QR, COUT), fvmem(DEVS, 2, COUT), fvmem(*QUAD, IMG, PT), fvmem(1, KP),
                        dma(5, NP), dma(5, NP), dma(5, NB), dma(5, NB), dma(5, NB), dma(5, NB), dma(DEVS), dma(DEVS), dma(NB), dma(4), dma(2, NB)],
        compiler_params=pltpu.CompilerParams(vmem_limit_bytes=63 * MIB, collective_id=1, has_side_effects=True),
        cost_estimate=pl.CostEstimate(flops=2 * ROWS * CIN * COUT, bytes_accessed=2 * ROWS * COUT * 4, transcendentals=0),
        name="bwd_conv",
    )(*args)


def trust_of(wsq, gsq):
    wn = jnp.sqrt(lanesum(rowsum(wsq)))
    gn = jnp.sqrt(lanesum(rowsum(gsq)))
    return TRUST_COEF * wn / (gn + WEIGHT_DECAY * wn)


def update_kernel(lr_ref, w_ref, v_ref, g_ref, wsq_ref, gsq_ref, wt_ref, vt_ref, gt_ref, tsq_ref, fsq_ref, bias_ref, vbias_ref, gb_ref, ls_ref,
                  gam_ref, bet_ref, vgam_ref, vbet_ref, dgb_ref,
                  wo_ref, vo_ref, wto_ref, vto_ref, bo_ref, vbo_ref, go_ref, vgo_ref, beo_ref, vbeo_ref, loss_ref):
    j = pl.program_id(0)
    lr = lr_ref[0]

    def plain(p, v, g, po, vo):
        nv = MOMENTUM * v[:] + lr * g
        vo[:] = nv
        po[:] = p[:] - nv

    @pl.when(j == 0)
    def _():
        plain(gam_ref, vgam_ref, dgb_ref[:1], go_ref, vgo_ref)
        plain(bet_ref, vbet_ref, dgb_ref[1:], beo_ref, vbeo_ref)
        plain(bias_ref, vbias_ref, rowsum(gb_ref[:])[:, :CLASSES], bo_ref, vbo_ref)
        loss_ref[:] = lanesum(rowsum(ls_ref[:])) * (-1.0 / TOTAL)

    def lars(w_ref, v_ref, g_ref, wsq, gsq, wo, vo, rows):
        rate = jnp.broadcast_to(lr * trust_of(wsq[:], gsq[:]), (SUB, CB))

        def row(i, carry):
            for q in range(2):
                r = pl.ds(pl.multiple_of(i * 2 * SUB + q * SUB, SUB), SUB)
                for c in range(0, COUT, CB):
                    cc = slice(c, c + CB)
                    w = w_ref[r, cc]
                    nv = MOMENTUM * v_ref[r, cc] + rate * (g_ref[r, cc] + WEIGHT_DECAY * w)
                    vo[r, cc] = nv
                    wo[r, cc] = w - nv
            return carry
        lax.fori_loop(0, rows // (2 * SUB), row, 0)

    @pl.when(j < NU)
    def _():
        lars(w_ref, v_ref, g_ref, wsq_ref, gsq_ref, wo_ref, vo_ref, UB)

    @pl.when(j >= NU)
    def _():
        lars(wt_ref, vt_ref, gt_ref, tsq_ref, fsq_ref, wto_ref, vto_ref, FB)


def update_all(*args):
    conv = pl.BlockSpec((UB, COUT), lambda j: (jnp.minimum(j, NU - 1), 0))
    fc = pl.BlockSpec((FB, COUT), lambda j: (jnp.clip(j - NU, 0, NF - 1), 0))
    vec, bvec, one = (1, COUT), (1, CLASSES), (1, 1)
    vs, bs = whole(*vec), whole(*bvec)
    big, fcs = struct((CIN, COUT)), struct((CLASSES, COUT))
    return pl.pallas_call(
        update_kernel,
        grid=(NU + NF,),
        in_specs=[pl.BlockSpec(memory_space=pltpu.SMEM), conv, conv, conv, whole(SUB, CB), whole(SUB, CB), fc, fc, fc, whole(SUB, COUT), whole(SUB, COUT),
                  bs, bs, whole(SUB, KP), whole(SUB, KP), vs, vs, vs, vs, whole(2, COUT)],
        out_specs=[conv, conv, fc, fc, bs, bs, vs, vs, vs, vs, whole(*one)],
        out_shape=[big, big, fcs, fcs] + [struct(bvec)] * 2 + [struct(vec)] * 4 + [struct(one)],
        compiler_params=pltpu.CompilerParams(vmem_limit_bytes=63 * MIB),
        cost_estimate=pl.CostEstimate(flops=CIN * COUT * 16, bytes_accessed=10 * CIN * COUT * 4, transcendentals=0),
        name="update",
    )(*args)


def solution(mesh):
    def local_step(act_in, shortcut, labels, w_conv, gamma, beta, w_fc, fc_bias, vel_conv, vel_gamma, vel_beta, vel_fc, vel_bias, lr):
        a = act_in.transpose(1, 2, 0, 3).reshape(ROWS, CIN)
        s = shortcut.transpose(1, 2, 0, 3).reshape(ROWS, COUT)
        wt = w_fc.T
        bias = fc_bias[None]
        z, at, pall, ptail, lab, wsq, tsq, wtb, da, sc, sh, bb, cc, dgb = forward(a, w_conv, s, gamma[None], beta[None], labels[None], bias, wt)
        g8, dgb, gsq, gfc, fsq, gb, ls = backward(at, z, s, sc, sh, bb, cc, da, dgb, pall, ptail, wtb, lab, bias)
        wo, vo, wto, vto, bo, vbo, go, vgo, beo, vbeo, loss = update_all(
            lr.reshape(1), w_conv, vel_conv, g8.reshape(CIN, COUT), wsq, gsq, wt, vel_fc.T, gfc, tsq, fsq, bias, vel_bias[None], gb, ls,
            gamma[None], beta[None], vel_gamma[None], vel_beta[None], dgb)
        return (wo, go[0], beo[0], wto.T, bo[0], vo, vgo[0], vbeo[0], vto.T, vbo[0], loss[0, 0])

    return jax.shard_map(local_step, mesh=mesh, in_specs=(P('dp'),) * 3 + (P(),) * 11, out_specs=(P(),) * 11, check_vma=False)
```

```python
import functools
import jax
import jax.numpy as jnp
from jax import lax
from jax.experimental import pallas as pl
from jax.experimental.pallas import tpu as pltpu
from jax.sharding import PartitionSpec as P

BN_EPS = 1e-5
SMOOTHING = 0.1
MOMENTUM = 0.9
TRUST_COEF = 0.001
WEIGHT_DECAY = 5e-5

LANES = 128
SUB = 8
IMG = 128
POS = 49
ROWS = IMG * POS
CIN = 1024
COUT = 2048
CLASSES = 1000
KP = 1024
DEVS = 8
TOTAL = DEVS * IMG
CB = 256
HC = CB // 2
NB = COUT // CB
CH = 7
NCH = POS // CH
NT = 16
PIECES = 8
BPIECES = 4
APAD = CIN + LANES
TAIL = 1
NG = 6
NP = NB - NG
PG, PT = NG * CB, NP * CB
LAGS = (2, 3, 4, 6, 8, 9)
BTAIL = LAGS[-1]
QR = CIN // DEVS
HALF = CIN // 2
BIG = 1792
BTILE = BIG // IMG
NBIG = ROWS // BIG
UB = 64
FB = 112
NU = CIN // UB
NF = pl.cdiv(CLASSES, FB)
LB = 256
MIB = 1024 * 1024
F32 = jnp.float32
BF16 = jnp.bfloat16
MESH = pl.DeviceIdType.MESH
XN, YN, PN = 'x', 'y', 'core'


def dot(a, b):
    return jnp.dot(a, b, preferred_element_type=F32)


def dot_t(a, b):
    return lax.dot_general(a, b, (((1,), (1,)), ((), ())), preferred_element_type=F32)


def fold(v, axis=0):
    return jnp.sum(v.reshape(v.shape[0] // SUB, SUB, v.shape[1]), axis=axis)


def rowsum(v, axis=0):
    return jnp.sum(v, axis=axis, keepdims=True)


def lanesum(v, axis=1):
    return jnp.sum(v, axis=axis, keepdims=True)


def cols(b, size=CB, at=0):
    return pl.ds(pl.multiple_of(b * CB + at, LANES), size)


def span(i, size):
    return pl.ds(pl.multiple_of(i * size, SUB), size)


def position():
    me = lax.axis_index('dp')
    return me, lax.rem(me, 2), lax.rem(me // 2, 2), me // 4


def dev(core, x, y):
    return (y * 2 + x) * 2 + core


def neighbour(name):
    me, core, x, y = position()
    flip = lambda v, k: 1 - v if k == name else v
    return dev(flip(core, PN), flip(x, XN), flip(y, YN))


def enter_all():
    me = lax.axis_index('dp')
    bar = pltpu.get_barrier_semaphore()
    for k in range(1, DEVS):
        pl.semaphore_signal(bar, inc=1, device_id=(lax.rem(me + k, DEVS),), device_id_type=MESH)
    pl.semaphore_wait(bar, DEVS - 1)


def rcopy(src, dst, send, recv, target):
    return pltpu.make_async_remote_copy(src_ref=src, dst_ref=dst, send_sem=send, recv_sem=recv, device_id=(target,), device_id_type=MESH)


def each(fn, copies):
    for c in copies:
        fn(c)


def start(c):
    c.start()


def wait(c):
    c.wait()


def wait_send(c):
    c.wait_send()


def wait_recv(c):
    c.wait_recv()


def gather_own(buf, send, recv, b, ka=0, kb=1):
    me, core, x, y = position()
    a, c = buf.at[core, y, x, :, cols(b, HC)], buf.at[core, y, x, :, cols(b, HC, HC)]
    return rcopy(a, a, send.at[ka, b], recv.at[ka, b], neighbour(YN)), rcopy(c, c, send.at[kb, b], recv.at[kb, b], neighbour(XN))


def gather_on(buf, send, recv, b, ka=2, kb=3):
    me, core, x, y = position()
    a, c = buf.at[core, :, x, :, cols(b, HC)], buf.at[core, y, :, :, cols(b, HC, HC)]
    return rcopy(a, a, send.at[ka, b], recv.at[ka, b], neighbour(XN)), rcopy(c, c, send.at[kb, b], recv.at[kb, b], neighbour(YN))


def gather_core(buf, send, recv, b, k=4):
    me, core, x, y = position()
    a = buf.at[core, :, :, :, cols(b)]
    return (rcopy(a, a, send.at[k, b], recv.at[k, b], neighbour(PN)),)


def gather_all(*a):
    return gather_own(*a) + gather_on(*a) + gather_core(*a)


def stage_list(j, blocks, fns, lags):
    for fn, lag in zip(fns, lags):
        b = j - lag
        pl.when(jnp.logical_and(b >= 0, b < blocks))(functools.partial(fn, b))


def loop(lo, hi, fn):
    def body(i, carry):
        fn(i)
        return carry
    lax.fori_loop(lo, hi, body, 0)


def pieces():
    return [(c, y, x) for c in range(2) for y in range(2) for x in range(2)]


def softmax_terms(logits, bias, labels):
    n = logits.shape[0]
    cls = lax.broadcasted_iota(jnp.int32, (n, KP), 1)
    valid = cls < CLASSES
    lg = jnp.where(valid, logits + bias, -1e30)
    sh = lg - jnp.max(lg, axis=1, keepdims=True)
    lp = sh - jnp.log(lanesum(jnp.exp(sh)))
    lab = jnp.concatenate([labels] * (KP // LANES), axis=1)
    hit = lab == cls.astype(F32)
    tg = jnp.where(valid, SMOOTHING / CLASSES + jnp.where(hit, 1.0 - SMOOTHING, 0.0), 0.0)
    return tg * lp, (jnp.exp(lp) - tg) * (1.0 / TOTAL)


def label_rows(row):
    return jnp.broadcast_to(row.astype(F32), (IMG, IMG)).T


def set_bias(bpad, bias_ref):
    bpad[:] = jnp.zeros_like(bpad)
    bpad[:, :CLASSES] = bias_ref[:]


def fwd_kernel(a_hbm, w_ref, s_ref, g_ref, b_ref, lab_ref, bias_ref, wt_ref,
               z_hbm, at_ref, pall_ref, ptail_ref, lall_ref, wsq_ref, fsq_ref, wtb_hbm, da_ref, sc_ref, sh_ref, bb_ref, cc_ref, db_ref,
               abf, z0, z1, wbf, stat, pfull, lfull, pool, cnt, sx, sv, wtb, bpad, asem, zsem, osem, gs, gr, ls, lr):
    j = pl.program_id(0)
    zs = (z0, z1)
    me, core, x, y = position()
    crow = CH * IMG

    def a_copy(i):
        r = span(i, crow)
        return pltpu.make_async_copy(a_hbm.at[r, :], abf.at[r, :CIN], asem.at[i])

    def z_copy(jj, par):
        return pltpu.make_async_copy(zs[par], z_hbm.at[jj], zsem.at[par])

    def wtb_copy():
        return pltpu.make_async_copy(wtb, wtb_hbm, osem)

    def label_copy(k):
        return rcopy(lab_ref, lfull.at[core, y, x], ls.at[k], lr.at[k], lax.rem(me + k, DEVS))

    labels = [label_copy(k) for k in range(1, DEVS)]

    @pl.when(j == 0)
    def _():
        for i in range(NCH):
            a_copy(i).start()
        enter_all()
        each(start, labels)
        lfull[core, y, x] = lab_ref[:]
        wsq_ref[:] = jnp.zeros_like(wsq_ref)
        wtb[CLASSES:] = jnp.zeros((KP - CLASSES, COUT), BF16)
        set_bias(bpad, bias_ref)

    def second(b):
        each(wait_recv, gather_own(pfull, gs, gr, b))
        each(start, gather_on(pfull, gs, gr, b))

    def third(b):
        each(wait_recv, gather_on(pfull, gs, gr, b))
        each(start, gather_core(pfull, gs, gr, b))

    def last(b):
        each(wait_recv, gather_core(pfull, gs, gr, b))
        for q, (c, py, px) in enumerate(pieces()):
            pall_ref[span(q, IMG), :] = pfull[c, py, px, :, cols(b)].astype(BF16)

    def stages():
        stage_list(j, NG, (second, third, last), (2, 3, 4))

    def step(par, do_mm, do_post):
        first = not do_post
        slot, prev = zs[par], zs[1 - par]
        if do_post:
            pl.when(j >= 2)(lambda: z_copy(j - 2, par).wait())
        if do_mm:
            wf = w_ref[:]
            wsq_ref[:] += fold(wf * wf)
            wtf = wt_ref[:]
            fsq_ref[:, cols(j)] = fold(wtf * wtf)
            wtb[:CLASSES, cols(j)] = wtf.astype(BF16)
            w = wf.astype(BF16)
            wbf[:] = w
            if first:
                a_copy(0).wait()
            m0 = rowsum(dot(abf[:IMG, :CIN], w)) * (1.0 / IMG)
            stat[:2 * SUB] = jnp.zeros((2 * SUB, CB), F32)
        if do_post and not do_mm:
            wtb_copy().start()
        if do_post:
            mean = stat[2 * SUB:2 * SUB + 1]
            inv = stat[3 * SUB:3 * SUB + 1]
            sc = g_ref[:] * inv
            sh = b_ref[:] - mean * sc
            pool[:] = jnp.zeros_like(pool)
            pc = cols(j - 1)
            cnt[:, pc] = jnp.zeros((IMG, CB), F32)
            sx[:, pc] = jnp.zeros((IMG, CB), F32)

        def post(base, n, slabs):
            nr = slice(n, n + NT)
            pa, ca, xa = pool[nr], cnt[nr, pc], sx[nr, pc]
            for p in range(slabs):
                r = pl.ds(base + p * IMG + n, NT)
                zz = prev[r, :]
                u = zz * sc + sh + s_ref[r, :].astype(F32)
                mk = u > 0
                pa = pa + jnp.maximum(u, 0.0)
                ca = ca + jnp.where(mk, 1.0, 0.0)
                xa = xa + jnp.where(mk, zz, 0.0)
            pool[nr], cnt[nr, pc], sx[nr, pc] = pa, ca, xa

        def flip(base, rows):
            r = pl.ds(base, rows)
            at_ref[:, r] = abf[r, pl.ds(pl.multiple_of(j * IMG, IMG), IMG)].astype(F32).T.astype(BF16)

        def region(base, slabs, parts):
            size = slabs * IMG // parts
            for k in range(parts):
                if do_mm:
                    r = pl.ds(base + k * size, size)
                    zc = dot(abf[r, :CIN], wbf[:])
                if do_post:
                    for n in range(k * IMG // parts, (k + 1) * IMG // parts, NT):
                        post(base, n, slabs)
                if do_mm:
                    slot[r, :] = zc
                    d = zc - m0
                    stat[:SUB] += fold(d)
                    stat[SUB:2 * SUB] += fold(d * d)

            if do_mm:
                flip(base, slabs * IMG)

        def chunk(i, carry):
            if first:
                pl.when(i > 0)(lambda: a_copy(i).wait())
            region(pl.multiple_of(i * crow, crow), CH, 4)
            return carry

        def chunk2(i, carry):
            region(pl.multiple_of(i * 2 * crow, 2 * crow), 2 * CH, PIECES)
            return carry

        if first:
            lax.fori_loop(0, NCH, chunk, 0)
        else:
            lax.fori_loop(0, NCH // 2, chunk2, 0)
            stages()
            region(pl.multiple_of((jnp.minimum(me, 0) + NCH - 1) * crow, crow), CH, 4)
        if do_post:
            pfull[core, y, x, :, pc] = pool[:] * (1.0 / POS)
            sx[:, pc] = (sx[:, pc] - mean * cnt[:, pc]) * inv
            sv[:1, pc] = mean
            sv[SUB:SUB + 1, pc] = inv
            sc_ref[:, pc] = sc
            sh_ref[:, pc] = sh
            pl.when(j - 1 < NG)(lambda: each(start, gather_own(pfull, gs, gr, j - 1)))
        if do_mm:
            dm = rowsum(stat[:SUB]) * (1.0 / ROWS)
            q = rowsum(stat[SUB:2 * SUB]) * (1.0 / ROWS)
            stat[2 * SUB:2 * SUB + 1] = m0 + dm
            stat[3 * SUB:3 * SUB + 1] = lax.rsqrt(jnp.maximum(q - dm * dm, 0.0) + BN_EPS)
            z_copy(j, par).start()

    @pl.when(j == 0)
    def _():
        step(0, True, False)

    for par in range(2):
        @pl.when(jnp.logical_and(jnp.logical_and(j > 0, j < NB), lax.rem(j, 2) == par))
        def _():
            step(par, True, True)

    @pl.when(j == NB)
    def _():
        step(0, False, True)

    @pl.when(j == NB + 1)
    def _():
        stages()
        ptail_ref[:] = pfull[core, y, x, :, PG:]
        lg = dot_t(pfull[core, y, x].astype(BF16), wtb[:])
        _, dl = softmax_terms(lg, bpad[:], label_rows(lab_ref[:]))
        dlb = dl.astype(BF16)

        def col(b, carry):
            c = cols(b)
            dp = dot(dlb, wtb[:, c]) * (1.0 / POS)
            dbeta = rowsum(dp * cnt[:, c])
            dgamma = rowsum(dp * sx[:, c])
            sc = sc_ref[:, c]
            cc = -(sc * sv[SUB:SUB + 1, c]) * (dgamma * (1.0 / ROWS))
            cc_ref[:, c] = cc
            bb_ref[:, c] = -sc * (dbeta * (1.0 / ROWS)) - sv[:1, c] * cc
            da_ref[:, c] = dp * sc
            db_ref[:1, c] = dgamma
            db_ref[1:, c] = dbeta
            return carry
        lax.fori_loop(0, NB, col, 0)

        each(wait, labels)
        lall_ref[:] = lfull[:]
        wtb_copy().wait()
        z_copy(NB - 1, 1).wait()
        loop(0, NG, lambda b: each(wait_send, gather_all(pfull, gs, gr, b)))


def whole(*shape):
    return pl.BlockSpec(shape, lambda j: (0,) * len(shape))


def struct(shape, dtype=F32):
    return jax.ShapeDtypeStruct(shape, dtype)


def fvmem(*shape):
    return pltpu.VMEM(shape, F32)


def bvmem(*shape):
    return pltpu.VMEM(shape, BF16)


def dma(*shape):
    return pltpu.SemaphoreType.DMA(shape)


HBM = pl.BlockSpec(memory_space=pl.ANY)
QUAD = (2, 2, 2)


def forward(a, w, s, gamma, beta, labels, bias, wt):
    prev = lambda j: (0, jnp.clip(j - 1, 0, NB - 1))
    cur = lambda j: (0, jnp.minimum(j, NB - 1))
    late = lambda j: (0, jnp.clip(j - 4, 0, NG - 1))
    vec, lab = (1, COUT), QUAD + (1, IMG)
    return pl.pallas_call(
        fwd_kernel,
        grid=(NB + 1 + TAIL,),
        in_specs=[HBM, pl.BlockSpec((CIN, CB), cur), pl.BlockSpec((ROWS, CB), prev), pl.BlockSpec((1, CB), prev), pl.BlockSpec((1, CB), prev),
                  whole(1, IMG), whole(1, CLASSES), pl.BlockSpec((CLASSES, CB), cur)],
        out_specs=[HBM, pl.BlockSpec((IMG, ROWS), lambda j: (jnp.minimum(j, NB - 1), 0)), pl.BlockSpec((TOTAL, CB), late), whole(IMG, PT), whole(*lab),
                   whole(SUB, CB), whole(SUB, COUT), HBM, whole(IMG, COUT)] + [whole(*vec)] * 4 + [whole(2, COUT)],
        out_shape=[struct((NB, ROWS, CB)), struct((CIN, ROWS), BF16), struct((TOTAL, PG), BF16), struct((IMG, PT)), struct(lab, jnp.int32),
                   struct((SUB, CB)), struct((SUB, COUT)), struct((KP, COUT), BF16), struct((IMG, COUT))] + [struct(vec)] * 4 + [struct((2, COUT))],
        scratch_shapes=[bvmem(ROWS, APAD), fvmem(ROWS, CB), fvmem(ROWS, CB), bvmem(CIN, CB), fvmem(4 * SUB, CB), fvmem(*QUAD, IMG, COUT), pltpu.VMEM(lab, jnp.int32),
                        fvmem(IMG, CB), fvmem(IMG, COUT), fvmem(IMG, COUT), fvmem(2 * SUB, COUT), bvmem(KP, COUT), fvmem(1, KP),
                        dma(NCH), dma(2), pltpu.SemaphoreType.DMA, dma(5, NG), dma(5, NG), dma(DEVS), dma(DEVS)],
        compiler_params=pltpu.CompilerParams(vmem_limit_bytes=63 * MIB, collective_id=0, has_side_effects=True),
        cost_estimate=pl.CostEstimate(flops=2 * ROWS * CIN * COUT, bytes_accessed=2 * ROWS * COUT * 4, transcendentals=0),
        name="fwd_conv",
    )(a, w, s, gamma, beta, labels, bias, wt)


def bwd_kernel(at_hbm, z_ref, s_ref, sc_ref, sh_ref, bb_ref, cc_ref, da_ref, db_ref, pall_hbm, ptail_hbm, wtb_hbm, lab_ref, bias_ref,
               g_hbm, dbo_ref, gsq_ref, gfc_hbm, fsq_ref, gb_ref, loss_ref,
               atv, dz0, dz1, dw, rd, ha, hb, ra, rb, ka, kb, r2a, r2b, gfull, dball, ptail, bpad, ps, pr, ss, rs, gs, gr, bs, br, osem, isem, fsem):
    j = pl.program_id(0)
    dzs = (dz0, dz1)
    me, core, x, y = position()
    plan = pl.ds(0, COUT)
    pall = atv.at[:, plan]
    wtb = atv.at[:, pl.ds(COUT, COUT)]
    dlt = atv.at[:, pl.ds(2 * COUT, TOTAL)]

    at_copy = pltpu.make_async_copy(at_hbm, atv, isem.at[0])
    pall_copy = pltpu.make_async_copy(pall_hbm, atv.at[:, pl.ds(0, PG)], isem.at[1])
    wtb_copy = pltpu.make_async_copy(wtb_hbm, wtb, isem.at[2])
    ptail_copy = pltpu.make_async_copy(ptail_hbm, ptail.at[core, y, x], isem.at[3])
    db_copies = [rcopy(db_ref, dball.at[me], bs.at[k], br.at[k], lax.rem(me + k, DEVS)) for k in range(1, DEVS)]

    @pl.when(j == 0)
    def _():
        ptail_copy.start()
        at_copy.start()
        enter_all()
        ptail_copy.wait()
        for b in range(NP):
            each(start, gather_own(ptail, ps, pr, b))
        each(start, db_copies)
        dball[me] = db_ref[:]
        for r in (gsq_ref, fsq_ref, gb_ref, loss_ref):
            r[:] = jnp.zeros_like(r)
        set_bias(bpad, bias_ref)

    @pl.when(j == 1)
    def _():
        at_copy.wait()

    def out_copy(b):
        c = cols(b)
        return pltpu.make_async_copy(gfull.at[:, :, :, :, c], g_hbm.at[:, :, :, :, c], osem.at[b])

    def core_copy(b, k=0):
        return rcopy(dw.at[lax.rem(b, 2), span(1 - core, HALF), :], rd.at[b], ss.at[k, b], rs.at[k, b], neighbour(PN))

    def first_copies(b, k=1, m=2):
        sl = lax.rem(b, 2)
        return (rcopy(ha.at[sl, 1 - x], ra.at[b], ss.at[k, b], rs.at[k, b], neighbour(XN)),
                rcopy(hb.at[sl, 1 - y], rb.at[b], ss.at[m, b], rs.at[m, b], neighbour(YN)))

    def second_copies(b, k=3, m=4):
        sl = lax.rem(b, 2)
        return (rcopy(ka.at[sl, 1 - y], r2a.at[b], ss.at[k, b], rs.at[k, b], neighbour(YN)),
                rcopy(kb.at[sl, 1 - x], r2b.at[b], ss.at[m, b], rs.at[m, b], neighbour(XN)))

    def stage1(b):
        core_copy(b).wait()
        sl = lax.rem(b, 2)
        for q, (py, px) in enumerate((py, px) for py in range(2) for px in range(2)):
            own = pl.ds(pl.multiple_of(core * HALF + q * QR, QR), QR)
            got = slice(q * QR, (q + 1) * QR)
            ha[sl, px, py] = dw[sl, own, :HC] + rd[b, got, :HC]
            hb[sl, py, px] = dw[sl, own, HC:] + rd[b, got, HC:]
        each(start, first_copies(b))

    def stage2(b):
        sl = lax.rem(b, 2)
        each(wait, first_copies(b))
        for k in range(2):
            ka[sl, k] = ha[sl, x, k] + ra[b, k]
            kb[sl, k] = hb[sl, y, k] + rb[b, k]
        each(start, second_copies(b))

    def stage3(b):
        sl = lax.rem(b, 2)
        each(wait, second_copies(b))
        gfull[core, y, x, :, cols(b, HC)] = ka[sl, y] + r2a[b]
        gfull[core, y, x, :, cols(b, HC, HC)] = kb[sl, x] + r2b[b]
        each(start, gather_own(gfull, gs, gr, b))

    def stage4(b):
        each(wait_recv, gather_own(gfull, gs, gr, b))
        each(start, gather_on(gfull, gs, gr, b))

    def stage5(b):
        each(wait_recv, gather_on(gfull, gs, gr, b))
        each(start, gather_core(gfull, gs, gr, b))

    def stage6(b):
        each(wait_recv, gather_core(gfull, gs, gr, b))
        out_copy(b).start()
        acc = gsq_ref[:]
        for q in pieces():
            gv = gfull[q + (slice(None), cols(b))]
            acc = acc + fold(gv * gv)
        gsq_ref[:] = acc

    def pooled_on():
        for b in range(NP):
            each(wait_recv, gather_own(ptail, ps, pr, b))
            each(start, gather_on(ptail, ps, pr, b))

    def pooled_core():
        for b in range(NP):
            each(wait_recv, gather_on(ptail, ps, pr, b))
            each(start, gather_core(ptail, ps, pr, b))

    def stages():
        stage_list(j, NB, (stage1, stage2, stage3, stage4, stage5, stage6), LAGS)
        pl.when(j == 1)(pooled_on)
        pl.when(j == 3)(pooled_core)

    def step(par, do_pre, do_mm):
        slot, prev = dzs[par], dzs[1 - par]
        out = dw.at[1 - par]
        if do_pre:
            sc, sh, bb, cc = sc_ref[:], sh_ref[:], bb_ref[:], cc_ref[:]

        def pre(base, n):
            da = da_ref[n:n + NT, :]
            for p in range(CH):
                r = pl.ds(base + p * IMG + n, NT)
                zz = z_ref[r, :]
                u = zz * sc + sh + s_ref[r, :].astype(F32)
                slot[r, :] = (jnp.where(u > 0, da, 0.0) + (zz * cc + bb)).astype(BF16)

        def body(base, slabs, add):
            work = [functools.partial(pre, base + p * IMG, n) for p in range(0, slabs, CH) for n in range(0, IMG, NT)]
            size = slabs * IMG
            for k in range(BPIECES):
                m = slice(k * CIN // BPIECES, (k + 1) * CIN // BPIECES)
                if do_mm:
                    g = dot(atv[m, pl.ds(base, size)], prev[pl.ds(base, size), :])
                if do_pre:
                    n = len(work)
                    for f in work[k * n // BPIECES:(k + 1) * n // BPIECES]:
                        f()
                if do_mm:
                    out[m] = out[m] + g if add else g

        rest = NBIG * BIG
        body(rest, POS - NBIG * BTILE, False)

        def chunk(i, carry):
            base = pl.multiple_of(i * BIG, BIG)
            if do_mm:
                pl.when(i == 1)(stages)
            body(base, BTILE, True)
            return carry
        lax.fori_loop(0, NBIG, chunk, 0)
        if do_mm:
            core_copy(j - 1).start()

    @pl.when(j == 0)
    def _():
        step(0, True, False)

    for par in range(2):
        @pl.when(jnp.logical_and(jnp.logical_and(j > 0, j < NB), lax.rem(j, 2) == par))
        def _():
            step(par, True, True)

    def logits_unit(i):
        rows = span(i, LB)
        lg = dot_t(pall[rows, :], wtb[:])
        lab = jnp.concatenate([label_rows(lab_ref[i // 2, lax.rem(i, 2), k]) for k in range(2)])
        lterm, dl = softmax_terms(lg, bpad[:], lab)
        loss_ref[:] += fold(lterm)
        gb_ref[:] += fold(dl)
        dlt[:, pl.ds(pl.multiple_of(i * LB, LB), LB)] = dl.T.astype(BF16)

    def fc_copies(c):
        sl = lax.rem(c, 4)
        return [pltpu.make_async_copy(rd.at[sl * 2 + h], gfc_hbm.at[pl.ds(h * HALF, HALF), cols(c)], fsem.at[h, c]) for h in range(2)]

    def dfc_unit(c):
        pl.when(c >= 4)(lambda: each(wait, fc_copies(c - 4)))
        acc = jnp.zeros((SUB, CB), F32)
        for h in range(2):
            g = dot(dlt[pl.ds(h * HALF, HALF), :], pall[:, cols(c)])
            rd[lax.rem(c, 4) * 2 + h] = g
            acc = acc + fold(g * g)
        fsq_ref[:, cols(c)] = acc
        each(start, fc_copies(c))

    @pl.when(j == NB)
    def _():
        step(0, False, True)
        pall_copy.start()
        wtb_copy.start()

    @pl.when(j > NB)
    def _():
        stages()
        k = j - NB - 1

        @pl.when(k == 0)
        def _():
            for b in range(NP):
                each(wait_recv, gather_core(ptail, ps, pr, b))
            for q, (c, py, px) in enumerate(pieces()):
                atv[span(q, IMG), PG:COUT] = ptail[c, py, px].astype(BF16)
            pall_copy.wait()
            wtb_copy.wait()

        loop(jnp.minimum(k * 3, 4), jnp.minimum(k * 3 + 3, 4), logits_unit)
        loop(jnp.clip(k * 3 - 3, 0, NB), jnp.clip(k * 3, 0, NB), dfc_unit)

    @pl.when(j == NB + BTAIL - 1)
    def _():
        each(wait, db_copies)
        acc = dball[0]
        for k in range(1, DEVS):
            acc = acc + dball[k]
        dbo_ref[:] = acc
        for c in range(4, NB):
            each(wait, fc_copies(c))

        def drain(b):
            each(wait_send, gather_all(gfull, gs, gr, b))
            out_copy(b).wait()
        loop(0, NB, drain)
        loop(0, NP, lambda b: each(wait_send, gather_all(ptail, ps, pr, b)))


def backward(*args):
    cur = lambda j: (0, jnp.minimum(j, NB - 1))
    row = pl.BlockSpec((1, CB), cur)
    pair, quad, side = (2, QR, HC), (2, 2, 2, QR, HC), (NB, QR, HC)
    return pl.pallas_call(
        bwd_kernel,
        grid=(NB + BTAIL,),
        in_specs=[HBM, pl.BlockSpec((None, ROWS, CB), lambda j: (jnp.minimum(j, NB - 1), 0, 0)), pl.BlockSpec((ROWS, CB), cur), row, row, row, row,
                  pl.BlockSpec((IMG, CB), cur), whole(2, COUT), HBM, HBM, HBM, whole(2, 2, 2, 1, IMG), whole(1, CLASSES)],
        out_specs=[HBM, whole(2, COUT), whole(SUB, CB), HBM, whole(SUB, COUT), whole(SUB, KP), whole(SUB, KP)],
        out_shape=[struct(QUAD + (QR, COUT)), struct((2, COUT)), struct((SUB, CB)), struct((KP, COUT)), struct((SUB, COUT)), struct((SUB, KP)), struct((SUB, KP))],
        scratch_shapes=[bvmem(CIN, ROWS), bvmem(ROWS, CB), bvmem(ROWS, CB), fvmem(2, CIN, CB), fvmem(NB, HALF, CB), fvmem(*quad), fvmem(*quad),
                        fvmem(NB, *pair), fvmem(NB, *pair), fvmem(2, *pair), fvmem(2, *pair), fvmem(*side), fvmem(*side),
                        fvmem(*QUAD, QR, COUT), fvmem(DEVS, 2, COUT), fvmem(*QUAD, IMG, PT), fvmem(1, KP),
                        dma(5, NP), dma(5, NP), dma(5, NB), dma(5, NB), dma(5, NB), dma(5, NB), dma(DEVS), dma(DEVS), dma(NB), dma(4), dma(2, NB)],
        compiler_params=pltpu.CompilerParams(vmem_limit_bytes=63 * MIB, collective_id=1, has_side_effects=True),
        cost_estimate=pl.CostEstimate(flops=2 * ROWS * CIN * COUT, bytes_accessed=2 * ROWS * COUT * 4, transcendentals=0),
        name="bwd_conv",
    )(*args)


def trust_of(wsq, gsq):
    wn = jnp.sqrt(lanesum(rowsum(wsq)))
    gn = jnp.sqrt(lanesum(rowsum(gsq)))
    return TRUST_COEF * wn / (gn + WEIGHT_DECAY * wn)


def update_kernel(lr_ref, w_ref, v_ref, g_ref, wsq_ref, gsq_ref, wt_ref, vt_ref, gt_ref, tsq_ref, fsq_ref, bias_ref, vbias_ref, gb_ref, ls_ref,
                  gam_ref, bet_ref, vgam_ref, vbet_ref, dgb_ref,
                  wo_ref, vo_ref, wto_ref, vto_ref, bo_ref, vbo_ref, go_ref, vgo_ref, beo_ref, vbeo_ref, loss_ref):
    j = pl.program_id(0)
    lr = lr_ref[0]

    def plain(p, v, g, po, vo):
        nv = MOMENTUM * v[:] + lr * g
        vo[:] = nv
        po[:] = p[:] - nv

    @pl.when(j == 0)
    def _():
        plain(gam_ref, vgam_ref, dgb_ref[:1], go_ref, vgo_ref)
        plain(bet_ref, vbet_ref, dgb_ref[1:], beo_ref, vbeo_ref)
        plain(bias_ref, vbias_ref, rowsum(gb_ref[:])[:, :CLASSES], bo_ref, vbo_ref)
        loss_ref[:] = lanesum(rowsum(ls_ref[:])) * (-1.0 / TOTAL)

    def lars(w_ref, v_ref, g_ref, wsq, gsq, wo, vo, rows):
        rate = jnp.broadcast_to(lr * trust_of(wsq[:], gsq[:]), (SUB, CB))

        def row(i, carry):
            for q in range(2):
                r = pl.ds(pl.multiple_of(i * 2 * SUB + q * SUB, SUB), SUB)
                for c in range(0, COUT, CB):
                    cc = slice(c, c + CB)
                    w = w_ref[r, cc]
                    nv = MOMENTUM * v_ref[r, cc] + rate * (g_ref[r, cc] + WEIGHT_DECAY * w)
                    vo[r, cc] = nv
                    wo[r, cc] = w - nv
            return carry
        lax.fori_loop(0, rows // (2 * SUB), row, 0)

    @pl.when(j < NU)
    def _():
        lars(w_ref, v_ref, g_ref, wsq_ref, gsq_ref, wo_ref, vo_ref, UB)

    @pl.when(j >= NU)
    def _():
        lars(wt_ref, vt_ref, gt_ref, tsq_ref, fsq_ref, wto_ref, vto_ref, FB)


def update_all(*args):
    conv = pl.BlockSpec((UB, COUT), lambda j: (jnp.minimum(j, NU - 1), 0))
    fc = pl.BlockSpec((FB, COUT), lambda j: (jnp.clip(j - NU, 0, NF - 1), 0))
    vec, bvec, one = (1, COUT), (1, CLASSES), (1, 1)
    vs, bs = whole(*vec), whole(*bvec)
    big, fcs = struct((CIN, COUT)), struct((CLASSES, COUT))
    return pl.pallas_call(
        update_kernel,
        grid=(NU + NF,),
        in_specs=[pl.BlockSpec(memory_space=pltpu.SMEM), conv, conv, conv, whole(SUB, CB), whole(SUB, CB), fc, fc, fc, whole(SUB, COUT), whole(SUB, COUT),
                  bs, bs, whole(SUB, KP), whole(SUB, KP), vs, vs, vs, vs, whole(2, COUT)],
        out_specs=[conv, conv, fc, fc, bs, bs, vs, vs, vs, vs, whole(*one)],
        out_shape=[big, big, fcs, fcs] + [struct(bvec)] * 2 + [struct(vec)] * 4 + [struct(one)],
        compiler_params=pltpu.CompilerParams(vmem_limit_bytes=63 * MIB),
        cost_estimate=pl.CostEstimate(flops=CIN * COUT * 16, bytes_accessed=10 * CIN * COUT * 4, transcendentals=0),
        name="update",
    )(*args)


def solution(mesh):
    def local_step(act_in, shortcut, labels, w_conv, gamma, beta, w_fc, fc_bias, vel_conv, vel_gamma, vel_beta, vel_fc, vel_bias, lr):
        a = act_in.transpose(1, 2, 0, 3).reshape(ROWS, CIN)
        s = shortcut.transpose(1, 2, 0, 3).reshape(ROWS, COUT)
        wt = w_fc.T
        bias = fc_bias[None]
        z, at, pall, ptail, lab, wsq, tsq, wtb, da, sc, sh, bb, cc, dgb = forward(a, w_conv, s, gamma[None], beta[None], labels[None], bias, wt)
        g8, dgb, gsq, gfc, fsq, gb, ls = backward(at, z, s, sc, sh, bb, cc, da, dgb, pall, ptail, wtb, lab, bias)
        wo, vo, wto, vto, bo, vbo, go, vgo, beo, vbeo, loss = update_all(
            lr.reshape(1), w_conv, vel_conv, g8.reshape(CIN, COUT), wsq, gsq, wt, vel_fc.T, gfc, tsq, fsq, bias, vel_bias[None], gb, ls,
            gamma[None], beta[None], vel_gamma[None], vel_beta[None], dgb)
        return (wo, go[0], beo[0], wto.T, bo[0], vo, vgo[0], vbeo[0], vto.T, vbo[0], loss[0, 0])

    return jax.shard_map(local_step, mesh=mesh, in_specs=(P('dp'),) * 3 + (P(),) * 11, out_specs=(P(),) * 11, check_vma=False)
```

```python
import functools
import jax
import jax.numpy as jnp
from jax import lax
from jax.experimental import pallas as pl
from jax.experimental.pallas import tpu as pltpu
from jax.sharding import PartitionSpec as P

BN_EPS = 1e-5
SMOOTHING = 0.1
MOMENTUM = 0.9
TRUST_COEF = 0.001
WEIGHT_DECAY = 5e-5

LANES = 128
SUB = 8
IMG = 128
POS = 49
ROWS = IMG * POS
CIN = 1024
COUT = 2048
CLASSES = 1000
KP = 1024
DEVS = 8
TOTAL = DEVS * IMG
CB = 256
HC = CB // 2
NB = COUT // CB
CH = 7
NCH = POS // CH
NT = 16
PIECES = 8
BPIECES = 4
APAD = CIN + LANES
TAIL = 1
NG = 6
NP = NB - NG
PG, PT = NG * CB, NP * CB
LAGS = (2, 3, 4, 6, 8, 9)
BTAIL = LAGS[-1]
QR = CIN // DEVS
HALF = CIN // 2
BIG = 1792
BTILE = BIG // IMG
NBIG = ROWS // BIG
UB = 256
NU = CIN // UB
LB = 256
MIB = 1024 * 1024
F32 = jnp.float32
BF16 = jnp.bfloat16
MESH = pl.DeviceIdType.MESH
XN, YN, PN = 'x', 'y', 'core'


def dot(a, b):
    return jnp.dot(a, b, preferred_element_type=F32)


def dot_t(a, b):
    return lax.dot_general(a, b, (((1,), (1,)), ((), ())), preferred_element_type=F32)


def fold(v, axis=0):
    return jnp.sum(v.reshape(v.shape[0] // SUB, SUB, v.shape[1]), axis=axis)


def rowsum(v, axis=0):
    return jnp.sum(v, axis=axis, keepdims=True)


def lanesum(v, axis=1):
    return jnp.sum(v, axis=axis, keepdims=True)


def cols(b, size=CB, at=0):
    return pl.ds(pl.multiple_of(b * CB + at, LANES), size)


def span(i, size):
    return pl.ds(pl.multiple_of(i * size, SUB), size)


def position():
    me = lax.axis_index('dp')
    return me, lax.rem(me, 2), lax.rem(me // 2, 2), me // 4


def dev(core, x, y):
    return (y * 2 + x) * 2 + core


def neighbour(name):
    me, core, x, y = position()
    flip = lambda v, k: 1 - v if k == name else v
    return dev(flip(core, PN), flip(x, XN), flip(y, YN))


def enter_all():
    me = lax.axis_index('dp')
    bar = pltpu.get_barrier_semaphore()
    for k in range(1, DEVS):
        pl.semaphore_signal(bar, inc=1, device_id=(lax.rem(me + k, DEVS),), device_id_type=MESH)
    pl.semaphore_wait(bar, DEVS - 1)


def rcopy(src, dst, send, recv, target):
    return pltpu.make_async_remote_copy(src_ref=src, dst_ref=dst, send_sem=send, recv_sem=recv, device_id=(target,), device_id_type=MESH)


def each(fn, copies):
    for c in copies:
        fn(c)


def start(c):
    c.start()


def wait(c):
    c.wait()


def wait_send(c):
    c.wait_send()


def wait_recv(c):
    c.wait_recv()


def gather_own(buf, send, recv, b, ka=0, kb=1):
    me, core, x, y = position()
    a, c = buf.at[core, y, x, :, cols(b, HC)], buf.at[core, y, x, :, cols(b, HC, HC)]
    return rcopy(a, a, send.at[ka, b], recv.at[ka, b], neighbour(YN)), rcopy(c, c, send.at[kb, b], recv.at[kb, b], neighbour(XN))


def gather_on(buf, send, recv, b, ka=2, kb=3):
    me, core, x, y = position()
    a, c = buf.at[core, :, x, :, cols(b, HC)], buf.at[core, y, :, :, cols(b, HC, HC)]
    return rcopy(a, a, send.at[ka, b], recv.at[ka, b], neighbour(XN)), rcopy(c, c, send.at[kb, b], recv.at[kb, b], neighbour(YN))


def gather_core(buf, send, recv, b, k=4):
    me, core, x, y = position()
    a = buf.at[core, :, :, :, cols(b)]
    return (rcopy(a, a, send.at[k, b], recv.at[k, b], neighbour(PN)),)


def gather_all(*a):
    return gather_own(*a) + gather_on(*a) + gather_core(*a)


def stage_list(j, blocks, fns, lags):
    for fn, lag in zip(fns, lags):
        b = j - lag
        pl.when(jnp.logical_and(b >= 0, b < blocks))(functools.partial(fn, b))


def loop(lo, hi, fn):
    def body(i, carry):
        fn(i)
        return carry
    lax.fori_loop(lo, hi, body, 0)


def pieces():
    return [(c, y, x) for c in range(2) for y in range(2) for x in range(2)]


def softmax_terms(logits, bias, labels):
    n = logits.shape[0]
    cls = lax.broadcasted_iota(jnp.int32, (n, KP), 1)
    valid = cls < CLASSES
    lg = jnp.where(valid, logits + bias, -1e30)
    sh = lg - jnp.max(lg, axis=1, keepdims=True)
    lp = sh - jnp.log(lanesum(jnp.exp(sh)))
    lab = jnp.concatenate([labels] * (KP // LANES), axis=1)
    hit = lab == cls.astype(F32)
    tg = jnp.where(valid, SMOOTHING / CLASSES + jnp.where(hit, 1.0 - SMOOTHING, 0.0), 0.0)
    return tg * lp, (jnp.exp(lp) - tg) * (1.0 / TOTAL)


def label_rows(row):
    return jnp.broadcast_to(row.astype(F32), (IMG, IMG)).T


def set_bias(bpad, bias_ref):
    bpad[:] = jnp.zeros_like(bpad)
    bpad[:, :CLASSES] = bias_ref[:]


def fwd_kernel(a_hbm, w_ref, s_ref, g_ref, b_ref, lab_ref, bias_ref, wt_ref,
               z_hbm, at_ref, pall_ref, ptail_ref, lall_ref, wsq_ref, fsq_ref, wtb_hbm, da_ref, sc_ref, sh_ref, bb_ref, cc_ref, db_ref,
               abf, z0, z1, wbf, stat, pfull, lfull, pool, cnt, sx, sv, wtb, bpad, asem, zsem, osem, gs, gr, ls, lr):
    j = pl.program_id(0)
    zs = (z0, z1)
    me, core, x, y = position()
    crow = CH * IMG

    def a_copy(i):
        r = span(i, crow)
        return pltpu.make_async_copy(a_hbm.at[r, :], abf.at[r, :CIN], asem.at[i])

    def z_copy(jj, par):
        return pltpu.make_async_copy(zs[par], z_hbm.at[jj], zsem.at[par])

    def wtb_copy():
        return pltpu.make_async_copy(wtb, wtb_hbm, osem)

    def label_copy(k):
        return rcopy(lab_ref, lfull.at[core, y, x], ls.at[k], lr.at[k], lax.rem(me + k, DEVS))

    labels = [label_copy(k) for k in range(1, DEVS)]

    @pl.when(j == 0)
    def _():
        for i in range(NCH):
            a_copy(i).start()
        enter_all()
        each(start, labels)
        lfull[core, y, x] = lab_ref[:]
        wsq_ref[:] = jnp.zeros_like(wsq_ref)
        wtb[CLASSES:] = jnp.zeros((KP - CLASSES, COUT), BF16)
        set_bias(bpad, bias_ref)

    def second(b):
        each(wait_recv, gather_own(pfull, gs, gr, b))
        each(start, gather_on(pfull, gs, gr, b))

    def third(b):
        each(wait_recv, gather_on(pfull, gs, gr, b))
        each(start, gather_core(pfull, gs, gr, b))

    def last(b):
        each(wait_recv, gather_core(pfull, gs, gr, b))
        for q, (c, py, px) in enumerate(pieces()):
            pall_ref[span(q, IMG), :] = pfull[c, py, px, :, cols(b)].astype(BF16)

    def stages():
        stage_list(j, NG, (second, third, last), (2, 3, 4))

    def step(par, do_mm, do_post):
        first = not do_post
        slot, prev = zs[par], zs[1 - par]
        if do_post:
            pl.when(j >= 2)(lambda: z_copy(j - 2, par).wait())
        if do_mm:
            wf = w_ref[:]
            wsq_ref[:] += fold(wf * wf)
            wtf = wt_ref[:]
            fsq_ref[:, cols(j)] = fold(wtf * wtf)
            wtb[:CLASSES, cols(j)] = wtf.astype(BF16)
            w = wf.astype(BF16)
            wbf[:] = w
            if first:
                a_copy(0).wait()
            m0 = rowsum(dot(abf[:IMG, :CIN], w)) * (1.0 / IMG)
            stat[:2 * SUB] = jnp.zeros((2 * SUB, CB), F32)
        if do_post and not do_mm:
            wtb_copy().start()
        if do_post:
            mean = stat[2 * SUB:2 * SUB + 1]
            inv = stat[3 * SUB:3 * SUB + 1]
            sc = g_ref[:] * inv
            sh = b_ref[:] - mean * sc
            pool[:] = jnp.zeros_like(pool)
            pc = cols(j - 1)
            cnt[:, pc] = jnp.zeros((IMG, CB), F32)
            sx[:, pc] = jnp.zeros((IMG, CB), F32)

        def post(base, n, slabs):
            nr = slice(n, n + NT)
            pa, ca, xa = pool[nr], cnt[nr, pc], sx[nr, pc]
            for p in range(slabs):
                r = pl.ds(base + p * IMG + n, NT)
                zz = prev[r, :]
                u = zz * sc + sh + s_ref[r, :].astype(F32)
                mk = u > 0
                pa = pa + jnp.maximum(u, 0.0)
                ca = ca + jnp.where(mk, 1.0, 0.0)
                xa = xa + jnp.where(mk, zz, 0.0)
            pool[nr], cnt[nr, pc], sx[nr, pc] = pa, ca, xa

        def flip(base, rows):
            r = pl.ds(base, rows)
            at_ref[:, r] = abf[r, pl.ds(pl.multiple_of(j * IMG, IMG), IMG)].astype(F32).T.astype(BF16)

        def region(base, slabs, parts):
            size = slabs * IMG // parts
            for k in range(parts):
                if do_mm:
                    r = pl.ds(base + k * size, size)
                    zc = dot(abf[r, :CIN], wbf[:])
                if do_post:
                    for n in range(k * IMG // parts, (k + 1) * IMG // parts, NT):
                        post(base, n, slabs)
                if do_mm:
                    slot[r, :] = zc
                    d = zc - m0
                    stat[:SUB] += fold(d)
                    stat[SUB:2 * SUB] += fold(d * d)

            if do_mm:
                flip(base, slabs * IMG)

        def chunk(i, carry):
            if first:
                pl.when(i > 0)(lambda: a_copy(i).wait())
            region(pl.multiple_of(i * crow, crow), CH, 4)
            return carry

        def chunk2(i, carry):
            pl.when(i == 2)(stages)
            region(pl.multiple_of(i * 2 * crow, 2 * crow), 2 * CH, PIECES)
            return carry

        if first:
            lax.fori_loop(0, NCH, chunk, 0)
        else:
            lax.fori_loop(0, NCH // 2, chunk2, 0)
            region(pl.multiple_of((jnp.minimum(me, 0) + NCH - 1) * crow, crow), CH, 4)
        if do_post:
            pfull[core, y, x, :, pc] = pool[:] * (1.0 / POS)
            sx[:, pc] = (sx[:, pc] - mean * cnt[:, pc]) * inv
            sv[:1, pc] = mean
            sv[SUB:SUB + 1, pc] = inv
            sc_ref[:, pc] = sc
            sh_ref[:, pc] = sh
            pl.when(j - 1 < NG)(lambda: each(start, gather_own(pfull, gs, gr, j - 1)))
        if do_mm:
            dm = rowsum(stat[:SUB]) * (1.0 / ROWS)
            q = rowsum(stat[SUB:2 * SUB]) * (1.0 / ROWS)
            stat[2 * SUB:2 * SUB + 1] = m0 + dm
            stat[3 * SUB:3 * SUB + 1] = lax.rsqrt(jnp.maximum(q - dm * dm, 0.0) + BN_EPS)
            z_copy(j, par).start()

    @pl.when(j == 0)
    def _():
        step(0, True, False)

    for par in range(2):
        @pl.when(jnp.logical_and(jnp.logical_and(j > 0, j < NB), lax.rem(j, 2) == par))
        def _():
            step(par, True, True)

    @pl.when(j == NB)
    def _():
        step(0, False, True)

    @pl.when(j == NB + 1)
    def _():
        stages()
        ptail_ref[:] = pfull[core, y, x, :, PG:]
        lg = dot_t(pfull[core, y, x].astype(BF16), wtb[:])
        _, dl = softmax_terms(lg, bpad[:], label_rows(lab_ref[:]))
        dlb = dl.astype(BF16)

        def col(b, carry):
            c = cols(b)
            dp = dot(dlb, wtb[:, c]) * (1.0 / POS)
            dbeta = rowsum(dp * cnt[:, c])
            dgamma = rowsum(dp * sx[:, c])
            sc = sc_ref[:, c]
            cc = -(sc * sv[SUB:SUB + 1, c]) * (dgamma * (1.0 / ROWS))
            cc_ref[:, c] = cc
            bb_ref[:, c] = -sc * (dbeta * (1.0 / ROWS)) - sv[:1, c] * cc
            da_ref[:, c] = dp * sc
            db_ref[:1, c] = dgamma
            db_ref[1:, c] = dbeta
            return carry
        lax.fori_loop(0, NB, col, 0)

        each(wait, labels)
        lall_ref[:] = lfull[:]
        wtb_copy().wait()
        z_copy(NB - 1, 1).wait()
        loop(0, NG, lambda b: each(wait_send, gather_all(pfull, gs, gr, b)))


def whole(*shape):
    return pl.BlockSpec(shape, lambda j: (0,) * len(shape))


def struct(shape, dtype=F32):
    return jax.ShapeDtypeStruct(shape, dtype)


def fvmem(*shape):
    return pltpu.VMEM(shape, F32)


def bvmem(*shape):
    return pltpu.VMEM(shape, BF16)


def dma(*shape):
    return pltpu.SemaphoreType.DMA(shape)


HBM = pl.BlockSpec(memory_space=pl.ANY)
QUAD = (2, 2, 2)


def forward(a, w, s, gamma, beta, labels, bias, wt):
    prev = lambda j: (0, jnp.clip(j - 1, 0, NB - 1))
    cur = lambda j: (0, jnp.minimum(j, NB - 1))
    late = lambda j: (0, jnp.clip(j - 4, 0, NG - 1))
    vec, lab = (1, COUT), QUAD + (1, IMG)
    return pl.pallas_call(
        fwd_kernel,
        grid=(NB + 1 + TAIL,),
        in_specs=[HBM, pl.BlockSpec((CIN, CB), cur), pl.BlockSpec((ROWS, CB), prev), pl.BlockSpec((1, CB), prev), pl.BlockSpec((1, CB), prev),
                  whole(1, IMG), whole(1, CLASSES), pl.BlockSpec((CLASSES, CB), cur)],
        out_specs=[HBM, pl.BlockSpec((IMG, ROWS), lambda j: (jnp.minimum(j, NB - 1), 0)), pl.BlockSpec((TOTAL, CB), late), whole(IMG, PT), whole(*lab),
                   whole(SUB, CB), whole(SUB, COUT), HBM, whole(IMG, COUT)] + [whole(*vec)] * 4 + [whole(2, COUT)],
        out_shape=[struct((NB, ROWS, CB)), struct((CIN, ROWS), BF16), struct((TOTAL, PG), BF16), struct((IMG, PT)), struct(lab, jnp.int32),
                   struct((SUB, CB)), struct((SUB, COUT)), struct((KP, COUT), BF16), struct((IMG, COUT))] + [struct(vec)] * 4 + [struct((2, COUT))],
        scratch_shapes=[bvmem(ROWS, APAD), fvmem(ROWS, CB), fvmem(ROWS, CB), bvmem(CIN, CB), fvmem(4 * SUB, CB), fvmem(*QUAD, IMG, COUT), pltpu.VMEM(lab, jnp.int32),
                        fvmem(IMG, CB), fvmem(IMG, COUT), fvmem(IMG, COUT), fvmem(2 * SUB, COUT), bvmem(KP, COUT), fvmem(1, KP),
                        dma(NCH), dma(2), pltpu.SemaphoreType.DMA, dma(5, NG), dma(5, NG), dma(DEVS), dma(DEVS)],
        compiler_params=pltpu.CompilerParams(vmem_limit_bytes=63 * MIB, collective_id=0, has_side_effects=True),
        cost_estimate=pl.CostEstimate(flops=2 * ROWS * CIN * COUT, bytes_accessed=2 * ROWS * COUT * 4, transcendentals=0),
        name="fwd_conv",
    )(a, w, s, gamma, beta, labels, bias, wt)


def bwd_kernel(at_hbm, z_ref, s_ref, sc_ref, sh_ref, bb_ref, cc_ref, da_ref, db_ref, pall_hbm, ptail_hbm, wtb_hbm, lab_ref, bias_ref,
               g_hbm, dbo_ref, gsq_ref, gfc_hbm, fsq_ref, gb_ref, loss_ref,
               atv, dz0, dz1, dw, rd, ha, hb, ra, rb, ka, kb, r2a, r2b, gfull, dball, ptail, bpad, ps, pr, ss, rs, gs, gr, bs, br, osem, isem, fsem):
    j = pl.program_id(0)
    dzs = (dz0, dz1)
    me, core, x, y = position()
    plan = pl.ds(0, COUT)
    pall = atv.at[:, plan]
    wtb = atv.at[:, pl.ds(COUT, COUT)]
    dlt = atv.at[:, pl.ds(2 * COUT, TOTAL)]

    at_copy = pltpu.make_async_copy(at_hbm, atv, isem.at[0])
    pall_copy = pltpu.make_async_copy(pall_hbm, atv.at[:, pl.ds(0, PG)], isem.at[1])
    wtb_copy = pltpu.make_async_copy(wtb_hbm, wtb, isem.at[2])
    ptail_copy = pltpu.make_async_copy(ptail_hbm, ptail.at[core, y, x], isem.at[3])
    db_copies = [rcopy(db_ref, dball.at[me], bs.at[k], br.at[k], lax.rem(me + k, DEVS)) for k in range(1, DEVS)]

    @pl.when(j == 0)
    def _():
        ptail_copy.start()
        at_copy.start()
        enter_all()
        ptail_copy.wait()
        for b in range(NP):
            each(start, gather_own(ptail, ps, pr, b))
        each(start, db_copies)
        dball[me] = db_ref[:]
        for r in (gsq_ref, fsq_ref, gb_ref, loss_ref):
            r[:] = jnp.zeros_like(r)
        set_bias(bpad, bias_ref)

    @pl.when(j == 1)
    def _():
        at_copy.wait()

    def out_copy(b):
        c = cols(b)
        return pltpu.make_async_copy(gfull.at[:, :, :, :, c], g_hbm.at[:, :, :, :, c], osem.at[b])

    def core_copy(b, k=0):
        return rcopy(dw.at[lax.rem(b, 2), span(1 - core, HALF), :], rd.at[b], ss.at[k, b], rs.at[k, b], neighbour(PN))

    def first_copies(b, k=1, m=2):
        sl = lax.rem(b, 2)
        return (rcopy(ha.at[sl, 1 - x], ra.at[b], ss.at[k, b], rs.at[k, b], neighbour(XN)),
                rcopy(hb.at[sl, 1 - y], rb.at[b], ss.at[m, b], rs.at[m, b], neighbour(YN)))

    def second_copies(b, k=3, m=4):
        sl = lax.rem(b, 2)
        return (rcopy(ka.at[sl, 1 - y], r2a.at[b], ss.at[k, b], rs.at[k, b], neighbour(YN)),
                rcopy(kb.at[sl, 1 - x], r2b.at[b], ss.at[m, b], rs.at[m, b], neighbour(XN)))

    def stage1(b):
        core_copy(b).wait()
        sl = lax.rem(b, 2)
        for q, (py, px) in enumerate((py, px) for py in range(2) for px in range(2)):
            own = pl.ds(pl.multiple_of(core * HALF + q * QR, QR), QR)
            got = slice(q * QR, (q + 1) * QR)
            ha[sl, px, py] = dw[sl, own, :HC] + rd[b, got, :HC]
            hb[sl, py, px] = dw[sl, own, HC:] + rd[b, got, HC:]
        each(start, first_copies(b))

    def stage2(b):
        sl = lax.rem(b, 2)
        each(wait, first_copies(b))
        for k in range(2):
            ka[sl, k] = ha[sl, x, k] + ra[b, k]
            kb[sl, k] = hb[sl, y, k] + rb[b, k]
        each(start, second_copies(b))

    def stage3(b):
        sl = lax.rem(b, 2)
        each(wait, second_copies(b))
        gfull[core, y, x, :, cols(b, HC)] = ka[sl, y] + r2a[b]
        gfull[core, y, x, :, cols(b, HC, HC)] = kb[sl, x] + r2b[b]
        each(start, gather_own(gfull, gs, gr, b))

    def stage4(b):
        each(wait_recv, gather_own(gfull, gs, gr, b))
        each(start, gather_on(gfull, gs, gr, b))

    def stage5(b):
        each(wait_recv, gather_on(gfull, gs, gr, b))
        each(start, gather_core(gfull, gs, gr, b))

    def stage6(b):
        each(wait_recv, gather_core(gfull, gs, gr, b))
        out_copy(b).start()
        acc = gsq_ref[:]
        for q in pieces():
            gv = gfull[q + (slice(None), cols(b))]
            acc = acc + fold(gv * gv)
        gsq_ref[:] = acc

    def pooled_on():
        for b in range(NP):
            each(wait_recv, gather_own(ptail, ps, pr, b))
            each(start, gather_on(ptail, ps, pr, b))

    def pooled_core():
        for b in range(NP):
            each(wait_recv, gather_on(ptail, ps, pr, b))
            each(start, gather_core(ptail, ps, pr, b))

    def stages():
        stage_list(j, NB, (stage1, stage2, stage3, stage4, stage5, stage6), LAGS)
        pl.when(j == 1)(pooled_on)
        pl.when(j == 3)(pooled_core)

    def step(par, do_pre, do_mm):
        slot, prev = dzs[par], dzs[1 - par]
        out = dw.at[1 - par]
        if do_pre:
            sc, sh, bb, cc = sc_ref[:], sh_ref[:], bb_ref[:], cc_ref[:]

        def pre(base, n):
            da = da_ref[n:n + NT, :]
            for p in range(CH):
                r = pl.ds(base + p * IMG + n, NT)
                zz = z_ref[r, :]
                u = zz * sc + sh + s_ref[r, :].astype(F32)
                slot[r, :] = (jnp.where(u > 0, da, 0.0) + (zz * cc + bb)).astype(BF16)

        def body(base, slabs, add):
            work = [functools.partial(pre, base + p * IMG, n) for p in range(0, slabs, CH) for n in range(0, IMG, NT)]
            size = slabs * IMG
            for k in range(BPIECES):
                m = slice(k * CIN // BPIECES, (k + 1) * CIN // BPIECES)
                if do_mm:
                    g = dot(atv[m, pl.ds(base, size)], prev[pl.ds(base, size), :])
                if do_pre:
                    n = len(work)
                    for f in work[k * n // BPIECES:(k + 1) * n // BPIECES]:
                        f()
                if do_mm:
                    out[m] = out[m] + g if add else g

        rest = NBIG * BIG
        body(rest, POS - NBIG * BTILE, False)

        def chunk(i, carry):
            base = pl.multiple_of(i * BIG, BIG)
            if do_mm:
                pl.when(i == 1)(stages)
            body(base, BTILE, True)
            return carry
        lax.fori_loop(0, NBIG, chunk, 0)
        if do_mm:
            core_copy(j - 1).start()

    @pl.when(j == 0)
    def _():
        step(0, True, False)

    for par in range(2):
        @pl.when(jnp.logical_and(jnp.logical_and(j > 0, j < NB), lax.rem(j, 2) == par))
        def _():
            step(par, True, True)

    def logits_unit(i):
        rows = span(i, LB)
        lg = dot_t(pall[rows, :], wtb[:])
        lab = jnp.concatenate([label_rows(lab_ref[i // 2, lax.rem(i, 2), k]) for k in range(2)])
        lterm, dl = softmax_terms(lg, bpad[:], lab)
        loss_ref[:] += fold(lterm)
        gb_ref[:] += fold(dl)
        dlt[:, pl.ds(pl.multiple_of(i * LB, LB), LB)] = dl.T.astype(BF16)

    def fc_copies(c):
        sl = lax.rem(c, 4)
        return [pltpu.make_async_copy(rd.at[sl * 2 + h], gfc_hbm.at[pl.ds(h * HALF, HALF), cols(c)], fsem.at[h, c]) for h in range(2)]

    def dfc_unit(c):
        pl.when(c >= 4)(lambda: each(wait, fc_copies(c - 4)))
        acc = jnp.zeros((SUB, CB), F32)
        for h in range(2):
            g = dot(dlt[pl.ds(h * HALF, HALF), :], pall[:, cols(c)])
            rd[lax.rem(c, 4) * 2 + h] = g
            acc = acc + fold(g * g)
        fsq_ref[:, cols(c)] = acc
        each(start, fc_copies(c))

    @pl.when(j == NB)
    def _():
        step(0, False, True)
        pall_copy.start()
        wtb_copy.start()

    @pl.when(j > NB)
    def _():
        stages()
        k = j - NB - 1

        @pl.when(k == 0)
        def _():
            for b in range(NP):
                each(wait_recv, gather_core(ptail, ps, pr, b))
            for q, (c, py, px) in enumerate(pieces()):
                atv[span(q, IMG), PG:COUT] = ptail[c, py, px].astype(BF16)
            pall_copy.wait()
            wtb_copy.wait()

        loop(jnp.minimum(k * 3, 4), jnp.minimum(k * 3 + 3, 4), logits_unit)
        loop(jnp.clip(k * 3 - 3, 0, NB), jnp.clip(k * 3, 0, NB), dfc_unit)

    @pl.when(j == NB + BTAIL - 1)
    def _():
        each(wait, db_copies)
        acc = dball[0]
        for k in range(1, DEVS):
            acc = acc + dball[k]
        dbo_ref[:] = acc
        for c in range(4, NB):
            each(wait, fc_copies(c))

        def drain(b):
            each(wait_send, gather_all(gfull, gs, gr, b))
            out_copy(b).wait()
        loop(0, NB, drain)
        loop(0, NP, lambda b: each(wait_send, gather_all(ptail, ps, pr, b)))


def backward(*args):
    cur = lambda j: (0, jnp.minimum(j, NB - 1))
    row = pl.BlockSpec((1, CB), cur)
    pair, quad, side = (2, QR, HC), (2, 2, 2, QR, HC), (NB, QR, HC)
    return pl.pallas_call(
        bwd_kernel,
        grid=(NB + BTAIL,),
        in_specs=[HBM, pl.BlockSpec((None, ROWS, CB), lambda j: (jnp.minimum(j, NB - 1), 0, 0)), pl.BlockSpec((ROWS, CB), cur), row, row, row, row,
                  pl.BlockSpec((IMG, CB), cur), whole(2, COUT), HBM, HBM, HBM, whole(2, 2, 2, 1, IMG), whole(1, CLASSES)],
        out_specs=[HBM, whole(2, COUT), whole(SUB, CB), HBM, whole(SUB, COUT), whole(SUB, KP), whole(SUB, KP)],
        out_shape=[struct(QUAD + (QR, COUT)), struct((2, COUT)), struct((SUB, CB)), struct((KP, COUT)), struct((SUB, COUT)), struct((SUB, KP)), struct((SUB, KP))],
        scratch_shapes=[bvmem(CIN, ROWS), bvmem(ROWS, CB), bvmem(ROWS, CB), fvmem(2, CIN, CB), fvmem(NB, HALF, CB), fvmem(*quad), fvmem(*quad),
                        fvmem(NB, *pair), fvmem(NB, *pair), fvmem(2, *pair), fvmem(2, *pair), fvmem(*side), fvmem(*side),
                        fvmem(*QUAD, QR, COUT), fvmem(DEVS, 2, COUT), fvmem(*QUAD, IMG, PT), fvmem(1, KP),
                        dma(5, NP), dma(5, NP), dma(5, NB), dma(5, NB), dma(5, NB), dma(5, NB), dma(DEVS), dma(DEVS), dma(NB), dma(4), dma(2, NB)],
        compiler_params=pltpu.CompilerParams(vmem_limit_bytes=63 * MIB, collective_id=1, has_side_effects=True),
        cost_estimate=pl.CostEstimate(flops=2 * ROWS * CIN * COUT, bytes_accessed=2 * ROWS * COUT * 4, transcendentals=0),
        name="bwd_conv",
    )(*args)


def trust_of(wsq, gsq):
    wn = jnp.sqrt(lanesum(rowsum(wsq)))
    gn = jnp.sqrt(lanesum(rowsum(gsq)))
    return TRUST_COEF * wn / (gn + WEIGHT_DECAY * wn)


def update_kernel(lr_ref, w_ref, v_ref, g_ref, wsq_ref, gsq_ref, wt_ref, vt_ref, gt_ref, tsq_ref, fsq_ref, bias_ref, vbias_ref, gb_ref, ls_ref,
                  gam_ref, bet_ref, vgam_ref, vbet_ref, dgb_ref,
                  wo_ref, vo_ref, wto_ref, vto_ref, bo_ref, vbo_ref, go_ref, vgo_ref, beo_ref, vbeo_ref, loss_ref):
    j = pl.program_id(0)
    lr = lr_ref[0]

    def plain(p, v, g, po, vo):
        nv = MOMENTUM * v[:] + lr * g
        vo[:] = nv
        po[:] = p[:] - nv

    @pl.when(j == 0)
    def _():
        plain(gam_ref, vgam_ref, dgb_ref[:1], go_ref, vgo_ref)
        plain(bet_ref, vbet_ref, dgb_ref[1:], beo_ref, vbeo_ref)
        plain(bias_ref, vbias_ref, rowsum(gb_ref[:])[:, :CLASSES], bo_ref, vbo_ref)
        loss_ref[:] = lanesum(rowsum(ls_ref[:])) * (-1.0 / TOTAL)

    def lars(w_ref, v_ref, g_ref, wsq, gsq, wo, vo, rows):
        rate = jnp.broadcast_to(lr * trust_of(wsq[:], gsq[:]), (SUB, CB))

        def row(i, carry):
            for q in range(2):
                r = pl.ds(pl.multiple_of(i * 2 * SUB + q * SUB, SUB), SUB)
                for c in range(0, COUT, CB):
                    cc = slice(c, c + CB)
                    w = w_ref[r, cc]
                    nv = MOMENTUM * v_ref[r, cc] + rate * (g_ref[r, cc] + WEIGHT_DECAY * w)
                    vo[r, cc] = nv
                    wo[r, cc] = w - nv
            return carry
        lax.fori_loop(0, rows // (2 * SUB), row, 0)

    lars(w_ref, v_ref, g_ref, wsq_ref, gsq_ref, wo_ref, vo_ref, UB)
    lars(wt_ref, vt_ref, gt_ref, tsq_ref, fsq_ref, wto_ref, vto_ref, UB)


def update_all(*args):
    conv = fc = pl.BlockSpec((UB, COUT), lambda j: (j, 0))
    vec, bvec, one = (1, COUT), (1, CLASSES), (1, 1)
    vs, bs = whole(*vec), whole(*bvec)
    big, fcs = struct((CIN, COUT)), struct((CLASSES, COUT))
    return pl.pallas_call(
        update_kernel,
        grid=(NU,),
        in_specs=[pl.BlockSpec(memory_space=pltpu.SMEM), conv, conv, conv, whole(SUB, CB), whole(SUB, CB), fc, fc, fc, whole(SUB, COUT), whole(SUB, COUT),
                  bs, bs, whole(SUB, KP), whole(SUB, KP), vs, vs, vs, vs, whole(2, COUT)],
        out_specs=[conv, conv, fc, fc, bs, bs, vs, vs, vs, vs, whole(*one)],
        out_shape=[big, big, fcs, fcs] + [struct(bvec)] * 2 + [struct(vec)] * 4 + [struct(one)],
        compiler_params=pltpu.CompilerParams(vmem_limit_bytes=63 * MIB),
        cost_estimate=pl.CostEstimate(flops=CIN * COUT * 16, bytes_accessed=10 * CIN * COUT * 4, transcendentals=0),
        name="update",
    )(*args)


def solution(mesh):
    def local_step(act_in, shortcut, labels, w_conv, gamma, beta, w_fc, fc_bias, vel_conv, vel_gamma, vel_beta, vel_fc, vel_bias, lr):
        a = act_in.transpose(1, 2, 0, 3).reshape(ROWS, CIN)
        s = shortcut.transpose(1, 2, 0, 3).reshape(ROWS, COUT)
        wt = w_fc.T
        bias = fc_bias[None]
        z, at, pall, ptail, lab, wsq, tsq, wtb, da, sc, sh, bb, cc, dgb = forward(a, w_conv, s, gamma[None], beta[None], labels[None], bias, wt)
        g8, dgb, gsq, gfc, fsq, gb, ls = backward(at, z, s, sc, sh, bb, cc, da, dgb, pall, ptail, wtb, lab, bias)
        wo, vo, wto, vto, bo, vbo, go, vgo, beo, vbeo, loss = update_all(
            lr.reshape(1), w_conv, vel_conv, g8.reshape(CIN, COUT), wsq, gsq, wt, vel_fc.T, gfc, tsq, fsq, bias, vel_bias[None], gb, ls,
            gamma[None], beta[None], vel_gamma[None], vel_beta[None], dgb)
        return (wo, go[0], beo[0], wto.T, bo[0], vo, vgo[0], vbeo[0], vto.T, vbo[0], loss[0, 0])

    return jax.shard_map(local_step, mesh=mesh, in_specs=(P('dp'),) * 3 + (P(),) * 11, out_specs=(P(),) * 11, check_vma=False)
```

```python
import functools
import jax
import jax.numpy as jnp
from jax import lax
from jax.experimental import pallas as pl
from jax.experimental.pallas import tpu as pltpu
from jax.sharding import PartitionSpec as P

BN_EPS = 1e-5
SMOOTHING = 0.1
MOMENTUM = 0.9
TRUST_COEF = 0.001
WEIGHT_DECAY = 5e-5

LANES = 128
SUB = 8
IMG = 128
POS = 49
ROWS = IMG * POS
CIN = 1024
COUT = 2048
CLASSES = 1000
KP = 1024
DEVS = 8
TOTAL = DEVS * IMG
CB = 256
HC = CB // 2
NB = COUT // CB
CH = 7
NCH = POS // CH
NT = 16
PIECES = 8
BPIECES = 4
APAD = CIN + LANES
TAIL = 1
NG = 6
NP = NB - NG
PG, PT = NG * CB, NP * CB
LAGS = (2, 3, 4, 6, 8, 9)
BTAIL = LAGS[-1]
QR = CIN // DEVS
HALF = CIN // 2
BIG = 1792
BTILE = BIG // IMG
NBIG = ROWS // BIG
UB = 256
NU = CIN // UB
LB = 256
MIB = 1024 * 1024
F32 = jnp.float32
BF16 = jnp.bfloat16
MESH = pl.DeviceIdType.MESH
XN, YN, PN = 'x', 'y', 'core'


def dot(a, b):
    return jnp.dot(a, b, preferred_element_type=F32)


def dot_t(a, b):
    return lax.dot_general(a, b, (((1,), (1,)), ((), ())), preferred_element_type=F32)


def fold(v, axis=0):
    return jnp.sum(v.reshape(v.shape[0] // SUB, SUB, v.shape[1]), axis=axis)


def rowsum(v, axis=0):
    return jnp.sum(v, axis=axis, keepdims=True)


def lanesum(v, axis=1):
    return jnp.sum(v, axis=axis, keepdims=True)


def cols(b, size=CB, at=0):
    return pl.ds(pl.multiple_of(b * CB + at, LANES), size)


def span(i, size):
    return pl.ds(pl.multiple_of(i * size, SUB), size)


def position():
    me = lax.axis_index('dp')
    return me, lax.rem(me, 2), lax.rem(me // 2, 2), me // 4


def dev(core, x, y):
    return (y * 2 + x) * 2 + core


def neighbour(name):
    me, core, x, y = position()
    flip = lambda v, k: 1 - v if k == name else v
    return dev(flip(core, PN), flip(x, XN), flip(y, YN))


def enter_all():
    me = lax.axis_index('dp')
    bar = pltpu.get_barrier_semaphore()
    for k in range(1, DEVS):
        pl.semaphore_signal(bar, inc=1, device_id=(lax.rem(me + k, DEVS),), device_id_type=MESH)
    pl.semaphore_wait(bar, DEVS - 1)


def rcopy(src, dst, send, recv, target):
    return pltpu.make_async_remote_copy(src_ref=src, dst_ref=dst, send_sem=send, recv_sem=recv, device_id=(target,), device_id_type=MESH)


def each(fn, copies):
    for c in copies:
        fn(c)


def start(c):
    c.start()


def wait(c):
    c.wait()


def wait_send(c):
    c.wait_send()


def wait_recv(c):
    c.wait_recv()


def gather_own(buf, send, recv, b, ka=0, kb=1):
    me, core, x, y = position()
    a, c = buf.at[core, y, x, :, cols(b, HC)], buf.at[core, y, x, :, cols(b, HC, HC)]
    return rcopy(a, a, send.at[ka, b], recv.at[ka, b], neighbour(YN)), rcopy(c, c, send.at[kb, b], recv.at[kb, b], neighbour(XN))


def gather_on(buf, send, recv, b, ka=2, kb=3):
    me, core, x, y = position()
    a, c = buf.at[core, :, x, :, cols(b, HC)], buf.at[core, y, :, :, cols(b, HC, HC)]
    return rcopy(a, a, send.at[ka, b], recv.at[ka, b], neighbour(XN)), rcopy(c, c, send.at[kb, b], recv.at[kb, b], neighbour(YN))


def gather_core(buf, send, recv, b, k=4):
    me, core, x, y = position()
    a = buf.at[core, :, :, :, cols(b)]
    return (rcopy(a, a, send.at[k, b], recv.at[k, b], neighbour(PN)),)


def gather_all(*a):
    return gather_own(*a) + gather_on(*a) + gather_core(*a)


def stage_list(j, blocks, fns, lags):
    for fn, lag in zip(fns, lags):
        b = j - lag
        pl.when(jnp.logical_and(b >= 0, b < blocks))(functools.partial(fn, b))


def loop(lo, hi, fn):
    def body(i, carry):
        fn(i)
        return carry
    lax.fori_loop(lo, hi, body, 0)


def pieces():
    return [(c, y, x) for c in range(2) for y in range(2) for x in range(2)]


def softmax_terms(logits, bias, labels):
    n = logits.shape[0]
    cls = lax.broadcasted_iota(jnp.int32, (n, KP), 1)
    valid = cls < CLASSES
    lg = jnp.where(valid, logits + bias, -1e30)
    sh = lg - jnp.max(lg, axis=1, keepdims=True)
    lp = sh - jnp.log(lanesum(jnp.exp(sh)))
    lab = jnp.concatenate([labels] * (KP // LANES), axis=1)
    hit = lab == cls.astype(F32)
    tg = jnp.where(valid, SMOOTHING / CLASSES + jnp.where(hit, 1.0 - SMOOTHING, 0.0), 0.0)
    return tg * lp, (jnp.exp(lp) - tg) * (1.0 / TOTAL)


def label_rows(row):
    return jnp.broadcast_to(row.astype(F32), (IMG, IMG)).T


def set_bias(bpad, bias_ref):
    bpad[:] = jnp.zeros_like(bpad)
    bpad[:, :CLASSES] = bias_ref[:]


def fwd_kernel(a_hbm, w_ref, s_ref, g_ref, b_ref, lab_ref, bias_ref, wt_ref,
               z_hbm, at_ref, pall_ref, ptail_ref, lall_ref, wsq_ref, fsq_ref, wtb_hbm, da_ref, sc_ref, sh_ref, bb_ref, cc_ref, db_ref,
               abf, z0, z1, wbf, stat, pfull, lfull, pool, cnt, sx, sv, wtb, bpad, asem, zsem, osem, gs, gr, ls, lr):
    j = pl.program_id(0)
    zs = (z0, z1)
    me, core, x, y = position()
    crow = CH * IMG

    def a_copy(i):
        r = span(i, crow)
        return pltpu.make_async_copy(a_hbm.at[r, :], abf.at[r, :CIN], asem.at[i])

    def z_copy(jj, par):
        return pltpu.make_async_copy(zs[par], z_hbm.at[jj], zsem.at[par])

    def wtb_copy():
        return pltpu.make_async_copy(wtb, wtb_hbm, osem)

    def label_copy(k):
        return rcopy(lab_ref, lfull.at[core, y, x], ls.at[k], lr.at[k], lax.rem(me + k, DEVS))

    labels = [label_copy(k) for k in range(1, DEVS)]

    @pl.when(j == 0)
    def _():
        for i in range(NCH):
            a_copy(i).start()
        enter_all()
        each(start, labels)
        lfull[core, y, x] = lab_ref[:]
        wsq_ref[:] = jnp.zeros_like(wsq_ref)
        wtb[CLASSES:] = jnp.zeros((KP - CLASSES, COUT), BF16)
        set_bias(bpad, bias_ref)

    def second(b):
        each(wait_recv, gather_own(pfull, gs, gr, b))
        each(start, gather_on(pfull, gs, gr, b))

    def third(b):
        each(wait_recv, gather_on(pfull, gs, gr, b))
        each(start, gather_core(pfull, gs, gr, b))

    def last(b):
        each(wait_recv, gather_core(pfull, gs, gr, b))
        for q, (c, py, px) in enumerate(pieces()):
            pall_ref[span(q, IMG), :] = pfull[c, py, px, :, cols(b)].astype(BF16)

    def stages():
        stage_list(j, NG, (second, third, last), (2, 3, 4))

    def step(par, do_mm, do_post):
        first = not do_post
        slot, prev = zs[par], zs[1 - par]
        if do_post:
            pl.when(j >= 2)(lambda: z_copy(j - 2, par).wait())
        if do_mm:
            wf = w_ref[:]
            wsq_ref[:] += fold(wf * wf)
            wtf = wt_ref[:]
            fsq_ref[:, cols(j)] = fold(wtf * wtf)
            wtb[:CLASSES, cols(j)] = wtf.astype(BF16)
            w = wf.astype(BF16)
            wbf[:] = w
            if first:
                a_copy(0).wait()
            m0 = rowsum(dot(abf[:IMG, :CIN], w)) * (1.0 / IMG)
            stat[:2 * SUB] = jnp.zeros((2 * SUB, CB), F32)
        if do_post and not do_mm:
            wtb_copy().start()
        if do_post:
            mean = stat[2 * SUB:2 * SUB + 1]
            inv = stat[3 * SUB:3 * SUB + 1]
            sc = g_ref[:] * inv
            sh = b_ref[:] - mean * sc
            pool[:] = jnp.zeros_like(pool)
            pc = cols(j - 1)
            cnt[:, pc] = jnp.zeros((IMG, CB), F32)
            sx[:, pc] = jnp.zeros((IMG, CB), F32)

        def post(base, n, slabs):
            nr = slice(n, n + NT)
            pa, ca, xa = pool[nr], cnt[nr, pc], sx[nr, pc]
            for p in range(slabs):
                r = pl.ds(base + p * IMG + n, NT)
                zz = prev[r, :]
                u = zz * sc + sh + s_ref[r, :].astype(F32)
                mk = u > 0
                pa = pa + jnp.maximum(u, 0.0)
                ca = ca + jnp.where(mk, 1.0, 0.0)
                xa = xa + jnp.where(mk, zz, 0.0)
            pool[nr], cnt[nr, pc], sx[nr, pc] = pa, ca, xa

        def flip(base, rows):
            r = pl.ds(base, rows)
            at_ref[:, r] = abf[r, pl.ds(pl.multiple_of(j * IMG, IMG), IMG)].astype(F32).T.astype(BF16)

        def region(base, slabs, parts):
            size = slabs * IMG // parts
            for k in range(parts):
                if do_mm:
                    r = pl.ds(base + k * size, size)
                    zc = dot(abf[r, :CIN], wbf[:])
                if do_post:
                    for n in range(k * IMG // parts, (k + 1) * IMG // parts, NT):
                        post(base, n, slabs)
                if do_mm:
                    slot[r, :] = zc
                    d = zc - m0
                    stat[:SUB] += fold(d)
                    stat[SUB:2 * SUB] += fold(d * d)

            if do_mm:
                flip(base, slabs * IMG)

        def chunk(i, carry):
            if first:
                pl.when(i > 0)(lambda: a_copy(i).wait())
            region(pl.multiple_of(i * crow, crow), CH, 4)
            return carry

        def chunk2(i, carry):
            pl.when(i == 2)(stages)
            region(pl.multiple_of(i * 2 * crow, 2 * crow), 2 * CH, PIECES)
            return carry

        if first:
            lax.fori_loop(0, NCH, chunk, 0)
        else:
            lax.fori_loop(0, NCH // 2, chunk2, 0)
            region(pl.multiple_of((jnp.minimum(me, 0) + NCH - 1) * crow, crow), CH, 4)
        if do_post:
            pfull[core, y, x, :, pc] = pool[:] * (1.0 / POS)
            sx[:, pc] = (sx[:, pc] - mean * cnt[:, pc]) * inv
            sv[:1, pc] = mean
            sv[SUB:SUB + 1, pc] = inv
            sc_ref[:, pc] = sc
            sh_ref[:, pc] = sh
            pl.when(j - 1 < NG)(lambda: each(start, gather_own(pfull, gs, gr, j - 1)))
        if do_mm:
            dm = rowsum(stat[:SUB]) * (1.0 / ROWS)
            q = rowsum(stat[SUB:2 * SUB]) * (1.0 / ROWS)
            stat[2 * SUB:2 * SUB + 1] = m0 + dm
            stat[3 * SUB:3 * SUB + 1] = lax.rsqrt(jnp.maximum(q - dm * dm, 0.0) + BN_EPS)
            z_copy(j, par).start()

    @pl.when(j == 0)
    def _():
        step(0, True, False)

    for par in range(2):
        @pl.when(jnp.logical_and(jnp.logical_and(j > 0, j < NB), lax.rem(j, 2) == par))
        def _():
            step(par, True, True)

    @pl.when(j == NB)
    def _():
        step(0, False, True)

    @pl.when(j == NB + 1)
    def _():
        stages()
        ptail_ref[:] = pfull[core, y, x, :, PG:]
        lg = dot_t(pfull[core, y, x].astype(BF16), wtb[:])
        _, dl = softmax_terms(lg, bpad[:], label_rows(lab_ref[:]))
        dlb = dl.astype(BF16)

        def col(b, carry):
            c = cols(b)
            dp = dot(dlb, wtb[:, c]) * (1.0 / POS)
            dbeta = rowsum(dp * cnt[:, c])
            dgamma = rowsum(dp * sx[:, c])
            sc = sc_ref[:, c]
            cc = -(sc * sv[SUB:SUB + 1, c]) * (dgamma * (1.0 / ROWS))
            cc_ref[:, c] = cc
            bb_ref[:, c] = -sc * (dbeta * (1.0 / ROWS)) - sv[:1, c] * cc
            da_ref[:, c] = dp * sc
            db_ref[:1, c] = dgamma
            db_ref[1:, c] = dbeta
            return carry
        lax.fori_loop(0, NB, col, 0)

        each(wait, labels)
        lall_ref[:] = lfull[:]
        wtb_copy().wait()
        z_copy(NB - 1, 1).wait()
        loop(0, NG, lambda b: each(wait_send, gather_all(pfull, gs, gr, b)))


def whole(*shape):
    return pl.BlockSpec(shape, lambda j: (0,) * len(shape))


def struct(shape, dtype=F32):
    return jax.ShapeDtypeStruct(shape, dtype)


def fvmem(*shape):
    return pltpu.VMEM(shape, F32)


def bvmem(*shape):
    return pltpu.VMEM(shape, BF16)


def dma(*shape):
    return pltpu.SemaphoreType.DMA(shape)


HBM = pl.BlockSpec(memory_space=pl.ANY)
QUAD = (2, 2, 2)


def forward(a, w, s, gamma, beta, labels, bias, wt):
    prev = lambda j: (0, jnp.clip(j - 1, 0, NB - 1))
    cur = lambda j: (0, jnp.minimum(j, NB - 1))
    late = lambda j: (0, jnp.clip(j - 4, 0, NG - 1))
    vec, lab = (1, COUT), QUAD + (1, IMG)
    return pl.pallas_call(
        fwd_kernel,
        grid=(NB + 1 + TAIL,),
        in_specs=[HBM, pl.BlockSpec((CIN, CB), cur), pl.BlockSpec((ROWS, CB), prev), pl.BlockSpec((1, CB), prev), pl.BlockSpec((1, CB), prev),
                  whole(1, IMG), whole(1, CLASSES), pl.BlockSpec((CLASSES, CB), cur)],
        out_specs=[HBM, pl.BlockSpec((IMG, ROWS), lambda j: (jnp.minimum(j, NB - 1), 0)), pl.BlockSpec((TOTAL, CB), late), whole(IMG, PT), whole(*lab),
                   whole(SUB, CB), whole(SUB, COUT), HBM, whole(IMG, COUT)] + [whole(*vec)] * 4 + [whole(2, COUT)],
        out_shape=[struct((NB, ROWS, CB)), struct((CIN, ROWS), BF16), struct((TOTAL, PG), BF16), struct((IMG, PT)), struct(lab, jnp.int32),
                   struct((SUB, CB)), struct((SUB, COUT)), struct((KP, COUT), BF16), struct((IMG, COUT))] + [struct(vec)] * 4 + [struct((2, COUT))],
        scratch_shapes=[bvmem(ROWS, APAD), fvmem(ROWS, CB), fvmem(ROWS, CB), bvmem(CIN, CB), fvmem(4 * SUB, CB), fvmem(*QUAD, IMG, COUT), pltpu.VMEM(lab, jnp.int32),
                        fvmem(IMG, CB), fvmem(IMG, COUT), fvmem(IMG, COUT), fvmem(2 * SUB, COUT), bvmem(KP, COUT), fvmem(1, KP),
                        dma(NCH), dma(2), pltpu.SemaphoreType.DMA, dma(5, NG), dma(5, NG), dma(DEVS), dma(DEVS)],
        compiler_params=pltpu.CompilerParams(vmem_limit_bytes=63 * MIB, collective_id=0, has_side_effects=True),
        cost_estimate=pl.CostEstimate(flops=2 * ROWS * CIN * COUT, bytes_accessed=2 * ROWS * COUT * 4, transcendentals=0),
        name="fwd_conv",
    )(a, w, s, gamma, beta, labels, bias, wt)


def bwd_kernel(at_hbm, z_ref, s_ref, sc_ref, sh_ref, bb_ref, cc_ref, da_ref, db_ref, pall_hbm, ptail_hbm, wtb_hbm, lab_ref, bias_ref,
               g_hbm, dbo_ref, gsq_ref, gfc_hbm, fsq_ref, gb_ref, loss_ref,
               atv, dz0, dz1, dw, rd, ha, hb, ra, rb, ka, kb, r2a, r2b, gfull, dball, ptail, bpad, asem, ps, pr, ss, rs, gs, gr, bs, br, osem, isem, fsem):
    j = pl.program_id(0)
    dzs = (dz0, dz1)
    me, core, x, y = position()
    plan = pl.ds(0, COUT)
    pall = atv.at[:, plan]
    wtb = atv.at[:, pl.ds(COUT, COUT)]
    dlt = atv.at[:, pl.ds(2 * COUT, TOTAL)]


    def at_copy(i, size=BIG):
        c = pl.ds(pl.multiple_of(i * BIG, BIG), size)
        return pltpu.make_async_copy(at_hbm.at[:, c], atv.at[:, c], asem.at[i])

    at_rest = at_copy(NBIG, ROWS - NBIG * BIG)
    pall_copy = pltpu.make_async_copy(pall_hbm, atv.at[:, pl.ds(0, PG)], isem.at[1])
    wtb_copy = pltpu.make_async_copy(wtb_hbm, wtb, isem.at[2])
    ptail_copy = pltpu.make_async_copy(ptail_hbm, ptail.at[core, y, x], isem.at[3])
    db_copies = [rcopy(db_ref, dball.at[me], bs.at[k], br.at[k], lax.rem(me + k, DEVS)) for k in range(1, DEVS)]

    @pl.when(j == 0)
    def _():
        ptail_copy.start()
        at_rest.start()
        for i in range(NBIG):
            at_copy(i).start()
        enter_all()
        ptail_copy.wait()
        for b in range(NP):
            each(start, gather_own(ptail, ps, pr, b))
        each(start, db_copies)
        dball[me] = db_ref[:]
        for r in (gsq_ref, fsq_ref, gb_ref, loss_ref):
            r[:] = jnp.zeros_like(r)
        set_bias(bpad, bias_ref)

    def out_copy(b):
        c = cols(b)
        return pltpu.make_async_copy(gfull.at[:, :, :, :, c], g_hbm.at[:, :, :, :, c], osem.at[b])

    def core_copy(b, k=0):
        return rcopy(dw.at[lax.rem(b, 2), span(1 - core, HALF), :], rd.at[b], ss.at[k, b], rs.at[k, b], neighbour(PN))

    def first_copies(b, k=1, m=2):
        sl = lax.rem(b, 2)
        return (rcopy(ha.at[sl, 1 - x], ra.at[b], ss.at[k, b], rs.at[k, b], neighbour(XN)),
                rcopy(hb.at[sl, 1 - y], rb.at[b], ss.at[m, b], rs.at[m, b], neighbour(YN)))

    def second_copies(b, k=3, m=4):
        sl = lax.rem(b, 2)
        return (rcopy(ka.at[sl, 1 - y], r2a.at[b], ss.at[k, b], rs.at[k, b], neighbour(YN)),
                rcopy(kb.at[sl, 1 - x], r2b.at[b], ss.at[m, b], rs.at[m, b], neighbour(XN)))

    def stage1(b):
        core_copy(b).wait()
        sl = lax.rem(b, 2)
        for q, (py, px) in enumerate((py, px) for py in range(2) for px in range(2)):
            own = pl.ds(pl.multiple_of(core * HALF + q * QR, QR), QR)
            got = slice(q * QR, (q + 1) * QR)
            ha[sl, px, py] = dw[sl, own, :HC] + rd[b, got, :HC]
            hb[sl, py, px] = dw[sl, own, HC:] + rd[b, got, HC:]
        each(start, first_copies(b))

    def stage2(b):
        sl = lax.rem(b, 2)
        each(wait, first_copies(b))
        for k in range(2):
            ka[sl, k] = ha[sl, x, k] + ra[b, k]
            kb[sl, k] = hb[sl, y, k] + rb[b, k]
        each(start, second_copies(b))

    def stage3(b):
        sl = lax.rem(b, 2)
        each(wait, second_copies(b))
        gfull[core, y, x, :, cols(b, HC)] = ka[sl, y] + r2a[b]
        gfull[core, y, x, :, cols(b, HC, HC)] = kb[sl, x] + r2b[b]
        each(start, gather_own(gfull, gs, gr, b))

    def stage4(b):
        each(wait_recv, gather_own(gfull, gs, gr, b))
        each(start, gather_on(gfull, gs, gr, b))

    def stage5(b):
        each(wait_recv, gather_on(gfull, gs, gr, b))
        each(start, gather_core(gfull, gs, gr, b))

    def stage6(b):
        each(wait_recv, gather_core(gfull, gs, gr, b))
        out_copy(b).start()
        acc = gsq_ref[:]
        for q in pieces():
            gv = gfull[q + (slice(None), cols(b))]
            acc = acc + fold(gv * gv)
        gsq_ref[:] = acc

    def pooled_on():
        for b in range(NP):
            each(wait_recv, gather_own(ptail, ps, pr, b))
            each(start, gather_on(ptail, ps, pr, b))

    def pooled_core():
        for b in range(NP):
            each(wait_recv, gather_on(ptail, ps, pr, b))
            each(start, gather_core(ptail, ps, pr, b))

    def stages():
        stage_list(j, NB, (stage1, stage2, stage3, stage4, stage5, stage6), LAGS)
        pl.when(j == 1)(pooled_on)
        pl.when(j == 3)(pooled_core)

    def step(par, do_pre, do_mm):
        slot, prev = dzs[par], dzs[1 - par]
        out = dw.at[1 - par]
        if do_pre:
            sc, sh, bb, cc = sc_ref[:], sh_ref[:], bb_ref[:], cc_ref[:]

        def pre(base, n):
            da = da_ref[n:n + NT, :]
            for p in range(CH):
                r = pl.ds(base + p * IMG + n, NT)
                zz = z_ref[r, :]
                u = zz * sc + sh + s_ref[r, :].astype(F32)
                slot[r, :] = (jnp.where(u > 0, da, 0.0) + (zz * cc + bb)).astype(BF16)

        def body(base, slabs, add):
            work = [functools.partial(pre, base + p * IMG, n) for p in range(0, slabs, CH) for n in range(0, IMG, NT)]
            size = slabs * IMG
            for k in range(BPIECES):
                m = slice(k * CIN // BPIECES, (k + 1) * CIN // BPIECES)
                if do_mm:
                    g = dot(atv[m, pl.ds(base, size)], prev[pl.ds(base, size), :])
                if do_pre:
                    n = len(work)
                    for f in work[k * n // BPIECES:(k + 1) * n // BPIECES]:
                        f()
                if do_mm:
                    out[m] = out[m] + g if add else g

        rest = NBIG * BIG
        new = do_mm and do_pre and par == 1
        if new:
            pl.when(j == 1)(at_rest.wait)
        body(rest, POS - NBIG * BTILE, False)

        def chunk(i, carry):
            base = pl.multiple_of(i * BIG, BIG)
            if do_mm:
                pl.when(i == 1)(stages)
            if new:
                pl.when(j == 1)(lambda: at_copy(i).wait())
            body(base, BTILE, True)
            return carry
        lax.fori_loop(0, NBIG, chunk, 0)
        if do_mm:
            core_copy(j - 1).start()

    @pl.when(j == 0)
    def _():
        step(0, True, False)

    for par in range(2):
        @pl.when(jnp.logical_and(jnp.logical_and(j > 0, j < NB), lax.rem(j, 2) == par))
        def _():
            step(par, True, True)

    def logits_unit(i):
        rows = span(i, LB)
        lg = dot_t(pall[rows, :], wtb[:])
        lab = jnp.concatenate([label_rows(lab_ref[i // 2, lax.rem(i, 2), k]) for k in range(2)])
        lterm, dl = softmax_terms(lg, bpad[:], lab)
        loss_ref[:] += fold(lterm)
        gb_ref[:] += fold(dl)
        dlt[:, pl.ds(pl.multiple_of(i * LB, LB), LB)] = dl.T.astype(BF16)

    def fc_copies(c):
        sl = lax.rem(c, 4)
        return [pltpu.make_async_copy(rd.at[sl * 2 + h], gfc_hbm.at[pl.ds(h * HALF, HALF), cols(c)], fsem.at[h, c]) for h in range(2)]

    def dfc_unit(c):
        pl.when(c >= 4)(lambda: each(wait, fc_copies(c - 4)))
        acc = jnp.zeros((SUB, CB), F32)
        for h in range(2):
            g = dot(dlt[pl.ds(h * HALF, HALF), :], pall[:, cols(c)])
            rd[lax.rem(c, 4) * 2 + h] = g
            acc = acc + fold(g * g)
        fsq_ref[:, cols(c)] = acc
        each(start, fc_copies(c))

    @pl.when(j == NB)
    def _():
        step(0, False, True)
        pall_copy.start()
        wtb_copy.start()

    @pl.when(j > NB)
    def _():
        stages()
        k = j - NB - 1

        @pl.when(k == 0)
        def _():
            for b in range(NP):
                each(wait_recv, gather_core(ptail, ps, pr, b))
            for q, (c, py, px) in enumerate(pieces()):
                atv[span(q, IMG), PG:COUT] = ptail[c, py, px].astype(BF16)
            pall_copy.wait()
            wtb_copy.wait()

        loop(jnp.minimum(k * 3, 4), jnp.minimum(k * 3 + 3, 4), logits_unit)
        loop(jnp.clip(k * 3 - 3, 0, NB), jnp.clip(k * 3, 0, NB), dfc_unit)

    @pl.when(j == NB + BTAIL - 1)
    def _():
        each(wait, db_copies)
        acc = dball[0]
        for k in range(1, DEVS):
            acc = acc + dball[k]
        dbo_ref[:] = acc
        for c in range(4, NB):
            each(wait, fc_copies(c))

        def drain(b):
            each(wait_send, gather_all(gfull, gs, gr, b))
            out_copy(b).wait()
        loop(0, NB, drain)
        loop(0, NP, lambda b: each(wait_send, gather_all(ptail, ps, pr, b)))


def backward(*args):
    cur = lambda j: (0, jnp.minimum(j, NB - 1))
    row = pl.BlockSpec((1, CB), cur)
    pair, quad, side = (2, QR, HC), (2, 2, 2, QR, HC), (NB, QR, HC)
    return pl.pallas_call(
        bwd_kernel,
        grid=(NB + BTAIL,),
        in_specs=[HBM, pl.BlockSpec((None, ROWS, CB), lambda j: (jnp.minimum(j, NB - 1), 0, 0)), pl.BlockSpec((ROWS, CB), cur), row, row, row, row,
                  pl.BlockSpec((IMG, CB), cur), whole(2, COUT), HBM, HBM, HBM, whole(2, 2, 2, 1, IMG), whole(1, CLASSES)],
        out_specs=[HBM, whole(2, COUT), whole(SUB, CB), HBM, whole(SUB, COUT), whole(SUB, KP), whole(SUB, KP)],
        out_shape=[struct(QUAD + (QR, COUT)), struct((2, COUT)), struct((SUB, CB)), struct((KP, COUT)), struct((SUB, COUT)), struct((SUB, KP)), struct((SUB, KP))],
        scratch_shapes=[bvmem(CIN, ROWS), bvmem(ROWS, CB), bvmem(ROWS, CB), fvmem(2, CIN, CB), fvmem(NB, HALF, CB), fvmem(*quad), fvmem(*quad),
                        fvmem(NB, *pair), fvmem(NB, *pair), fvmem(2, *pair), fvmem(2, *pair), fvmem(*side), fvmem(*side),
                        fvmem(*QUAD, QR, COUT), fvmem(DEVS, 2, COUT), fvmem(*QUAD, IMG, PT), fvmem(1, KP),
                        dma(NBIG + 1), dma(5, NP), dma(5, NP), dma(5, NB), dma(5, NB), dma(5, NB), dma(5, NB), dma(DEVS), dma(DEVS), dma(NB), dma(4), dma(2, NB)],
        compiler_params=pltpu.CompilerParams(vmem_limit_bytes=63 * MIB, collective_id=1, has_side_effects=True),
        cost_estimate=pl.CostEstimate(flops=2 * ROWS * CIN * COUT, bytes_accessed=2 * ROWS * COUT * 4, transcendentals=0),
        name="bwd_conv",
    )(*args)


def trust_of(wsq, gsq):
    wn = jnp.sqrt(lanesum(rowsum(wsq)))
    gn = jnp.sqrt(lanesum(rowsum(gsq)))
    return TRUST_COEF * wn / (gn + WEIGHT_DECAY * wn)


def update_kernel(lr_ref, w_ref, v_ref, g_ref, wsq_ref, gsq_ref, wt_ref, vt_ref, gt_ref, tsq_ref, fsq_ref, bias_ref, vbias_ref, gb_ref, ls_ref,
                  gam_ref, bet_ref, vgam_ref, vbet_ref, dgb_ref,
                  wo_ref, vo_ref, wto_ref, vto_ref, bo_ref, vbo_ref, go_ref, vgo_ref, beo_ref, vbeo_ref, loss_ref):
    j = pl.program_id(0)
    lr = lr_ref[0]

    def plain(p, v, g, po, vo):
        nv = MOMENTUM * v[:] + lr * g
        vo[:] = nv
        po[:] = p[:] - nv

    @pl.when(j == 0)
    def _():
        plain(gam_ref, vgam_ref, dgb_ref[:1], go_ref, vgo_ref)
        plain(bet_ref, vbet_ref, dgb_ref[1:], beo_ref, vbeo_ref)
        plain(bias_ref, vbias_ref, rowsum(gb_ref[:])[:, :CLASSES], bo_ref, vbo_ref)
        loss_ref[:] = lanesum(rowsum(ls_ref[:])) * (-1.0 / TOTAL)

    def lars(w_ref, v_ref, g_ref, wsq, gsq, wo, vo, rows):
        rate = jnp.broadcast_to(lr * trust_of(wsq[:], gsq[:]), (SUB, CB))

        def row(i, carry):
            for q in range(2):
                r = pl.ds(pl.multiple_of(i * 2 * SUB + q * SUB, SUB), SUB)
                for c in range(0, COUT, CB):
                    cc = slice(c, c + CB)
                    w = w_ref[r, cc]
                    nv = MOMENTUM * v_ref[r, cc] + rate * (g_ref[r, cc] + WEIGHT_DECAY * w)
                    vo[r, cc] = nv
                    wo[r, cc] = w - nv
            return carry
        lax.fori_loop(0, rows // (2 * SUB), row, 0)

    lars(w_ref, v_ref, g_ref, wsq_ref, gsq_ref, wo_ref, vo_ref, UB)
    lars(wt_ref, vt_ref, gt_ref, tsq_ref, fsq_ref, wto_ref, vto_ref, UB)


def update_all(*args):
    conv = fc = pl.BlockSpec((UB, COUT), lambda j: (j, 0))
    vec, bvec, one = (1, COUT), (1, CLASSES), (1, 1)
    vs, bs = whole(*vec), whole(*bvec)
    big, fcs = struct((CIN, COUT)), struct((CLASSES, COUT))
    return pl.pallas_call(
        update_kernel,
        grid=(NU,),
        in_specs=[pl.BlockSpec(memory_space=pltpu.SMEM), conv, conv, conv, whole(SUB, CB), whole(SUB, CB), fc, fc, fc, whole(SUB, COUT), whole(SUB, COUT),
                  bs, bs, whole(SUB, KP), whole(SUB, KP), vs, vs, vs, vs, whole(2, COUT)],
        out_specs=[conv, conv, fc, fc, bs, bs, vs, vs, vs, vs, whole(*one)],
        out_shape=[big, big, fcs, fcs] + [struct(bvec)] * 2 + [struct(vec)] * 4 + [struct(one)],
        compiler_params=pltpu.CompilerParams(vmem_limit_bytes=63 * MIB),
        cost_estimate=pl.CostEstimate(flops=CIN * COUT * 16, bytes_accessed=10 * CIN * COUT * 4, transcendentals=0),
        name="update",
    )(*args)


def solution(mesh):
    def local_step(act_in, shortcut, labels, w_conv, gamma, beta, w_fc, fc_bias, vel_conv, vel_gamma, vel_beta, vel_fc, vel_bias, lr):
        a = act_in.transpose(1, 2, 0, 3).reshape(ROWS, CIN)
        s = shortcut.transpose(1, 2, 0, 3).reshape(ROWS, COUT)
        wt = w_fc.T
        bias = fc_bias[None]
        z, at, pall, ptail, lab, wsq, tsq, wtb, da, sc, sh, bb, cc, dgb = forward(a, w_conv, s, gamma[None], beta[None], labels[None], bias, wt)
        g8, dgb, gsq, gfc, fsq, gb, ls = backward(at, z, s, sc, sh, bb, cc, da, dgb, pall, ptail, wtb, lab, bias)
        wo, vo, wto, vto, bo, vbo, go, vgo, beo, vbeo, loss = update_all(
            lr.reshape(1), w_conv, vel_conv, g8.reshape(CIN, COUT), wsq, gsq, wt, vel_fc.T, gfc, tsq, fsq, bias, vel_bias[None], gb, ls,
            gamma[None], beta[None], vel_gamma[None], vel_beta[None], dgb)
        return (wo, go[0], beo[0], wto.T, bo[0], vo, vgo[0], vbeo[0], vto.T, vbo[0], loss[0, 0])

    return jax.shard_map(local_step, mesh=mesh, in_specs=(P('dp'),) * 3 + (P(),) * 11, out_specs=(P(),) * 11, check_vma=False)
```

```python
import functools
import jax
import jax.numpy as jnp
from jax import lax
from jax.experimental import pallas as pl
from jax.experimental.pallas import tpu as pltpu
from jax.sharding import PartitionSpec as P

BN_EPS = 1e-5
SMOOTHING = 0.1
MOMENTUM = 0.9
TRUST_COEF = 0.001
WEIGHT_DECAY = 5e-5

LANES = 128
SUB = 8
IMG = 128
POS = 49
ROWS = IMG * POS
CIN = 1024
COUT = 2048
CLASSES = 1000
KP = 1024
DEVS = 8
TOTAL = DEVS * IMG
CB = 256
HC = CB // 2
NB = COUT // CB
CH = 7
NCH = POS // CH
NT = 16
PIECES = 8
BPIECES = 4
APAD = CIN + LANES
TAIL = 1
NG = 6
NP = NB - NG
PG, PT = NG * CB, NP * CB
LAGS = (2, 3, 4, 5, 7, 8)
BTAIL = LAGS[-1]
QR = CIN // DEVS
HALF = CIN // 2
BIG = 1792
BTILE = BIG // IMG
NBIG = ROWS // BIG
UB = 256
NU = CIN // UB
LB = 256
MIB = 1024 * 1024
F32 = jnp.float32
BF16 = jnp.bfloat16
MESH = pl.DeviceIdType.MESH
XN, YN, PN = 'x', 'y', 'core'


def dot(a, b):
    return jnp.dot(a, b, preferred_element_type=F32)


def dot_t(a, b):
    return lax.dot_general(a, b, (((1,), (1,)), ((), ())), preferred_element_type=F32)


def fold(v, axis=0):
    return jnp.sum(v.reshape(v.shape[0] // SUB, SUB, v.shape[1]), axis=axis)


def rowsum(v, axis=0):
    return jnp.sum(v, axis=axis, keepdims=True)


def lanesum(v, axis=1):
    return jnp.sum(v, axis=axis, keepdims=True)


def cols(b, size=CB, at=0):
    return pl.ds(pl.multiple_of(b * CB + at, LANES), size)


def span(i, size):
    return pl.ds(pl.multiple_of(i * size, SUB), size)


def position():
    me = lax.axis_index('dp')
    return me, lax.rem(me, 2), lax.rem(me // 2, 2), me // 4


def dev(core, x, y):
    return (y * 2 + x) * 2 + core


def neighbour(name):
    me, core, x, y = position()
    flip = lambda v, k: 1 - v if k == name else v
    return dev(flip(core, PN), flip(x, XN), flip(y, YN))


def enter_all():
    me = lax.axis_index('dp')
    bar = pltpu.get_barrier_semaphore()
    for k in range(1, DEVS):
        pl.semaphore_signal(bar, inc=1, device_id=(lax.rem(me + k, DEVS),), device_id_type=MESH)
    pl.semaphore_wait(bar, DEVS - 1)


def rcopy(src, dst, send, recv, target):
    return pltpu.make_async_remote_copy(src_ref=src, dst_ref=dst, send_sem=send, recv_sem=recv, device_id=(target,), device_id_type=MESH)


def each(fn, copies):
    for c in copies:
        fn(c)


def start(c):
    c.start()


def wait(c):
    c.wait()


def wait_send(c):
    c.wait_send()


def wait_recv(c):
    c.wait_recv()


def gather_own(buf, send, recv, b, ka=0, kb=1):
    me, core, x, y = position()
    a, c = buf.at[core, y, x, :, cols(b, HC)], buf.at[core, y, x, :, cols(b, HC, HC)]
    return rcopy(a, a, send.at[ka, b], recv.at[ka, b], neighbour(YN)), rcopy(c, c, send.at[kb, b], recv.at[kb, b], neighbour(XN))


def gather_on(buf, send, recv, b, ka=2, kb=3):
    me, core, x, y = position()
    a, c = buf.at[core, :, x, :, cols(b, HC)], buf.at[core, y, :, :, cols(b, HC, HC)]
    return rcopy(a, a, send.at[ka, b], recv.at[ka, b], neighbour(XN)), rcopy(c, c, send.at[kb, b], recv.at[kb, b], neighbour(YN))


def gather_core(buf, send, recv, b, k=4):
    me, core, x, y = position()
    a = buf.at[core, :, :, :, cols(b)]
    return (rcopy(a, a, send.at[k, b], recv.at[k, b], neighbour(PN)),)


def gather_all(*a):
    return gather_own(*a) + gather_on(*a) + gather_core(*a)


def stage_list(j, blocks, fns, lags):
    for fn, lag in zip(fns, lags):
        b = j - lag
        pl.when(jnp.logical_and(b >= 0, b < blocks))(functools.partial(fn, b))


def loop(lo, hi, fn):
    def body(i, carry):
        fn(i)
        return carry
    lax.fori_loop(lo, hi, body, 0)


def pieces():
    return [(c, y, x) for c in range(2) for y in range(2) for x in range(2)]


def softmax_terms(logits, bias, labels):
    n = logits.shape[0]
    cls = lax.broadcasted_iota(jnp.int32, (n, KP), 1)
    valid = cls < CLASSES
    lg = jnp.where(valid, logits + bias, -1e30)
    sh = lg - jnp.max(lg, axis=1, keepdims=True)
    lp = sh - jnp.log(lanesum(jnp.exp(sh)))
    lab = jnp.concatenate([labels] * (KP // LANES), axis=1)
    hit = lab == cls.astype(F32)
    tg = jnp.where(valid, SMOOTHING / CLASSES + jnp.where(hit, 1.0 - SMOOTHING, 0.0), 0.0)
    return tg * lp, (jnp.exp(lp) - tg) * (1.0 / TOTAL)


def label_rows(row):
    return jnp.broadcast_to(row.astype(F32), (IMG, IMG)).T


def set_bias(bpad, bias_ref):
    bpad[:] = jnp.zeros_like(bpad)
    bpad[:, :CLASSES] = bias_ref[:]


def fwd_kernel(a_hbm, w_ref, s_ref, g_ref, b_ref, lab_ref, bias_ref, wt_ref,
               z_hbm, at_ref, pall_ref, ptail_ref, lall_ref, wsq_ref, fsq_ref, wtb_hbm, da_ref, sc_ref, sh_ref, bb_ref, cc_ref, db_ref,
               abf, z0, z1, wbf, stat, pfull, lfull, pool, cnt, sx, sv, wtb, bpad, asem, zsem, osem, gs, gr, ls, lr):
    j = pl.program_id(0)
    zs = (z0, z1)
    me, core, x, y = position()
    crow = CH * IMG

    def a_copy(i):
        r = span(i, crow)
        return pltpu.make_async_copy(a_hbm.at[r, :], abf.at[r, :CIN], asem.at[i])

    def z_copy(jj, par):
        return pltpu.make_async_copy(zs[par], z_hbm.at[jj], zsem.at[par])

    def wtb_copy():
        return pltpu.make_async_copy(wtb, wtb_hbm, osem)

    def label_copy(k):
        return rcopy(lab_ref, lfull.at[core, y, x], ls.at[k], lr.at[k], lax.rem(me + k, DEVS))

    labels = [label_copy(k) for k in range(1, DEVS)]

    @pl.when(j == 0)
    def _():
        for i in range(NCH):
            a_copy(i).start()
        enter_all()
        each(start, labels)
        lfull[core, y, x] = lab_ref[:]
        wsq_ref[:] = jnp.zeros_like(wsq_ref)
        wtb[CLASSES:] = jnp.zeros((KP - CLASSES, COUT), BF16)
        set_bias(bpad, bias_ref)

    def second(b):
        each(wait_recv, gather_own(pfull, gs, gr, b))
        each(start, gather_on(pfull, gs, gr, b))

    def third(b):
        each(wait_recv, gather_on(pfull, gs, gr, b))
        each(start, gather_core(pfull, gs, gr, b))

    def last(b):
        each(wait_recv, gather_core(pfull, gs, gr, b))
        for q, (c, py, px) in enumerate(pieces()):
            pall_ref[span(q, IMG), :] = pfull[c, py, px, :, cols(b)].astype(BF16)

    def stages():
        stage_list(j, NG, (second, third, last), (2, 3, 4))

    def step(par, do_mm, do_post):
        first = not do_post
        slot, prev = zs[par], zs[1 - par]
        if do_post:
            pl.when(j >= 2)(lambda: z_copy(j - 2, par).wait())
        if do_mm:
            wf = w_ref[:]
            wsq_ref[:] += fold(wf * wf)
            wtf = wt_ref[:]
            fsq_ref[:, cols(j)] = fold(wtf * wtf)
            wtb[:CLASSES, cols(j)] = wtf.astype(BF16)
            w = wf.astype(BF16)
            wbf[:] = w
            if first:
                a_copy(0).wait()
            m0 = rowsum(dot(abf[:IMG, :CIN], w)) * (1.0 / IMG)
            stat[:2 * SUB] = jnp.zeros((2 * SUB, CB), F32)
        if do_post and not do_mm:
            wtb_copy().start()
        if do_post:
            mean = stat[2 * SUB:2 * SUB + 1]
            inv = stat[3 * SUB:3 * SUB + 1]
            sc = g_ref[:] * inv
            sh = b_ref[:] - mean * sc
            pool[:] = jnp.zeros_like(pool)
            pc = cols(j - 1)
            cnt[:, pc] = jnp.zeros((IMG, CB), F32)
            sx[:, pc] = jnp.zeros((IMG, CB), F32)

        def post(base, n, slabs):
            nr = slice(n, n + NT)
            pa, ca, xa = pool[nr], cnt[nr, pc], sx[nr, pc]
            for p in range(slabs):
                r = pl.ds(base + p * IMG + n, NT)
                zz = prev[r, :]
                u = zz * sc + sh + s_ref[r, :].astype(F32)
                mk = u > 0
                pa = pa + jnp.maximum(u, 0.0)
                ca = ca + jnp.where(mk, 1.0, 0.0)
                xa = xa + jnp.where(mk, zz, 0.0)
            pool[nr], cnt[nr, pc], sx[nr, pc] = pa, ca, xa

        def flip(base, rows):
            r = pl.ds(base, rows)
            at_ref[:, r] = abf[r, pl.ds(pl.multiple_of(j * IMG, IMG), IMG)].astype(F32).T.astype(BF16)

        def region(base, slabs, parts):
            size = slabs * IMG // parts
            for k in range(parts):
                if do_mm:
                    r = pl.ds(base + k * size, size)
                    zc = dot(abf[r, :CIN], wbf[:])
                if do_post:
                    for n in range(k * IMG // parts, (k + 1) * IMG // parts, NT):
                        post(base, n, slabs)
                if do_mm:
                    slot[r, :] = zc
                    d = zc - m0
                    stat[:SUB] += fold(d)
                    stat[SUB:2 * SUB] += fold(d * d)

            if do_mm:
                flip(base, slabs * IMG)

        def chunk(i, carry):
            if first:
                pl.when(i > 0)(lambda: a_copy(i).wait())
            region(pl.multiple_of(i * crow, crow), CH, 4)
            return carry

        def chunk2(i, carry):
            pl.when(i == 2)(stages)
            region(pl.multiple_of(i * 2 * crow, 2 * crow), 2 * CH, PIECES)
            return carry

        if first:
            lax.fori_loop(0, NCH, chunk, 0)
        else:
            lax.fori_loop(0, NCH // 2, chunk2, 0)
            region(pl.multiple_of((jnp.minimum(me, 0) + NCH - 1) * crow, crow), CH, 4)
        if do_post:
            pfull[core, y, x, :, pc] = pool[:] * (1.0 / POS)
            sx[:, pc] = (sx[:, pc] - mean * cnt[:, pc]) * inv
            sv[:1, pc] = mean
            sv[SUB:SUB + 1, pc] = inv
            sc_ref[:, pc] = sc
            sh_ref[:, pc] = sh
            pl.when(j - 1 < NG)(lambda: each(start, gather_own(pfull, gs, gr, j - 1)))
        if do_mm:
            dm = rowsum(stat[:SUB]) * (1.0 / ROWS)
            q = rowsum(stat[SUB:2 * SUB]) * (1.0 / ROWS)
            stat[2 * SUB:2 * SUB + 1] = m0 + dm
            stat[3 * SUB:3 * SUB + 1] = lax.rsqrt(jnp.maximum(q - dm * dm, 0.0) + BN_EPS)
            z_copy(j, par).start()

    @pl.when(j == 0)
    def _():
        step(0, True, False)

    for par in range(2):
        @pl.when(jnp.logical_and(jnp.logical_and(j > 0, j < NB), lax.rem(j, 2) == par))
        def _():
            step(par, True, True)

    @pl.when(j == NB)
    def _():
        step(0, False, True)

    @pl.when(j == NB + 1)
    def _():
        stages()
        ptail_ref[:] = pfull[core, y, x, :, PG:]
        lg = dot_t(pfull[core, y, x].astype(BF16), wtb[:])
        _, dl = softmax_terms(lg, bpad[:], label_rows(lab_ref[:]))
        dlb = dl.astype(BF16)

        def col(b, carry):
            c = cols(b)
            dp = dot(dlb, wtb[:, c]) * (1.0 / POS)
            dbeta = rowsum(dp * cnt[:, c])
            dgamma = rowsum(dp * sx[:, c])
            sc = sc_ref[:, c]
            cc = -(sc * sv[SUB:SUB + 1, c]) * (dgamma * (1.0 / ROWS))
            cc_ref[:, c] = cc
            bb_ref[:, c] = -sc * (dbeta * (1.0 / ROWS)) - sv[:1, c] * cc
            da_ref[:, c] = dp * sc
            db_ref[:1, c] = dgamma
            db_ref[1:, c] = dbeta
            return carry
        lax.fori_loop(0, NB, col, 0)

        each(wait, labels)
        lall_ref[:] = lfull[:]
        wtb_copy().wait()
        z_copy(NB - 1, 1).wait()
        loop(0, NG, lambda b: each(wait_send, gather_all(pfull, gs, gr, b)))


def whole(*shape):
    return pl.BlockSpec(shape, lambda j: (0,) * len(shape))


def struct(shape, dtype=F32):
    return jax.ShapeDtypeStruct(shape, dtype)


def fvmem(*shape):
    return pltpu.VMEM(shape, F32)


def bvmem(*shape):
    return pltpu.VMEM(shape, BF16)


def dma(*shape):
    return pltpu.SemaphoreType.DMA(shape)


HBM = pl.BlockSpec(memory_space=pl.ANY)
QUAD = (2, 2, 2)


def forward(a, w, s, gamma, beta, labels, bias, wt):
    prev = lambda j: (0, jnp.clip(j - 1, 0, NB - 1))
    cur = lambda j: (0, jnp.minimum(j, NB - 1))
    late = lambda j: (0, jnp.clip(j - 4, 0, NG - 1))
    vec, lab = (1, COUT), QUAD + (1, IMG)
    return pl.pallas_call(
        fwd_kernel,
        grid=(NB + 1 + TAIL,),
        in_specs=[HBM, pl.BlockSpec((CIN, CB), cur), pl.BlockSpec((ROWS, CB), prev), pl.BlockSpec((1, CB), prev), pl.BlockSpec((1, CB), prev),
                  whole(1, IMG), whole(1, CLASSES), pl.BlockSpec((CLASSES, CB), cur)],
        out_specs=[HBM, pl.BlockSpec((IMG, ROWS), lambda j: (jnp.minimum(j, NB - 1), 0)), pl.BlockSpec((TOTAL, CB), late), whole(IMG, PT), whole(*lab),
                   whole(SUB, CB), whole(SUB, COUT), HBM, whole(IMG, COUT)] + [whole(*vec)] * 4 + [whole(2, COUT)],
        out_shape=[struct((NB, ROWS, CB)), struct((CIN, ROWS), BF16), struct((TOTAL, PG), BF16), struct((IMG, PT)), struct(lab, jnp.int32),
                   struct((SUB, CB)), struct((SUB, COUT)), struct((KP, COUT), BF16), struct((IMG, COUT))] + [struct(vec)] * 4 + [struct((2, COUT))],
        scratch_shapes=[bvmem(ROWS, APAD), fvmem(ROWS, CB), fvmem(ROWS, CB), bvmem(CIN, CB), fvmem(4 * SUB, CB), fvmem(*QUAD, IMG, COUT), pltpu.VMEM(lab, jnp.int32),
                        fvmem(IMG, CB), fvmem(IMG, COUT), fvmem(IMG, COUT), fvmem(2 * SUB, COUT), bvmem(KP, COUT), fvmem(1, KP),
                        dma(NCH), dma(2), pltpu.SemaphoreType.DMA, dma(5, NG), dma(5, NG), dma(DEVS), dma(DEVS)],
        compiler_params=pltpu.CompilerParams(vmem_limit_bytes=63 * MIB, collective_id=0, has_side_effects=True),
        cost_estimate=pl.CostEstimate(flops=2 * ROWS * CIN * COUT, bytes_accessed=2 * ROWS * COUT * 4, transcendentals=0),
        name="fwd_conv",
    )(a, w, s, gamma, beta, labels, bias, wt)


def bwd_kernel(at_hbm, z_ref, s_ref, sc_ref, sh_ref, bb_ref, cc_ref, da_ref, db_ref, pall_hbm, ptail_hbm, wtb_hbm, lab_ref, bias_ref,
               g_hbm, dbo_ref, gsq_ref, gfc_hbm, fsq_ref, gb_ref, loss_ref,
               atv, dz0, dz1, dw, rd, ha, hb, ra, rb, ka, kb, r2a, r2b, gfull, dball, ptail, bpad, ps, pr, ss, rs, gs, gr, bs, br, osem, isem, fsem):
    j = pl.program_id(0)
    dzs = (dz0, dz1)
    me, core, x, y = position()
    plan = pl.ds(0, COUT)
    pall = atv.at[:, plan]
    wtb = atv.at[:, pl.ds(COUT, COUT)]
    dlt = atv.at[:, pl.ds(2 * COUT, TOTAL)]

    at_copy = pltpu.make_async_copy(at_hbm, atv, isem.at[0])
    pall_copy = pltpu.make_async_copy(pall_hbm, atv.at[:, pl.ds(0, PG)], isem.at[1])
    wtb_copy = pltpu.make_async_copy(wtb_hbm, wtb, isem.at[2])
    ptail_copy = pltpu.make_async_copy(ptail_hbm, ptail.at[core, y, x], isem.at[3])
    db_copies = [rcopy(db_ref, dball.at[me], bs.at[k], br.at[k], lax.rem(me + k, DEVS)) for k in range(1, DEVS)]

    @pl.when(j == 0)
    def _():
        ptail_copy.start()
        at_copy.start()
        enter_all()
        ptail_copy.wait()
        for b in range(NP):
            each(start, gather_own(ptail, ps, pr, b))
        each(start, db_copies)
        dball[me] = db_ref[:]
        for r in (gsq_ref, fsq_ref, gb_ref, loss_ref):
            r[:] = jnp.zeros_like(r)
        set_bias(bpad, bias_ref)

    @pl.when(j == 1)
    def _():
        at_copy.wait()

    def out_copy(b):
        c = cols(b)
        return pltpu.make_async_copy(gfull.at[:, :, :, :, c], g_hbm.at[:, :, :, :, c], osem.at[b])

    def core_copy(b, k=0):
        return rcopy(dw.at[lax.rem(b, 2), span(1 - core, HALF), :], rd.at[b], ss.at[k, b], rs.at[k, b], neighbour(PN))

    def first_copies(b, k=1, m=2):
        sl = lax.rem(b, 2)
        return (rcopy(ha.at[sl, 1 - x], ra.at[b], ss.at[k, b], rs.at[k, b], neighbour(XN)),
                rcopy(hb.at[sl, 1 - y], rb.at[b], ss.at[m, b], rs.at[m, b], neighbour(YN)))

    def second_copies(b, k=3, m=4):
        sl = lax.rem(b, 2)
        return (rcopy(ka.at[sl, 1 - y], r2a.at[b], ss.at[k, b], rs.at[k, b], neighbour(YN)),
                rcopy(kb.at[sl, 1 - x], r2b.at[b], ss.at[m, b], rs.at[m, b], neighbour(XN)))

    def stage1(b):
        core_copy(b).wait()
        sl = lax.rem(b, 2)
        for q, (py, px) in enumerate((py, px) for py in range(2) for px in range(2)):
            own = pl.ds(pl.multiple_of(core * HALF + q * QR, QR), QR)
            got = slice(q * QR, (q + 1) * QR)
            ha[sl, px, py] = dw[sl, own, :HC] + rd[b, got, :HC]
            hb[sl, py, px] = dw[sl, own, HC:] + rd[b, got, HC:]
        each(start, first_copies(b))

    def stage2(b):
        sl = lax.rem(b, 2)
        each(wait, first_copies(b))
        for k in range(2):
            ka[sl, k] = ha[sl, x, k] + ra[b, k]
            kb[sl, k] = hb[sl, y, k] + rb[b, k]
        each(start, second_copies(b))

    def stage3(b):
        sl = lax.rem(b, 2)
        each(wait, second_copies(b))
        gfull[core, y, x, :, cols(b, HC)] = ka[sl, y] + r2a[b]
        gfull[core, y, x, :, cols(b, HC, HC)] = kb[sl, x] + r2b[b]
        each(start, gather_own(gfull, gs, gr, b))

    def stage4(b):
        each(wait_recv, gather_own(gfull, gs, gr, b))
        each(start, gather_on(gfull, gs, gr, b))

    def stage5(b):
        each(wait_recv, gather_on(gfull, gs, gr, b))
        each(start, gather_core(gfull, gs, gr, b))

    def stage6(b):
        each(wait_recv, gather_core(gfull, gs, gr, b))
        out_copy(b).start()
        acc = gsq_ref[:]
        for q in pieces():
            gv = gfull[q + (slice(None), cols(b))]
            acc = acc + fold(gv * gv)
        gsq_ref[:] = acc

    def pooled_on():
        for b in range(NP):
            each(wait_recv, gather_own(ptail, ps, pr, b))
            each(start, gather_on(ptail, ps, pr, b))

    def pooled_core():
        for b in range(NP):
            each(wait_recv, gather_on(ptail, ps, pr, b))
            each(start, gather_core(ptail, ps, pr, b))

    def stages():
        stage_list(j, NB, (stage1, stage2, stage3, stage4, stage5, stage6), LAGS)
        pl.when(j == 1)(pooled_on)
        pl.when(j == 3)(pooled_core)

    def step(par, do_pre, do_mm):
        slot, prev = dzs[par], dzs[1 - par]
        out = dw.at[1 - par]
        if do_pre:
            sc, sh, bb, cc = sc_ref[:], sh_ref[:], bb_ref[:], cc_ref[:]

        def pre(base, n):
            da = da_ref[n:n + NT, :]
            for p in range(CH):
                r = pl.ds(base + p * IMG + n, NT)
                zz = z_ref[r, :]
                u = zz * sc + sh + s_ref[r, :].astype(F32)
                slot[r, :] = (jnp.where(u > 0, da, 0.0) + (zz * cc + bb)).astype(BF16)

        def body(base, slabs, add):
            work = [functools.partial(pre, base + p * IMG, n) for p in range(0, slabs, CH) for n in range(0, IMG, NT)]
            size = slabs * IMG
            for k in range(BPIECES):
                m = slice(k * CIN // BPIECES, (k + 1) * CIN // BPIECES)
                if do_mm:
                    g = dot(atv[m, pl.ds(base, size)], prev[pl.ds(base, size), :])
                if do_pre:
                    n = len(work)
                    for f in work[k * n // BPIECES:(k + 1) * n // BPIECES]:
                        f()
                if do_mm:
                    out[m] = out[m] + g if add else g

        rest = NBIG * BIG
        body(rest, POS - NBIG * BTILE, False)

        def chunk(i, carry):
            base = pl.multiple_of(i * BIG, BIG)
            if do_mm:
                pl.when(i == 1)(stages)
            body(base, BTILE, True)
            return carry
        lax.fori_loop(0, NBIG, chunk, 0)
        if do_mm:
            core_copy(j - 1).start()

    @pl.when(j == 0)
    def _():
        step(0, True, False)

    for par in range(2):
        @pl.when(jnp.logical_and(jnp.logical_and(j > 0, j < NB), lax.rem(j, 2) == par))
        def _():
            step(par, True, True)

    def logits_unit(i):
        rows = span(i, LB)
        lg = dot_t(pall[rows, :], wtb[:])
        lab = jnp.concatenate([label_rows(lab_ref[i // 2, lax.rem(i, 2), k]) for k in range(2)])
        lterm, dl = softmax_terms(lg, bpad[:], lab)
        loss_ref[:] += fold(lterm)
        gb_ref[:] += fold(dl)
        dlt[:, pl.ds(pl.multiple_of(i * LB, LB), LB)] = dl.T.astype(BF16)

    def fc_copies(c):
        sl = lax.rem(c, 4)
        return [pltpu.make_async_copy(rd.at[sl * 2 + h], gfc_hbm.at[pl.ds(h * HALF, HALF), cols(c)], fsem.at[h, c]) for h in range(2)]

    def dfc_unit(c):
        pl.when(c >= 4)(lambda: each(wait, fc_copies(c - 4)))
        acc = jnp.zeros((SUB, CB), F32)
        for h in range(2):
            g = dot(dlt[pl.ds(h * HALF, HALF), :], pall[:, cols(c)])
            rd[lax.rem(c, 4) * 2 + h] = g
            acc = acc + fold(g * g)
        fsq_ref[:, cols(c)] = acc
        each(start, fc_copies(c))

    @pl.when(j == NB)
    def _():
        step(0, False, True)
        pall_copy.start()
        wtb_copy.start()

    @pl.when(j > NB)
    def _():
        stages()
        k = j - NB - 1

        @pl.when(k == 0)
        def _():
            for b in range(NP):
                each(wait_recv, gather_core(ptail, ps, pr, b))
            for q, (c, py, px) in enumerate(pieces()):
                atv[span(q, IMG), PG:COUT] = ptail[c, py, px].astype(BF16)
            pall_copy.wait()
            wtb_copy.wait()

        loop(jnp.minimum(k * 3, 4), jnp.minimum(k * 3 + 3, 4), logits_unit)
        loop(jnp.clip(k * 3 - 3, 0, NB), jnp.clip(k * 3, 0, NB), dfc_unit)

    @pl.when(j == NB + BTAIL - 1)
    def _():
        each(wait, db_copies)
        acc = dball[0]
        for k in range(1, DEVS):
            acc = acc + dball[k]
        dbo_ref[:] = acc
        for c in range(4, NB):
            each(wait, fc_copies(c))

        def drain(b):
            each(wait_send, gather_all(gfull, gs, gr, b))
            out_copy(b).wait()
        loop(0, NB, drain)
        loop(0, NP, lambda b: each(wait_send, gather_all(ptail, ps, pr, b)))


def backward(*args):
    cur = lambda j: (0, jnp.minimum(j, NB - 1))
    row = pl.BlockSpec((1, CB), cur)
    pair, quad, side = (2, QR, HC), (2, 2, 2, QR, HC), (NB, QR, HC)
    return pl.pallas_call(
        bwd_kernel,
        grid=(NB + BTAIL,),
        in_specs=[HBM, pl.BlockSpec((None, ROWS, CB), lambda j: (jnp.minimum(j, NB - 1), 0, 0)), pl.BlockSpec((ROWS, CB), cur), row, row, row, row,
                  pl.BlockSpec((IMG, CB), cur), whole(2, COUT), HBM, HBM, HBM, whole(2, 2, 2, 1, IMG), whole(1, CLASSES)],
        out_specs=[HBM, whole(2, COUT), whole(SUB, CB), HBM, whole(SUB, COUT), whole(SUB, KP), whole(SUB, KP)],
        out_shape=[struct(QUAD + (QR, COUT)), struct((2, COUT)), struct((SUB, CB)), struct((KP, COUT)), struct((SUB, COUT)), struct((SUB, KP)), struct((SUB, KP))],
        scratch_shapes=[bvmem(CIN, ROWS), bvmem(ROWS, CB), bvmem(ROWS, CB), fvmem(2, CIN, CB), fvmem(NB, HALF, CB), fvmem(*quad), fvmem(*quad),
                        fvmem(NB, *pair), fvmem(NB, *pair), fvmem(2, *pair), fvmem(2, *pair), fvmem(*side), fvmem(*side),
                        fvmem(*QUAD, QR, COUT), fvmem(DEVS, 2, COUT), fvmem(*QUAD, IMG, PT), fvmem(1, KP),
                        dma(5, NP), dma(5, NP), dma(5, NB), dma(5, NB), dma(5, NB), dma(5, NB), dma(DEVS), dma(DEVS), dma(NB), dma(4), dma(2, NB)],
        compiler_params=pltpu.CompilerParams(vmem_limit_bytes=63 * MIB, collective_id=1, has_side_effects=True),
        cost_estimate=pl.CostEstimate(flops=2 * ROWS * CIN * COUT, bytes_accessed=2 * ROWS * COUT * 4, transcendentals=0),
        name="bwd_conv",
    )(*args)


def trust_of(wsq, gsq):
    wn = jnp.sqrt(lanesum(rowsum(wsq)))
    gn = jnp.sqrt(lanesum(rowsum(gsq)))
    return TRUST_COEF * wn / (gn + WEIGHT_DECAY * wn)


def update_kernel(lr_ref, w_ref, v_ref, g_ref, wsq_ref, gsq_ref, wt_ref, vt_ref, gt_ref, tsq_ref, fsq_ref, bias_ref, vbias_ref, gb_ref, ls_ref,
                  gam_ref, bet_ref, vgam_ref, vbet_ref, dgb_ref,
                  wo_ref, vo_ref, wto_ref, vto_ref, bo_ref, vbo_ref, go_ref, vgo_ref, beo_ref, vbeo_ref, loss_ref):
    j = pl.program_id(0)
    lr = lr_ref[0]

    def plain(p, v, g, po, vo):
        nv = MOMENTUM * v[:] + lr * g
        vo[:] = nv
        po[:] = p[:] - nv

    @pl.when(j == 0)
    def _():
        plain(gam_ref, vgam_ref, dgb_ref[:1], go_ref, vgo_ref)
        plain(bet_ref, vbet_ref, dgb_ref[1:], beo_ref, vbeo_ref)
        plain(bias_ref, vbias_ref, rowsum(gb_ref[:])[:, :CLASSES], bo_ref, vbo_ref)
        loss_ref[:] = lanesum(rowsum(ls_ref[:])) * (-1.0 / TOTAL)

    def lars(w_ref, v_ref, g_ref, wsq, gsq, wo, vo, rows):
        rate = jnp.broadcast_to(lr * trust_of(wsq[:], gsq[:]), (SUB, CB))

        def row(i, carry):
            for q in range(2):
                r = pl.ds(pl.multiple_of(i * 2 * SUB + q * SUB, SUB), SUB)
                for c in range(0, COUT, CB):
                    cc = slice(c, c + CB)
                    w = w_ref[r, cc]
                    nv = MOMENTUM * v_ref[r, cc] + rate * (g_ref[r, cc] + WEIGHT_DECAY * w)
                    vo[r, cc] = nv
                    wo[r, cc] = w - nv
            return carry
        lax.fori_loop(0, rows // (2 * SUB), row, 0)

    lars(w_ref, v_ref, g_ref, wsq_ref, gsq_ref, wo_ref, vo_ref, UB)
    lars(wt_ref, vt_ref, gt_ref, tsq_ref, fsq_ref, wto_ref, vto_ref, UB)


def update_all(*args):
    conv = fc = pl.BlockSpec((UB, COUT), lambda j: (j, 0))
    vec, bvec, one = (1, COUT), (1, CLASSES), (1, 1)
    vs, bs = whole(*vec), whole(*bvec)
    big, fcs = struct((CIN, COUT)), struct((CLASSES, COUT))
    return pl.pallas_call(
        update_kernel,
        grid=(NU,),
        in_specs=[pl.BlockSpec(memory_space=pltpu.SMEM), conv, conv, conv, whole(SUB, CB), whole(SUB, CB), fc, fc, fc, whole(SUB, COUT), whole(SUB, COUT),
                  bs, bs, whole(SUB, KP), whole(SUB, KP), vs, vs, vs, vs, whole(2, COUT)],
        out_specs=[conv, conv, fc, fc, bs, bs, vs, vs, vs, vs, whole(*one)],
        out_shape=[big, big, fcs, fcs] + [struct(bvec)] * 2 + [struct(vec)] * 4 + [struct(one)],
        compiler_params=pltpu.CompilerParams(vmem_limit_bytes=63 * MIB),
        cost_estimate=pl.CostEstimate(flops=CIN * COUT * 16, bytes_accessed=10 * CIN * COUT * 4, transcendentals=0),
        name="update",
    )(*args)


def solution(mesh):
    def local_step(act_in, shortcut, labels, w_conv, gamma, beta, w_fc, fc_bias, vel_conv, vel_gamma, vel_beta, vel_fc, vel_bias, lr):
        a = act_in.transpose(1, 2, 0, 3).reshape(ROWS, CIN)
        s = shortcut.transpose(1, 2, 0, 3).reshape(ROWS, COUT)
        wt = w_fc.T
        bias = fc_bias[None]
        z, at, pall, ptail, lab, wsq, tsq, wtb, da, sc, sh, bb, cc, dgb = forward(a, w_conv, s, gamma[None], beta[None], labels[None], bias, wt)
        g8, dgb, gsq, gfc, fsq, gb, ls = backward(at, z, s, sc, sh, bb, cc, da, dgb, pall, ptail, wtb, lab, bias)
        wo, vo, wto, vto, bo, vbo, go, vgo, beo, vbeo, loss = update_all(
            lr.reshape(1), w_conv, vel_conv, g8.reshape(CIN, COUT), wsq, gsq, wt, vel_fc.T, gfc, tsq, fsq, bias, vel_bias[None], gb, ls,
            gamma[None], beta[None], vel_gamma[None], vel_beta[None], dgb)
        return (wo, go[0], beo[0], wto.T, bo[0], vo, vgo[0], vbeo[0], vto.T, vbo[0], loss[0, 0])

    return jax.shard_map(local_step, mesh=mesh, in_specs=(P('dp'),) * 3 + (P(),) * 11, out_specs=(P(),) * 11, check_vma=False)
```
